32 devices in a mesh: pod: 1 (over z), data: 4 (over y), model: 8 (over x, core).
Axes of the slice: x: 4, y: 4, z: 1, core: 2. Of those that a mesh axis runs over, the one named last changes fastest.
The devices are a block of a 4x4x8 slice.
Arguments:
- x_in: bfloat16 [4, 1024, 2048], P(('pod', 'data'), 'model')
- dy_in: bfloat16 [4, 1024, 2048], P(('pod', 'data'), 'model')
- w_q: bfloat16 [2048, 16, 128], P(None, 'model')
- w_k: bfloat16 [1, 2048, 128], replicated
- w_v: bfloat16 [1, 2048, 128], replicated
- w_o: bfloat16 [16, 128, 2048], P('model')
Outputs:
- output 1: bfloat16 [4, 1024, 2048], P(('pod', 'data'), 'model')
- output 2: float32 [2048, 16, 128], P(('pod', 'data'), 'model')
- output 3: float32 [2048, 128], P(('pod', 'model', 'data'))
- output 4: float32 [2048, 128], P(('pod', 'model', 'data'))
- output 5: float32 [16, 128, 2048], P(('pod', 'model'), None, 'data')
All inputs are finite; a program needn't handle non-finite values.
Results may differ from the reference program's by a relative error of at most 0.00940278.
Values are sent between devices in bfloat16 or wider.
A program may use at most 768 MiB of HBM per device.

```python
import jax
import jax.numpy as jnp
from jax import lax

NUM_SEQS = 4
SEQ_LEN = 1024
MODEL_DIM = 2048
Q_HEADS = 16
KV_HEADS = 1
HEAD_DIM = 128

GROUP_HEADS = Q_HEADS // KV_HEADS


def setup_inputs(seed: int = 0, part: int = 0) -> dict:
    shared_key = jax.random.key(seed)
    part_key = jax.random.fold_in(jax.random.key(seed + 1), part)
    key_x, key_dy = jax.random.split(part_key, 2)
    key_wq, key_wk, key_wv, key_wo = jax.random.split(shared_key, 4)
    act_shape = (NUM_SEQS, SEQ_LEN, MODEL_DIM)
    in_scale = MODEL_DIM ** -0.5
    out_scale = (Q_HEADS * HEAD_DIM) ** -0.5
    x_in = jax.random.normal(key_x, act_shape, jnp.float32)
    dy_in = jax.random.normal(key_dy, act_shape, jnp.float32)
    w_q = jax.random.normal(key_wq, (MODEL_DIM, Q_HEADS, HEAD_DIM), jnp.float32) * in_scale
    w_k = jax.random.normal(key_wk, (KV_HEADS, MODEL_DIM, HEAD_DIM), jnp.float32) * in_scale
    w_v = jax.random.normal(key_wv, (KV_HEADS, MODEL_DIM, HEAD_DIM), jnp.float32) * in_scale
    w_o = jax.random.normal(key_wo, (Q_HEADS, HEAD_DIM, MODEL_DIM), jnp.float32) * out_scale
    return {'x_in': x_in.astype(jnp.bfloat16), 'dy_in': dy_in.astype(jnp.bfloat16),
            'w_q': w_q.astype(jnp.bfloat16), 'w_k': w_k.astype(jnp.bfloat16),
            'w_v': w_v.astype(jnp.bfloat16), 'w_o': w_o.astype(jnp.bfloat16)}


def group_attention(operands):
    q_grp, k_one, v_one, dout_grp = operands
    score_scale = HEAD_DIM ** -0.5
    q_f32 = q_grp.astype(jnp.float32)
    k_f32 = k_one.astype(jnp.float32)
    v_f32 = v_one.astype(jnp.float32)
    dout_f32 = dout_grp.astype(jnp.float32)
    positions = jnp.arange(SEQ_LEN)
    causal = positions[:, None] >= positions[None, :]
    scores = jnp.einsum('qhe,ke->hqk', q_f32, k_f32) * score_scale
    attn_prob = jax.nn.softmax(jnp.where(causal, scores, -jnp.inf), axis=-1)
    prob_bf = attn_prob.astype(jnp.bfloat16).astype(jnp.float32)
    attn_out = jnp.einsum('hqk,ke->qhe', prob_bf, v_f32).astype(jnp.bfloat16)
    grad_prob = jnp.einsum('qhe,ke->hqk', dout_f32, v_f32)
    row_delta = jnp.einsum('qhe,qhe->hq', dout_f32, attn_out.astype(jnp.float32))
    grad_score = (attn_prob * (grad_prob - row_delta[:, :, None])).astype(jnp.bfloat16).astype(jnp.float32)
    grad_q = (jnp.einsum('hqk,ke->qhe', grad_score, k_f32) * score_scale).astype(jnp.bfloat16)
    grad_k = (jnp.einsum('hqk,qhe->ke', grad_score, q_f32) * score_scale).astype(jnp.bfloat16)
    grad_v = jnp.einsum('hqk,qhe->ke', prob_bf, dout_f32).astype(jnp.bfloat16)
    return attn_out, grad_q, grad_k, grad_v


def heads_to_items(per_head):
    return per_head.reshape(NUM_SEQS, SEQ_LEN, KV_HEADS, GROUP_HEADS, HEAD_DIM).transpose(0, 2, 1, 3, 4).reshape(NUM_SEQS * KV_HEADS, SEQ_LEN, GROUP_HEADS, HEAD_DIM)


def items_to_heads(per_item):
    return per_item.reshape(NUM_SEQS, KV_HEADS, SEQ_LEN, GROUP_HEADS, HEAD_DIM).transpose(0, 2, 1, 3, 4).reshape(NUM_SEQS, SEQ_LEN, Q_HEADS, HEAD_DIM)


def reference(x_in, dy_in, w_q, w_k, w_v, w_o):
    x_f32 = x_in.astype(jnp.float32)
    dy_f32 = dy_in.astype(jnp.float32)
    wq_f32 = w_q.astype(jnp.float32)
    wk_f32 = w_k.astype(jnp.float32)
    wv_f32 = w_v.astype(jnp.float32)
    wo_f32 = w_o.astype(jnp.float32)
    q_proj = jnp.einsum('std,dhe->sthe', x_f32, wq_f32).astype(jnp.bfloat16)
    k_proj = jnp.einsum('std,jde->sjte', x_f32, wk_f32).astype(jnp.bfloat16)
    v_proj = jnp.einsum('std,jde->sjte', x_f32, wv_f32).astype(jnp.bfloat16)
    dout_proj = jnp.einsum('std,hed->sthe', dy_f32, wo_f32).astype(jnp.bfloat16)
    item_count = NUM_SEQS * KV_HEADS
    attn_out, grad_q, grad_k, grad_v = lax.map(group_attention, (
        heads_to_items(q_proj), k_proj.reshape(item_count, SEQ_LEN, HEAD_DIM),
        v_proj.reshape(item_count, SEQ_LEN, HEAD_DIM), heads_to_items(dout_proj)))
    out_f32 = items_to_heads(attn_out).astype(jnp.float32)
    gq_f32 = items_to_heads(grad_q).astype(jnp.float32)
    gk_f32 = grad_k.reshape(NUM_SEQS, KV_HEADS, SEQ_LEN, HEAD_DIM).astype(jnp.float32)
    gv_f32 = grad_v.reshape(NUM_SEQS, KV_HEADS, SEQ_LEN, HEAD_DIM).astype(jnp.float32)
    dw_q = jnp.einsum('std,sthe->dhe', x_f32, gq_f32)
    dw_k = jnp.einsum('std,sjte->jde', x_f32, gk_f32).reshape(KV_HEADS * MODEL_DIM, HEAD_DIM)
    dw_v = jnp.einsum('std,sjte->jde', x_f32, gv_f32).reshape(KV_HEADS * MODEL_DIM, HEAD_DIM)
    dw_o = jnp.einsum('sthe,std->hed', out_f32, dy_f32)
    dx_f32 = (jnp.einsum('sthe,dhe->std', gq_f32, wq_f32)
              + jnp.einsum('sjte,jde->std', gk_f32, wk_f32)
              + jnp.einsum('sjte,jde->std', gv_f32, wv_f32))
    return dx_f32.astype(jnp.bfloat16), dw_q, dw_k, dw_v, dw_o
```

```python
import functools

import jax
import jax.numpy as jnp
from jax import lax
from jax.experimental import pallas as pl
from jax.experimental.pallas import tpu as pltpu
from jax.sharding import PartitionSpec as P

F32 = jnp.float32
BF16 = jnp.bfloat16
NN = (((1,), (0,)), ((), ()))
NT = (((1,), (1,)), ((), ()))
TN = (((0,), (0,)), ((), ()))


def dot(a, b, dims):
    return lax.dot_general(a, b, dims, preferred_element_type=F32)


def body(cfg, x_hbm, dy_hbm, wq_hbm, wo_hbm, wk_hbm, wv_hbm,
         dx_ref, dwq_ref, dwk_ref, dwv_ref, dwo_ref,
         xf, yf, wq, wo, wkv, qf, kv, of, prob, kvb,
         dxp, dxr, xr, kvp, kvr, kr, dwa, yr, wkp, wkr,
         load_sem, ag_s, ag_r, dd_s, dd_r, xr_s, xr_r, kd_s, kd_r, kr_s, kr_r, yr_s, yr_r, wk_s, wk_r):
    tok, width, head_cols, head_dim, chips, rows = cfg
    half = tok // 2
    chunk = 2 * tok
    seq = chips * chunk
    heads = head_cols // head_dim
    wcol = width // rows
    hcol = width // 2
    hrow = head_cols // 2
    scale = head_dim ** -0.5

    me = lax.axis_index('model')
    cx = me // 2
    cc = me % 2
    cp = 1 - cc
    xright = (cx + 1) % chips
    xleft = (cx + chips - 1) % chips
    xfar = (cx + 2) % chips
    my = lax.axis_index('data')
    yup = (my + 1) % rows
    ydn = (my + rows - 1) % rows
    yfar = (my + 2) % rows
    to_r = {'model': xright * 2 + cc}
    to_l = {'model': xleft * 2 + cc}
    to_p = {'model': cx * 2 + cp}
    to_u = {'data': yup}
    to_d = {'data': ydn}
    to_f = {'data': yfar}

    def rcopy(src, dst, ssem, rsem, dev):
        return pltpu.make_async_remote_copy(src_ref=src, dst_ref=dst, send_sem=ssem, recv_sem=rsem,
                                            device_id=dev, device_id_type=pl.DeviceIdType.MESH)

    bufs = (xf, yf, kvb)

    def piece(arr, xc, core, h):
        return bufs[arr].at[pl.ds((xc * 2 + core) * tok + h * half, half), :]

    def ag_copy(arr, idx, xc, core, h, dev):
        p = piece(arr, xc, core, h)
        return rcopy(p, p, ag_s.at[arr, idx], ag_r.at[arr, (xc * 2 + core) * 2 + h], dev)

    def ag_own(arr):
        return [ag_copy(arr, 0, cx, cc, 0, to_r), ag_copy(arr, 2, cx, cc, 1, to_l),
                ag_copy(arr, 4, cx, cc, 0, to_p), ag_copy(arr, 5, cx, cc, 1, to_p),
                ag_copy(arr, 1, cx, cc, 1, to_r), ag_copy(arr, 3, cx, cc, 0, to_l)]

    def ag_relay(arr):
        return [ag_copy(arr, 6, xleft, cc, 0, to_r), ag_copy(arr, 7, xright, cc, 1, to_l)]

    def ag_cross(arr, idx, xc, h):
        return ag_copy(arr, idx, xc, cc, h, to_p)

    def ag_all_sends(arr):
        out = ag_own(arr) + ag_relay(arr)
        for idx, xc, h in ((8, xleft, 0), (9, xleft, 1), (10, xright, 0), (11, xright, 1), (12, xfar, 0), (13, xfar, 1)):
            out.append(ag_cross(arr, idx, xc, h))
        return out

    def ag_wait(arr, xc, core, h):
        p = piece(arr, xc, core, h)
        rcopy(p, p, ag_s.at[arr, 0], ag_r.at[arr, (xc * 2 + core) * 2 + h], to_p).wait_recv()

    def ag_stage1(arr):
        relays = ag_relay(arr)
        ag_wait(arr, xleft, cc, 0)
        relays[0].start()
        ag_wait(arr, xright, cc, 1)
        relays[1].start()
        ag_cross(arr, 8, xleft, 0).start()
        ag_cross(arr, 11, xright, 1).start()

    def ag_stage2(arr):
        ag_wait(arr, xright, cc, 0)
        ag_cross(arr, 10, xright, 0).start()
        ag_wait(arr, xleft, cc, 1)
        ag_cross(arr, 9, xleft, 1).start()

    def ag_stage3(arr):
        ag_wait(arr, xfar, cc, 0)
        ag_cross(arr, 12, xfar, 0).start()
        ag_wait(arr, xfar, cc, 1)
        ag_cross(arr, 13, xfar, 1).start()

    def ag_partner(arr, xc):
        ag_wait(arr, xc, cp, 0)
        ag_wait(arr, xc, cp, 1)

    def dd_copy(xc):
        return rcopy(dxp.at[xc * 2 + cp], dxr.at[xc], dd_s.at[xc], dd_r.at[xc], to_p)

    def dd_add(xc):
        dd_copy(xc).wait_recv()
        blk = xc * 2 + cc
        dxp[blk] = dxp[blk] + dxr[xc]

    def kd_copy(xc):
        return rcopy(kvp.at[xc * 2 + cp], kvr.at[xc], kd_s.at[xc], kd_r.at[xc], to_p)

    def xpart(xc, h, cl):
        return dxp.at[xc * 2 + cc, pl.ds(h * half, half), pl.ds(cl * hcol, hcol)]

    def kpart(xc, h):
        return kvp.at[xc * 2 + cc, pl.ds(h * half, half), :]

    def ring_src(kind, side):
        if kind == 0:
            return (xright, 1) if side == 0 else (xleft, 0)
        if kind == 1:
            return (xfar, 0) if side == 0 else (xfar, 1)
        return (xright, 0) if side == 0 else (xleft, 1)

    def x_copy(side, kind, cl):
        xc, h = ring_src(kind, side)
        return rcopy(xpart(xc, h, cl), xr.at[side, kind, cl], xr_s.at[side, kind, cl], xr_r.at[side, kind, cl],
                     to_r if side == 0 else to_l)

    def k_copy(side, kind):
        xc, h = ring_src(kind, side)
        return rcopy(kpart(xc, h), kr.at[side, kind], kr_s.at[side, kind], kr_r.at[side, kind],
                     to_r if side == 0 else to_l)

    def x_pass(cl):
        for side in range(2):
            x_copy(side, 1, cl).wait_recv()
            xc, h = ring_src(2, side)
            ref = xpart(xc, h, cl)
            ref[...] = ref[...] + xr[side, 1, cl]
            x_copy(side, 2, cl).start()

    def k_pass():
        for side in range(2):
            k_copy(side, 1).wait_recv()
            xc, h = ring_src(2, side)
            ref = kpart(xc, h)
            ref[...] = ref[...] + kr[side, 1]
            k_copy(side, 2).start()

    def wpart(w, blk, h):
        return dwa.at[w, blk, pl.ds(h * hrow, hrow), :]

    def y_src(kind, side):
        if kind == 0:
            return (yup, 1) if side == 0 else (ydn, 0)
        if kind == 1:
            return (yfar, 0) if side == 0 else (yfar, 1)
        return (yup, 0) if side == 0 else (ydn, 1)

    def y_copy(w, side, kind):
        blk, h = y_src(kind, side)
        return rcopy(wpart(w, blk, h), yr.at[w, side, kind], yr_s.at[w, side, kind], yr_r.at[w, side, kind],
                     to_u if side == 0 else to_d)

    def y_first(w):
        for kind in (1, 0):
            for side in range(2):
                y_copy(w, side, kind).start()

    def y_pass(w):
        for side in range(2):
            y_copy(w, side, 1).wait_recv()
            blk, h = y_src(2, side)
            ref = wpart(w, blk, h)
            ref[...] = ref[...] + yr[w, side, 1]
            y_copy(w, side, 2).start()

    def y_final(w):
        for side in range(2):
            y_copy(w, side, 0).wait_recv()
            y_copy(w, side, 2).wait_recv()
        top = dwa[w, my, 0:hrow, :] + yr[w, 1, 0] + yr[w, 0, 2]
        low = dwa[w, my, hrow:, :] + yr[w, 0, 0] + yr[w, 1, 2]
        return top, low

    own_rows = pl.ds(me * tok, tok)
    loads = [pltpu.make_async_copy(x_hbm, xf.at[own_rows, :], load_sem.at[0]),
             pltpu.make_async_copy(dy_hbm, yf.at[own_rows, :], load_sem.at[1]),
             pltpu.make_async_copy(wq_hbm, wq, load_sem.at[2]),
             pltpu.make_async_copy(wk_hbm, wkv.at[:, pl.ds(0, head_dim)], load_sem.at[3]),
             pltpu.make_async_copy(wv_hbm, wkv.at[:, pl.ds(head_dim, head_dim)], load_sem.at[4]),
             pltpu.make_async_copy(wo_hbm, wo, load_sem.at[5])]
    for cp_ in loads:
        cp_.start()
    barrier = pltpu.get_barrier_semaphore()
    for dev in (to_r, to_l, to_p, to_u, to_d, to_f):
        pl.semaphore_signal(barrier, inc=1, device_id=dev, device_id_type=pl.DeviceIdType.MESH)
    pl.semaphore_wait(barrier, 6)
    loads[0].wait()
    for cp_ in ag_own(0):
        cp_.start()
    dwa[...] = jnp.zeros_like(dwa)
    kvp[...] = jnp.zeros_like(kvp)
    for cp_ in loads[1:]:
        cp_.wait()

    def chunk_of(s):
        return (cx + s + s // 2 - 2 * (s // 3)) % chips

    @pl.loop(0, chips)
    def _(s):
        @pl.when(s == 0)
        def _():
            ag_partner(0, cx)

        @pl.when(s == 1)
        def _():
            ag_stage1(0)
            for cp_ in ag_own(1):
                cp_.start()
            ag_stage2(0)
            ag_partner(0, xright)

        @pl.when(s == 2)
        def _():
            ag_partner(0, xleft)

        @pl.when(s == 3)
        def _():
            ag_stage3(0)
            ag_partner(0, xfar)

        r = pl.ds(chunk_of(s) * chunk, chunk)
        xc = xf[r, :]
        qf[r, :] = dot(xc, wq[...], NN).astype(BF16)
        kv[r, :] = dot(xc, wkv[...], NN).astype(BF16)

    @pl.loop(0, chips)
    def _(s):
        @pl.when(s == 2)
        def _():
            ag_stage1(1)

        i = chunk_of(s)
        r = pl.ds(i * chunk, chunk)
        row_id = lax.broadcasted_iota(jnp.int32, (chunk, seq), 0) + i * chunk
        keep = row_id >= lax.broadcasted_iota(jnp.int32, (chunk, seq), 1)
        for h in range(heads):
            hc = pl.ds(h * head_dim, head_dim)
            sc = dot(qf[r, hc], kv[:, 0:head_dim], NT) * scale
            sc = jnp.where(keep, sc, -jnp.inf)
            ex = jnp.exp(sc - jnp.max(sc, axis=-1, keepdims=True))
            pr = ex * (1.0 / jnp.sum(ex, axis=-1, keepdims=True))
            prob[h, r, :] = pr
            of[r, hc] = dot(pr.astype(BF16), kv[:, head_dim:], NN).astype(BF16)

    @pl.loop(0, chips)
    def _(s):
        @pl.when(s == 0)
        def _():
            ag_partner(1, cx)

        @pl.when(s == 1)
        def _():
            ag_stage2(1)
            ag_partner(1, xright)

        @pl.when(s == 2)
        def _():
            ag_partner(1, xleft)

        @pl.when(s == 3)
        def _():
            dd_add(xright)
            x_copy(0, 0, 0).start()
            ag_stage3(1)
            dd_add(xleft)
            x_copy(1, 0, 0).start()
            ag_partner(1, xfar)

        i = chunk_of(s)
        r = pl.ds(i * chunk, chunk)
        yc = yf[r, :]
        oc = of[r, :]
        for j in range(rows):
            dwa[0, j] += dot(oc, yf[r, j * wcol:(j + 1) * wcol], TN)

        @pl.when(s == 3)
        def _():
            y_first(0)

        do = dot(yc, wo[...], NT).astype(BF16)
        od = do.astype(F32) * oc.astype(F32)
        dqs = []
        for h in range(heads):
            hs = slice(h * head_dim, (h + 1) * head_dim)
            dp = dot(do[:, hs], kv[:, head_dim:], NT)
            pr = prob[h, r, :]
            ds = (pr * (dp - jnp.sum(od[:, hs], axis=-1, keepdims=True))).astype(BF16)
            dqs.append((dot(ds, kv[:, 0:head_dim], NN) * scale).astype(BF16))
            dk = dot(ds, qf[r, hs], TN)
            dv = dot(pr.astype(BF16), do[:, hs], TN)
            kvp[:, :, 0:head_dim] += dk.reshape(2 * chips, tok, head_dim)
            kvp[:, :, head_dim:] += dv.reshape(2 * chips, tok, head_dim)
        dq = jnp.concatenate(dqs, axis=1)
        for j in range(rows):
            dwa[1, j] += dot(dq, xf[r, j * wcol:(j + 1) * wcol], TN)
        for j in range(rows):
            dxp[pl.ds(2 * i, 2), :, j * wcol:(j + 1) * wcol] = dot(dq, wq[j * wcol:(j + 1) * wcol, :], NT).reshape(2, tok, wcol)
        dd_copy(i).start()

    kvp[:, :, 0:head_dim] = kvp[:, :, 0:head_dim] * scale
    for xc in range(chips):
        kd_copy(xc).start()
    y_first(1)
    for xc in range(chips):
        kd_copy(xc).wait_recv()
        blk = xc * 2 + cc
        kvp[blk] = kvp[blk] + kvr[xc]
    for kind in (1, 0):
        for side in range(2):
            k_copy(side, kind).start()
    for side in range(2):
        x_copy(side, 0, 1).start()
    dd_add(xfar)
    k_pass()
    for side in range(2):
        x_copy(side, 1, 0).start()
    dd_add(cx)
    y_pass(0)
    for side in range(2):
        k_copy(side, 0).wait_recv()
        k_copy(side, 2).wait_recv()
    own = cx * 2 + cc
    kvb[pl.ds(me * tok, half), :] = (kvp[own, 0:half, :] + kr[1, 0] + kr[0, 2]).astype(BF16)
    kvb[pl.ds(me * tok + half, half), :] = (kvp[own, half:, :] + kr[0, 0] + kr[1, 2]).astype(BF16)
    for cp_ in ag_own(2):
        cp_.start()
    for side in range(2):
        x_copy(side, 1, 1).start()
    ag_stage1(2)
    ag_stage2(2)
    x_pass(0)
    ag_stage3(2)
    ag_partner(2, cx)
    ag_partner(2, xright)
    ag_partner(2, xleft)
    ag_partner(2, xfar)
    mrow = width // (2 * chips)
    krow = mrow // rows
    part = dot(xf[:, pl.ds(pl.multiple_of(me * mrow, mrow), mrow)], kvb[...], TN)
    wkp[...] = part.reshape(rows, krow, head_cols)

    def wk_copy(idx, blk, dev):
        return rcopy(wkp.at[blk], wkr.at[idx], wk_s.at[idx], wk_r.at[idx], dev)

    wk_copies = [wk_copy(0, yup, to_u), wk_copy(1, ydn, to_d), wk_copy(2, yfar, to_f)]
    for cp_ in wk_copies:
        cp_.start()
    x_pass(1)
    y_pass(1)
    top, low = y_final(0)
    dwo_ref[0:hrow, :] = top
    dwo_ref[hrow:, :] = low
    top, low = y_final(1)
    dwq_ref[:, 0:hrow] = top.T
    dwq_ref[:, hrow:] = low.T
    for cp_ in wk_copies:
        cp_.wait_recv()
    wk_sum = wkp[my] + wkr[0] + wkr[1] + wkr[2]
    dwk_ref[...] = wk_sum[:, 0:head_dim]
    dwv_ref[...] = wk_sum[:, head_dim:]
    kv_own = kvb[own_rows, :]
    for cl in range(2):
        cols = slice(cl * hcol, (cl + 1) * hcol)
        kv_term = dot(kv_own, wkv[cols, :], NT)
        for side in range(2):
            x_copy(side, 0, cl).wait_recv()
            x_copy(side, 2, cl).wait_recv()
        dx_ref[0:half, cols] = (kv_term[0:half] + dxp[own, 0:half, cols] + xr[1, 0, cl] + xr[0, 2, cl]).astype(BF16)
        dx_ref[half:, cols] = (kv_term[half:] + dxp[own, half:, cols] + xr[0, 0, cl] + xr[1, 2, cl]).astype(BF16)

    for arr in range(3):
        for cp_ in ag_all_sends(arr):
            cp_.wait_send()
    for xc in range(chips):
        dd_copy(xc).wait_send()
        kd_copy(xc).wait_send()
    for side in range(2):
        for kind in range(3):
            k_copy(side, kind).wait_send()
            for cl in range(2):
                x_copy(side, kind, cl).wait_send()
            for w in range(2):
                y_copy(w, side, kind).wait_send()
    for cp_ in wk_copies:
        cp_.wait_send()


def solution(mesh):
    model_size = mesh.shape['model']
    data_size = mesh.shape['data']
    tok_spec = P(('pod', 'data'), 'model', None)
    chips = model_size // 2

    def device_step(x_loc, dy_loc, w_q, w_k, w_v, w_o):
        tok, width = x_loc.shape[1:]
        head_dim = w_k.shape[2]
        head_cols = w_q.shape[1] * head_dim
        assert chips == 4 and data_size == 4 and w_k.shape[0] == 1 and x_loc.shape[0] == 1
        seq = model_size * tok
        half = tok // 2
        wcol = width // data_size
        krow = width // (model_size * data_size)
        cfg = (tok, width, head_cols, head_dim, chips, data_size)
        vm = pltpu.VMEM
        dma = pltpu.SemaphoreType.DMA
        scratch = [
            vm((seq, width), BF16), vm((seq, width), BF16), vm((width, head_cols), BF16), vm((head_cols, width), BF16),
            vm((width, 2 * head_dim), BF16), vm((seq, head_cols), BF16), vm((seq, 2 * head_dim), BF16), vm((seq, head_cols), BF16),
            vm((head_cols // head_dim, seq, seq), F32), vm((seq, 2 * head_dim), BF16),
            vm((model_size, tok, width), F32), vm((chips, tok, width), F32), vm((2, 3, 2, half, width // 2), F32),
            vm((model_size, tok, 2 * head_dim), F32), vm((chips, tok, 2 * head_dim), F32), vm((2, 3, half, 2 * head_dim), F32),
            vm((2, data_size, head_cols, wcol), F32), vm((2, 2, 3, head_cols // 2, wcol), F32),
            vm((data_size, krow, 2 * head_dim), F32), vm((3, krow, 2 * head_dim), F32),
            dma((6,)), dma((3, 14)), dma((3, 16)), dma((chips,)), dma((chips,)), dma((2, 3, 2)), dma((2, 3, 2)),
            dma((chips,)), dma((chips,)), dma((2, 3)), dma((2, 3)), dma((2, 2, 3)), dma((2, 2, 3)), dma((3,)), dma((3,)),
        ]
        anyspec = pl.BlockSpec(memory_space=pl.ANY)
        vspec = pl.BlockSpec(memory_space=pltpu.VMEM)
        dx, dwq, dwk, dwv, dwo = pl.pallas_call(
            functools.partial(body, cfg),
            out_shape=(jax.ShapeDtypeStruct((tok, width), BF16), jax.ShapeDtypeStruct((wcol, head_cols), F32),
                       jax.ShapeDtypeStruct((krow, head_dim), F32), jax.ShapeDtypeStruct((krow, head_dim), F32),
                       jax.ShapeDtypeStruct((head_cols, wcol), F32)),
            in_specs=[anyspec] * 6,
            out_specs=(vspec,) * 5,
            scratch_shapes=scratch,
            compiler_params=pltpu.CompilerParams(collective_id=0, has_side_effects=True, vmem_limit_bytes=67000000),
            name='attn_bwd',
        )(x_loc[0], dy_loc[0], w_q.reshape(width, head_cols), w_o.reshape(head_cols, width), w_k[0], w_v[0])
        return (dx[None], dwq.reshape(wcol, head_cols // head_dim, head_dim), dwk, dwv,
                dwo.reshape(head_cols // head_dim, head_dim, wcol))

    kv_rows = P(('pod', 'model', 'data'), None)
    return jax.shard_map(device_step, mesh=mesh,
                         in_specs=(tok_spec, tok_spec, P(None, 'model', None), P(), P(), P('model', None, None)),
                         out_specs=(tok_spec, P(('pod', 'data'), 'model', None), kv_rows, kv_rows, P(('pod', 'model'), None, 'data')),
                         check_vma=False)
```

```python
import functools

import jax
import jax.numpy as jnp
from jax import lax
from jax.experimental import pallas as pl
from jax.experimental.pallas import tpu as pltpu
from jax.sharding import PartitionSpec as P

F32 = jnp.float32
BF16 = jnp.bfloat16
NN = (((1,), (0,)), ((), ()))
NT = (((1,), (1,)), ((), ()))
TN = (((0,), (0,)), ((), ()))


def dot(a, b, dims):
    return lax.dot_general(a, b, dims, preferred_element_type=F32)


def body(cfg, x_hbm, dy_hbm, wq_hbm, wo_hbm, wk_hbm, wv_hbm,
         dx_ref, dwq_ref, dwk_ref, dwv_ref, dwo_ref,
         xf, yf, wq, wo, wkv, wq2, wq2f, qf, kv, of, prob, dsf, dqf, dof, kvb,
         dxp, dxr, xr, kvp, kvr, kr, dwa, yr, wkp, wkr,
         load_sem, ag_s, ag_r, dd_s, dd_r, xr_s, xr_r, kd_s, kd_r, kr_s, kr_r, yr_s, yr_r, wk_s, wk_r):
    tok, width, head_cols, head_dim, chips, rows = cfg
    half = tok // 2
    chunk = 2 * tok
    seq = chips * chunk
    heads = head_cols // head_dim
    wcol = width // (2 * rows)
    pieces = 4
    pcol = width // pieces
    hcol = width // 2
    scale = head_dim ** -0.5

    me = lax.axis_index('model')
    cx = me // 2
    cc = me % 2
    cp = 1 - cc
    xright = (cx + 1) % chips
    xleft = (cx + chips - 1) % chips
    xfar = (cx + 2) % chips
    my = lax.axis_index('data')
    yup = (my + 1) % rows
    ydn = (my + rows - 1) % rows
    yfar = (my + 2) % rows
    to_r = {'model': xright * 2 + cc}
    to_l = {'model': xleft * 2 + cc}
    to_p = {'model': cx * 2 + cp}
    to_u = {'data': yup}
    to_d = {'data': ydn}
    to_f = {'data': yfar}

    def rcopy(src, dst, ssem, rsem, dev):
        return pltpu.make_async_remote_copy(src_ref=src, dst_ref=dst, send_sem=ssem, recv_sem=rsem,
                                            device_id=dev, device_id_type=pl.DeviceIdType.MESH)

    def piece(arr, xc, core, h):
        r = pl.ds((xc * 2 + core) * tok + h * half, half)
        if arr == 0:
            return xf.at[r, :]
        if arr == 3:
            return kvb.at[r, :]
        return yf.at[r, pl.ds((arr - 1) * hcol, hcol)]

    def ag_copy(arr, idx, xc, core, h, dev):
        p = piece(arr, xc, core, h)
        return rcopy(p, p, ag_s.at[arr, idx], ag_r.at[arr, (xc * 2 + core) * 2 + h], dev)

    def ag_first(arr):
        return [ag_copy(arr, 0, cx, cc, 0, to_r), ag_copy(arr, 2, cx, cc, 1, to_l),
                ag_copy(arr, 4, cx, cc, 0, to_p), ag_copy(arr, 5, cx, cc, 1, to_p)]

    def ag_second(arr):
        return [ag_copy(arr, 1, cx, cc, 1, to_r), ag_copy(arr, 3, cx, cc, 0, to_l)]

    def ag_own(arr):
        return ag_first(arr) + ag_second(arr)

    def ag_relay(arr):
        return [ag_copy(arr, 6, xleft, cc, 0, to_r), ag_copy(arr, 7, xright, cc, 1, to_l)]

    def ag_cross(arr, idx, xc, h):
        return ag_copy(arr, idx, xc, cc, h, to_p)

    def ag_all_sends(arr):
        out = ag_own(arr) + ag_relay(arr)
        for idx, xc, h in ((8, xleft, 0), (9, xleft, 1), (10, xright, 0), (11, xright, 1), (12, xfar, 0), (13, xfar, 1)):
            out.append(ag_cross(arr, idx, xc, h))
        return out

    def ag_wait(arr, xc, core, h):
        p = piece(arr, xc, core, h)
        rcopy(p, p, ag_s.at[arr, 0], ag_r.at[arr, (xc * 2 + core) * 2 + h], to_p).wait_recv()

    def ag_stage1(arr):
        relays = ag_relay(arr)
        ag_wait(arr, xleft, cc, 0)
        relays[0].start()
        ag_wait(arr, xright, cc, 1)
        relays[1].start()
        ag_cross(arr, 8, xleft, 0).start()
        ag_cross(arr, 11, xright, 1).start()

    def ag_stage2(arr):
        ag_wait(arr, xright, cc, 0)
        ag_cross(arr, 10, xright, 0).start()
        ag_wait(arr, xleft, cc, 1)
        ag_cross(arr, 9, xleft, 1).start()

    def ag_stage3(arr):
        ag_wait(arr, xfar, cc, 0)
        ag_cross(arr, 12, xfar, 0).start()
        ag_wait(arr, xfar, cc, 1)
        ag_cross(arr, 13, xfar, 1).start()

    def ag_partner(arr, xc):
        ag_wait(arr, xc, cp, 0)
        ag_wait(arr, xc, cp, 1)

    def dd_copy(xc):
        return rcopy(dxp.at[xc * 2 + cp], dxr.at[xc], dd_s.at[xc], dd_r.at[xc], to_p)

    def dd_add(xc):
        dd_copy(xc).wait_recv()
        blk = xc * 2 + cc
        dxp[blk] = dxp[blk] + dxr[xc]

    def kd_copy(xc):
        return rcopy(kvp.at[xc * 2 + cp], kvr.at[xc], kd_s.at[xc], kd_r.at[xc], to_p)

    def xpart(xc, h, cl):
        return dxp.at[xc * 2 + cc, pl.ds(h * half, half), pl.ds(cl * pcol, pcol)]

    def kpart(xc, h):
        return kvp.at[xc * 2 + cc, pl.ds(h * half, half), :]

    def ring_src(kind, side):
        if kind == 0:
            return (xright, 1) if side == 0 else (xleft, 0)
        if kind == 1:
            return (xfar, 0) if side == 0 else (xfar, 1)
        return (xright, 0) if side == 0 else (xleft, 1)

    def x_copy(side, kind, cl):
        xc, h = ring_src(kind, side)
        return rcopy(xpart(xc, h, cl), xr.at[side, kind, cl], xr_s.at[side, kind, cl], xr_r.at[side, kind, cl],
                     to_r if side == 0 else to_l)

    def k_copy(side, kind):
        xc, h = ring_src(kind, side)
        return rcopy(kpart(xc, h), kr.at[side, kind], kr_s.at[side, kind], kr_r.at[side, kind],
                     to_r if side == 0 else to_l)

    def x_pass(cl):
        for side in range(2):
            x_copy(side, 1, cl).wait_recv()
            xc, h = ring_src(2, side)
            ref = xpart(xc, h, cl)
            ref[...] = ref[...] + xr[side, 1, cl]
            x_copy(side, 2, cl).start()

    def k_pass():
        for side in range(2):
            k_copy(side, 1).wait_recv()
            xc, h = ring_src(2, side)
            ref = kpart(xc, h)
            ref[...] = ref[...] + kr[side, 1]
            k_copy(side, 2).start()

    order = ((yfar, 0), (yfar, 1), (yup, 1), (ydn, 0), (yup, 0), (ydn, 1), (my, 0), (my, 1))

    def y_blk(w, kind, side):
        pos = {(1, 0): 0, (1, 1): 1, (0, 0): 2, (0, 1): 3, (2, 0): 4, (2, 1): 5, (3, 0): 6, (3, 1): 7}[kind, side]
        if w == 0:
            return pos
        return order[pos][0] * 2 + order[pos][1]

    def y_copy(w, side, kind):
        return rcopy(dwa.at[w, y_blk(w, kind, side)], yr.at[w, side, kind], yr_s.at[w, side, kind], yr_r.at[w, side, kind],
                     to_u if side == 0 else to_d)

    def dw_block(w, kind, side):
        blk = y_blk(w, kind, side)
        if w == 0:
            dwa[0, blk] = dot(of[...], yf[:, blk * wcol:(blk + 1) * wcol], TN)
        else:
            dwa[1, blk] = dot(dqf[...], xf[:, pl.ds(pl.multiple_of(blk * wcol, wcol), wcol)], TN)

    def y_first(w):
        for kind in (1, 0):
            for side in range(2):
                dw_block(w, kind, side)
                y_copy(w, side, kind).start()

    def y_rest(w):
        for kind in (2, 3):
            for side in range(2):
                dw_block(w, kind, side)

    def y_pass(w):
        for side in range(2):
            y_copy(w, side, 1).wait_recv()
            blk = y_blk(w, 2, side)
            dwa[w, blk] = dwa[w, blk] + yr[w, side, 1]
            y_copy(w, side, 2).start()

    def y_final(w):
        for side in range(2):
            y_copy(w, side, 0).wait_recv()
            y_copy(w, side, 2).wait_recv()
        first = dwa[w, y_blk(w, 3, 0)] + yr[w, 1, 0] + yr[w, 0, 2]
        second = dwa[w, y_blk(w, 3, 1)] + yr[w, 0, 0] + yr[w, 1, 2]
        return first, second

    own_rows = pl.ds(me * tok, tok)
    loads = [pltpu.make_async_copy(x_hbm, xf.at[own_rows, :], load_sem.at[0]),
             pltpu.make_async_copy(wq_hbm, wq2, load_sem.at[1]),
             pltpu.make_async_copy(wk_hbm, wkv.at[:, pl.ds(0, head_dim)], load_sem.at[2]),
             pltpu.make_async_copy(wv_hbm, wkv.at[:, pl.ds(head_dim, head_dim)], load_sem.at[3])]
    for pos, (dest, part) in enumerate(order):
        src = pl.ds(pl.multiple_of((dest * 2 + part) * wcol, wcol), wcol)
        dst = pl.ds(pos * wcol, wcol)
        loads.append(pltpu.make_async_copy(dy_hbm.at[:, src], yf.at[own_rows, dst], load_sem.at[4 + pos]))
        loads.append(pltpu.make_async_copy(wo_hbm.at[:, src], wo.at[:, dst], load_sem.at[12 + pos]))
    for cp_ in loads:
        cp_.start()
    barrier = pltpu.get_barrier_semaphore()
    for dev in (to_r, to_l, to_p, to_u, to_d, to_f):
        pl.semaphore_signal(barrier, inc=1, device_id=dev, device_id_type=pl.DeviceIdType.MESH)
    with jax.named_scope('barrier'):
        pl.semaphore_wait(barrier, 6)
    loads[0].wait()
    for cp_ in ag_own(0):
        cp_.start()
    with jax.named_scope('loadw'):
        for cp_ in loads[1:]:
            cp_.wait()
        step = 2 * width // 8

        @pl.loop(0, 8)
        def _(b):
            r2 = pl.ds(pl.multiple_of(b * step, step), step)
            wq2f[r2, :] = wq2[r2, :].astype(F32)
            r1 = pl.ds(pl.multiple_of(b * (step // 2), step // 2), step // 2)
            for h in range(heads):
                wq[r1, h * head_dim:(h + 1) * head_dim] = wq2f[pl.ds(b * step + h, step // 2, stride=heads), :].astype(BF16)

    def chunk_of(s):
        return (cx + s + s // 2 - 2 * (s // 3)) % chips

    @pl.loop(0, chips)
    def _(s):
        @pl.when(s == 0)
        def _():
            ag_partner(0, cx)

        @pl.when(s == 1)
        def _():
            ag_stage1(0)
            for cp_ in ag_own(1):
                cp_.start()
            for cp_ in ag_first(2):
                cp_.start()
            ag_stage2(0)
            ag_partner(0, xright)

        @pl.when(s == 2)
        def _():
            ag_partner(0, xleft)

        @pl.when(s == 3)
        def _():
            ag_stage3(0)
            ag_partner(0, xfar)

        r = pl.ds(chunk_of(s) * chunk, chunk)
        xc = xf[r, :]
        qf[r, :] = dot(xc, wq[...], NN).astype(BF16)
        kv[r, :] = dot(xc, wkv[...], NN).astype(BF16)

    @pl.loop(0, chips)
    def _(s):
        @pl.when(s == 1)
        def _():
            ag_stage1(1)
            for cp_ in ag_second(2):
                cp_.start()

        @pl.when(s == 2)
        def _():
            ag_stage2(1)

        i = chunk_of(s)
        r = pl.ds(i * chunk, chunk)
        row_id = lax.broadcasted_iota(jnp.int32, (chunk, seq), 0) + i * chunk
        keep = row_id >= lax.broadcasted_iota(jnp.int32, (chunk, seq), 1)
        for h in range(heads):
            hc = pl.ds(h * head_dim, head_dim)
            sc = dot(qf[r, hc], kv[:, 0:head_dim], NT) * scale
            sc = jnp.where(keep, sc, -jnp.inf)
            ex = jnp.exp(sc - jnp.max(sc, axis=-1, keepdims=True))
            pr = ex * (1.0 / jnp.sum(ex, axis=-1, keepdims=True))
            prob[h, r, :] = pr
            of[r, hc] = dot(pr.astype(BF16), kv[:, head_dim:], NN).astype(BF16)

    ag_stage1(2)
    ag_partner(1, cx)
    ag_partner(2, cx)

    @pl.loop(0, chips)
    def _(s):
        @pl.when(s == 1)
        def _():
            with jax.named_scope('b1'):
                ag_stage3(1)
                for xc in (xright, xleft, xfar):
                    ag_partner(1, xc)
            with jax.named_scope('b1y'):
                y_first(0)
            with jax.named_scope('b1w'):
                ag_stage2(2)
                ag_partner(2, xright)

        @pl.when(s == 2)
        def _():
            with jax.named_scope('b2'):
                ag_stage3(2)
                ag_partner(2, xleft)

        @pl.when(s == 3)
        def _():
            with jax.named_scope('b3'):
                dd_add(xright)
                for cl in range(2):
                    x_copy(0, 0, cl).start()
                ag_partner(2, xfar)

        with jax.named_scope('b_comp'):
            i = chunk_of(s)
            r = pl.ds(i * chunk, chunk)
            oc = of[r, :]
            do = dot(yf[r, :], wo[...], NT).astype(BF16)
            dof[r, :] = do
            od = do.astype(F32) * oc.astype(F32)
            for h in range(heads):
                hs = slice(h * head_dim, (h + 1) * head_dim)
                dp = dot(do[:, hs], kv[:, head_dim:], NT)
                ds = (prob[h, r, :] * (dp - jnp.sum(od[:, hs], axis=-1, keepdims=True))).astype(BF16)
                dsf[h, r, :] = ds
                dqf[r, hs] = (dot(ds, kv[:, 0:head_dim], NN) * scale).astype(BF16)
            dq = dqf[r, :]
            for j in range(pieces):
                dxp[pl.ds(2 * i, 2), :, j * pcol:(j + 1) * pcol] = dot(dq, wq[j * pcol:(j + 1) * pcol, :], NT).reshape(2, tok, pcol)
        dd_copy(i).start()

    with jax.named_scope('t00_dkv'):
        dd_add(xleft)
        for cl in range(2):
            x_copy(1, 0, cl).start()
        for kc in range(chips):
            ks = slice(kc * chunk, (kc + 1) * chunk)
            qs = slice(kc * chunk, seq)
            dk = jnp.zeros((chunk, head_dim), F32)
            dv = jnp.zeros((chunk, head_dim), F32)
            for h in range(heads):
                hs = slice(h * head_dim, (h + 1) * head_dim)
                dk = dk + dot(dsf[h, qs, ks], qf[qs, hs], TN)
                dv = dv + dot(prob[h, qs, ks].astype(BF16), dof[qs, hs], TN)
            kvp[2 * kc:2 * kc + 2, :, 0:head_dim] = (dk * scale).reshape(2, tok, head_dim)
            kvp[2 * kc:2 * kc + 2, :, head_dim:] = dv.reshape(2, tok, head_dim)
        for xc in range(chips):
            kd_copy(xc).start()

    def x_send(kind, cl):
        for side in range(2):
            x_copy(side, kind, cl).start()

    own = cx * 2 + cc

    def dx_final(cl):
        cols = slice(cl * pcol, (cl + 1) * pcol)
        kv_term = dot(kvb[own_rows, :], wkv[cols, :], NT)
        for side in range(2):
            x_copy(side, 0, cl).wait_recv()
            x_copy(side, 2, cl).wait_recv()
        dx_ref[0:half, cols] = (kv_term[0:half] + dxp[own, 0:half, cols] + xr[1, 0, cl] + xr[0, 2, cl]).astype(BF16)
        dx_ref[half:, cols] = (kv_term[half:] + dxp[own, half:, cols] + xr[0, 0, cl] + xr[1, 2, cl]).astype(BF16)

    with jax.named_scope('t01_ddfar'):
        dd_add(xfar)
        x_send(1, 0)
    with jax.named_scope('t02_y1'):
        y_first(1)
    with jax.named_scope('t03_kd'):
        for xc in range(chips):
            kd_copy(xc).wait_recv()
            blk = xc * 2 + cc
            kvp[blk] = kvp[blk] + kvr[xc]
        for kind in (1, 0):
            for side in range(2):
                k_copy(side, kind).start()
        x_send(0, 2)
    with jax.named_scope('t04_y0'):
        y_rest(0)
        y_pass(0)
    with jax.named_scope('t05_y1r'):
        y_rest(1)
        dd_add(cx)
    with jax.named_scope('t06_kpass'):
        k_pass()
        x_send(1, 1)
    with jax.named_scope('t07_kfin'):
        for side in range(2):
            k_copy(side, 0).wait_recv()
            k_copy(side, 2).wait_recv()
        kvb[pl.ds(me * tok, half), :] = (kvp[own, 0:half, :] + kr[1, 0] + kr[0, 2]).astype(BF16)
        kvb[pl.ds(me * tok + half, half), :] = (kvp[own, half:, :] + kr[0, 0] + kr[1, 2]).astype(BF16)
        for cp_ in ag_own(3):
            cp_.start()
    with jax.named_scope('t08_xp0'):
        x_pass(0)
    with jax.named_scope('t09_ag'):
        ag_stage1(3)
        x_send(1, 2)
        ag_stage2(3)
    with jax.named_scope('t10_xp1'):
        x_pass(1)
        x_send(1, 3)
        x_send(0, 3)
    with jax.named_scope('t11_ag'):
        ag_stage3(3)
        for xc in (cx, xright, xleft, xfar):
            ag_partner(3, xc)
    mrow = width // (2 * chips)
    krow = mrow // rows
    with jax.named_scope('t12_wk'):
        part = dot(xf[:, pl.ds(pl.multiple_of(me * mrow, mrow), mrow)], kvb[...], TN)
        wkp[...] = part.reshape(rows, krow, 2 * head_dim)

    def wk_copy(idx, blk, dev):
        return rcopy(wkp.at[blk], wkr.at[idx], wk_s.at[idx], wk_r.at[idx], dev)

    wk_copies = [wk_copy(0, yup, to_u), wk_copy(1, ydn, to_d), wk_copy(2, yfar, to_f)]
    for cp_ in wk_copies:
        cp_.start()
    with jax.named_scope('t13_y1'):
        y_pass(1)
    with jax.named_scope('t14_xp2'):
        x_pass(2)
    with jax.named_scope('t15_y0f'):
        first, second = y_final(0)
        dwo_ref[:, 0:wcol] = first
        dwo_ref[:, wcol:] = second
        dx_final(0)
    with jax.named_scope('t16_xp3'):
        x_pass(3)
    with jax.named_scope('t17_y1f'):
        for idx, val in enumerate(y_final(1)):
            val = val.T
            for h in range(heads):
                dwq_ref[pl.ds(idx * wcol * heads + h, wcol, stride=heads), :] = val[:, h * head_dim:(h + 1) * head_dim]
        for cp_ in wk_copies:
            cp_.wait_recv()
        wk_sum = wkp[my] + wkr[0] + wkr[1] + wkr[2]
        dwk_ref[...] = wk_sum[:, 0:head_dim]
        dwv_ref[...] = wk_sum[:, head_dim:]
    for cl in range(1, pieces):
        with jax.named_scope('t18_dx%d' % cl):
            dx_final(cl)

    with jax.named_scope('t19_sends'):
        for arr in range(4):
            for cp_ in ag_all_sends(arr):
                cp_.wait_send()
        for xc in range(chips):
            dd_copy(xc).wait_send()
            kd_copy(xc).wait_send()
        for side in range(2):
            for kind in range(3):
                k_copy(side, kind).wait_send()
                for cl in range(pieces):
                    x_copy(side, kind, cl).wait_send()
                for w in range(2):
                    y_copy(w, side, kind).wait_send()
        for cp_ in wk_copies:
            cp_.wait_send()


def copy_out(*refs):
    n = (len(refs) - 1) // 2
    sem = refs[-1]
    copies = [pltpu.make_async_copy(refs[k], refs[n + k], sem.at[k]) for k in range(n)]
    for cp_ in copies:
        cp_.start()
    for cp_ in copies:
        cp_.wait()


VMEM_LIMIT = 64 * 1000 * 1000


def solution(mesh):
    model_size = mesh.shape['model']
    data_size = mesh.shape['data']
    tok_spec = P(('pod', 'data'), 'model', None)
    chips = model_size // 2

    def device_step(x_loc, dy_loc, w_q, w_k, w_v, w_o):
        tok, width = x_loc.shape[1:]
        head_dim = w_k.shape[2]
        head_cols = w_q.shape[1] * head_dim
        assert chips == 4 and data_size == 4 and w_k.shape[0] == 1 and x_loc.shape[0] == 1
        seq = model_size * tok
        half = tok // 2
        heads = head_cols // head_dim
        wcol = width // (2 * data_size)
        krow = width // (model_size * data_size)
        cfg = (tok, width, head_cols, head_dim, chips, data_size)
        vm = pltpu.VMEM
        dma = pltpu.SemaphoreType.DMA
        pieces = 4
        scratch = [
            vm((seq, width), BF16), vm((seq, width), BF16), vm((width, head_cols), BF16), vm((head_cols, width), BF16),
            vm((width, 2 * head_dim), BF16), vm((heads * width, head_dim), BF16), vm((heads * width, head_dim), F32),
            vm((seq, head_cols), BF16), vm((seq, 2 * head_dim), BF16), vm((seq, head_cols), BF16),
            vm((heads, seq, seq), F32), vm((heads, seq, seq), BF16), vm((seq, head_cols), BF16), vm((seq, head_cols), BF16),
            vm((seq, 2 * head_dim), BF16),
            vm((model_size, tok, width), F32), vm((chips, tok, width), F32), vm((2, 3, pieces, half, width // pieces), F32),
            vm((model_size, tok, 2 * head_dim), F32), vm((chips, tok, 2 * head_dim), F32), vm((2, 3, half, 2 * head_dim), F32),
            vm((2, 2 * data_size, head_cols, wcol), F32), vm((2, 2, 3, head_cols, wcol), F32),
            vm((data_size, krow, 2 * head_dim), F32), vm((3, krow, 2 * head_dim), F32),
            dma((20,)), dma((4, 14)), dma((4, 16)), dma((chips,)), dma((chips,)), dma((2, 3, pieces)), dma((2, 3, pieces)),
            dma((chips,)), dma((chips,)), dma((2, 3)), dma((2, 3)), dma((2, 2, 3)), dma((2, 2, 3)), dma((3,)), dma((3,)),
        ]
        anyspec = pl.BlockSpec(memory_space=pl.ANY)
        vspec = pl.BlockSpec(memory_space=pltpu.VMEM)
        shapes = (jax.ShapeDtypeStruct((tok, width), BF16), jax.ShapeDtypeStruct((heads * 2 * wcol, head_dim), F32),
                  jax.ShapeDtypeStruct((krow, head_dim), F32), jax.ShapeDtypeStruct((krow, head_dim), F32),
                  jax.ShapeDtypeStruct((head_cols, 2 * wcol), F32))
        outs = pl.pallas_call(
            functools.partial(body, cfg),
            out_shape=shapes,
            in_specs=[anyspec] * 6,
            out_specs=(vspec,) * 5,
            scratch_shapes=scratch,
            compiler_params=pltpu.CompilerParams(collective_id=0, has_side_effects=True, vmem_limit_bytes=VMEM_LIMIT),
            name='attn_bwd',
        )(x_loc[0], dy_loc[0], w_q.reshape(width * heads, head_dim), w_o.reshape(head_cols, width), w_k[0], w_v[0])
        dx, dwq, dwk, dwv, dwo = pl.pallas_call(
            copy_out,
            out_shape=shapes,
            in_specs=[vspec] * 5,
            out_specs=(anyspec,) * 5,
            scratch_shapes=[dma((5,))],
            compiler_params=pltpu.CompilerParams(vmem_limit_bytes=4 * 1024 * 1024),
            name='copy_out',
        )(*outs)
        return (dx[None], dwq.reshape(2 * wcol, heads, head_dim), dwk, dwv, dwo.reshape(heads, head_dim, 2 * wcol))

    kv_rows = P(('pod', 'model', 'data'), None)
    return jax.shard_map(device_step, mesh=mesh,
                         in_specs=(tok_spec, tok_spec, P(None, 'model', None), P(), P(), P('model', None, None)),
                         out_specs=(tok_spec, P(('pod', 'data'), 'model', None), kv_rows, kv_rows, P(('pod', 'model'), None, 'data')),
                         check_vma=False)
```

```python
import functools

import jax
import jax.numpy as jnp
from jax import lax
from jax.experimental import pallas as pl
from jax.experimental.pallas import tpu as pltpu
from jax.sharding import PartitionSpec as P

F32 = jnp.float32
BF16 = jnp.bfloat16
NN = (((1,), (0,)), ((), ()))
NT = (((1,), (1,)), ((), ()))
TN = (((0,), (0,)), ((), ()))


def dot(a, b, dims):
    return lax.dot_general(a, b, dims, preferred_element_type=F32)


def body(cfg, x_hbm, dy_hbm, wq_hbm, wo_hbm, wk_hbm, wv_hbm,
         dx_ref, dwq_ref, dwk_ref, dwv_ref, dwo_ref,
         xf, yf, wq, wo, wkv, wq2, wq2f, qf, kv, of, prob, dsf, dqf, dof, kvb,
         dxp, dxr, xr, kvp, kvr, kr, dwa, yr, wkp, wkr,
         load_sem, ag_s, ag_r, dd_s, dd_r, xr_s, xr_r, kd_s, kd_r, kr_s, kr_r, yr_s, yr_r, wk_s, wk_r):
    tok, width, head_cols, head_dim, chips, rows = cfg
    half = tok // 2
    chunk = 2 * tok
    seq = chips * chunk
    heads = head_cols // head_dim
    wcol = width // (2 * rows)
    pieces = 4
    pcol = width // pieces
    hcol = width // 2
    scale = head_dim ** -0.5

    me = lax.axis_index('model')
    cx = me // 2
    cc = me % 2
    cp = 1 - cc
    xright = (cx + 1) % chips
    xleft = (cx + chips - 1) % chips
    xfar = (cx + 2) % chips
    my = lax.axis_index('data')
    yup = (my + 1) % rows
    ydn = (my + rows - 1) % rows
    yfar = (my + 2) % rows
    to_r = {'model': xright * 2 + cc}
    to_l = {'model': xleft * 2 + cc}
    to_p = {'model': cx * 2 + cp}
    to_u = {'data': yup}
    to_d = {'data': ydn}
    to_f = {'data': yfar}

    def rcopy(src, dst, ssem, rsem, dev):
        return pltpu.make_async_remote_copy(src_ref=src, dst_ref=dst, send_sem=ssem, recv_sem=rsem,
                                            device_id=dev, device_id_type=pl.DeviceIdType.MESH)

    def piece(arr, xc, core, h):
        r = pl.ds((xc * 2 + core) * tok + h * half, half)
        if arr == 0:
            return xf.at[r, :]
        if arr == 3:
            return kvb.at[r, :]
        return yf.at[r, pl.ds((arr - 1) * hcol, hcol)]

    def ag_copy(arr, idx, xc, core, h, dev):
        p = piece(arr, xc, core, h)
        return rcopy(p, p, ag_s.at[arr, idx], ag_r.at[arr, (xc * 2 + core) * 2 + h], dev)

    def ag_first(arr):
        return [ag_copy(arr, 0, cx, cc, 0, to_r), ag_copy(arr, 2, cx, cc, 1, to_l),
                ag_copy(arr, 4, cx, cc, 0, to_p), ag_copy(arr, 5, cx, cc, 1, to_p)]

    def ag_second(arr):
        return [ag_copy(arr, 1, cx, cc, 1, to_r), ag_copy(arr, 3, cx, cc, 0, to_l)]

    def ag_own(arr):
        return ag_first(arr) + ag_second(arr)

    def ag_relay(arr):
        return [ag_copy(arr, 6, xleft, cc, 0, to_r), ag_copy(arr, 7, xright, cc, 1, to_l)]

    def ag_cross(arr, idx, xc, h):
        return ag_copy(arr, idx, xc, cc, h, to_p)

    def ag_all_sends(arr):
        out = ag_own(arr) + ag_relay(arr)
        for idx, xc, h in ((8, xleft, 0), (9, xleft, 1), (10, xright, 0), (11, xright, 1), (12, xfar, 0), (13, xfar, 1)):
            out.append(ag_cross(arr, idx, xc, h))
        return out

    def ag_wait(arr, xc, core, h):
        p = piece(arr, xc, core, h)
        rcopy(p, p, ag_s.at[arr, 0], ag_r.at[arr, (xc * 2 + core) * 2 + h], to_p).wait_recv()

    def ag_stage1(arr):
        relays = ag_relay(arr)
        ag_wait(arr, xleft, cc, 0)
        relays[0].start()
        ag_wait(arr, xright, cc, 1)
        relays[1].start()
        ag_cross(arr, 8, xleft, 0).start()
        ag_cross(arr, 11, xright, 1).start()

    def ag_stage2(arr):
        ag_wait(arr, xright, cc, 0)
        ag_cross(arr, 10, xright, 0).start()
        ag_wait(arr, xleft, cc, 1)
        ag_cross(arr, 9, xleft, 1).start()

    def ag_stage3(arr):
        ag_wait(arr, xfar, cc, 0)
        ag_cross(arr, 12, xfar, 0).start()
        ag_wait(arr, xfar, cc, 1)
        ag_cross(arr, 13, xfar, 1).start()

    def ag_partner(arr, xc):
        ag_wait(arr, xc, cp, 0)
        ag_wait(arr, xc, cp, 1)

    def dd_copy(xc):
        return rcopy(dxp.at[xc * 2 + cp], dxr.at[xc], dd_s.at[xc], dd_r.at[xc], to_p)

    def dd_add(xc):
        dd_copy(xc).wait_recv()
        blk = xc * 2 + cc
        dxp[blk] = dxp[blk] + dxr[xc]

    def kd_copy(xc):
        return rcopy(kvp.at[xc * 2 + cp], kvr.at[xc], kd_s.at[xc], kd_r.at[xc], to_p)

    def xpart(xc, h, cl):
        return dxp.at[xc * 2 + cc, pl.ds(h * half, half), pl.ds(cl * pcol, pcol)]

    def kpart(xc, h):
        return kvp.at[xc * 2 + cc, pl.ds(h * half, half), :]

    def ring_src(kind, side):
        if kind == 0:
            return (xright, 1) if side == 0 else (xleft, 0)
        if kind == 1:
            return (xfar, 0) if side == 0 else (xfar, 1)
        return (xright, 0) if side == 0 else (xleft, 1)

    def x_copy(side, kind, cl):
        xc, h = ring_src(kind, side)
        return rcopy(xpart(xc, h, cl), xr.at[side, kind, cl], xr_s.at[side, kind, cl], xr_r.at[side, kind, cl],
                     to_r if side == 0 else to_l)

    def k_copy(side, kind):
        xc, h = ring_src(kind, side)
        return rcopy(kpart(xc, h), kr.at[side, kind], kr_s.at[side, kind], kr_r.at[side, kind],
                     to_r if side == 0 else to_l)

    def x_pass(cl):
        for side in range(2):
            x_copy(side, 1, cl).wait_recv()
            xc, h = ring_src(2, side)
            ref = xpart(xc, h, cl)
            ref[...] = ref[...] + xr[side, 1, cl]
            x_copy(side, 2, cl).start()

    def k_pass():
        for side in range(2):
            k_copy(side, 1).wait_recv()
            xc, h = ring_src(2, side)
            ref = kpart(xc, h)
            ref[...] = ref[...] + kr[side, 1]
            k_copy(side, 2).start()

    order = ((yfar, 0), (yfar, 1), (yup, 1), (ydn, 0), (yup, 0), (ydn, 1), (my, 0), (my, 1))

    def y_blk(w, kind, side):
        pos = {(1, 0): 0, (1, 1): 1, (0, 0): 2, (0, 1): 3, (2, 0): 4, (2, 1): 5, (3, 0): 6, (3, 1): 7}[kind, side]
        if w == 0:
            return pos
        return order[pos][0] * 2 + order[pos][1]

    def y_copy(w, side, kind):
        return rcopy(dwa.at[w, y_blk(w, kind, side)], yr.at[w, side, kind], yr_s.at[w, side, kind], yr_r.at[w, side, kind],
                     to_u if side == 0 else to_d)

    def dw_block(w, kind, side):
        blk = y_blk(w, kind, side)
        if w == 0:
            dwa[0, blk] = dot(of[...], yf[:, blk * wcol:(blk + 1) * wcol], TN)
        else:
            dwa[1, blk] = dot(dqf[...], xf[:, pl.ds(pl.multiple_of(blk * wcol, wcol), wcol)], TN)

    def y_first(w):
        for kind in (1, 0):
            for side in range(2):
                dw_block(w, kind, side)
                y_copy(w, side, kind).start()

    def y_rest(w):
        for kind in (2, 3):
            for side in range(2):
                dw_block(w, kind, side)

    def y_pass(w):
        for side in range(2):
            y_copy(w, side, 1).wait_recv()
            blk = y_blk(w, 2, side)
            dwa[w, blk] = dwa[w, blk] + yr[w, side, 1]
            y_copy(w, side, 2).start()

    def y_final(w):
        for side in range(2):
            y_copy(w, side, 0).wait_recv()
            y_copy(w, side, 2).wait_recv()
        first = dwa[w, y_blk(w, 3, 0)] + yr[w, 1, 0] + yr[w, 0, 2]
        second = dwa[w, y_blk(w, 3, 1)] + yr[w, 0, 0] + yr[w, 1, 2]
        return first, second

    own_rows = pl.ds(me * tok, tok)
    loads = [pltpu.make_async_copy(x_hbm, xf.at[own_rows, :], load_sem.at[0]),
             pltpu.make_async_copy(wq_hbm, wq2, load_sem.at[1]),
             pltpu.make_async_copy(wk_hbm, wkv.at[:, pl.ds(0, head_dim)], load_sem.at[2]),
             pltpu.make_async_copy(wv_hbm, wkv.at[:, pl.ds(head_dim, head_dim)], load_sem.at[3])]
    for pos, (dest, part) in enumerate(order):
        src = pl.ds(pl.multiple_of((dest * 2 + part) * wcol, wcol), wcol)
        dst = pl.ds(pos * wcol, wcol)
        loads.append(pltpu.make_async_copy(dy_hbm.at[:, src], yf.at[own_rows, dst], load_sem.at[4 + pos]))
        loads.append(pltpu.make_async_copy(wo_hbm.at[:, src], wo.at[:, dst], load_sem.at[12 + pos]))
    for cp_ in loads:
        cp_.start()
    barrier = pltpu.get_barrier_semaphore()
    for dev in (to_r, to_l, to_p, to_u, to_d, to_f):
        pl.semaphore_signal(barrier, inc=1, device_id=dev, device_id_type=pl.DeviceIdType.MESH)
    with jax.named_scope('barrier'):
        pl.semaphore_wait(barrier, 6)
    loads[0].wait()
    for cp_ in ag_own(0):
        cp_.start()
    with jax.named_scope('loadw'):
        for cp_ in loads[1:]:
            cp_.wait()
        step = 2 * width // 8

        @pl.loop(0, 8)
        def _(b):
            r2 = pl.ds(pl.multiple_of(b * step, step), step)
            wq2f[r2, :] = wq2[r2, :].astype(F32)
            r1 = pl.ds(pl.multiple_of(b * (step // 2), step // 2), step // 2)
            for h in range(heads):
                wq[r1, h * head_dim:(h + 1) * head_dim] = wq2f[pl.ds(b * step + h, step // 2, stride=heads), :].astype(BF16)

    def chunk_of(s):
        return (cx + s + s // 2 - 2 * (s // 3)) % chips

    @pl.loop(0, chips)
    def _(s):
        @pl.when(s == 0)
        def _():
            ag_partner(0, cx)

        @pl.when(s == 1)
        def _():
            ag_stage1(0)
            for cp_ in ag_own(1):
                cp_.start()
            for cp_ in ag_own(2):
                cp_.start()
            ag_stage2(0)
            ag_partner(0, xright)

        @pl.when(s == 2)
        def _():
            ag_partner(0, xleft)

        @pl.when(s == 3)
        def _():
            ag_stage3(0)
            ag_partner(0, xfar)

        r = pl.ds(chunk_of(s) * chunk, chunk)
        xc = xf[r, :]
        qf[r, :] = dot(xc, wq[...], NN).astype(BF16)
        kv[r, :] = dot(xc, wkv[...], NN).astype(BF16)

    @pl.loop(0, chips)
    def _(s):
        @pl.when(s == 2)
        def _():
            ag_stage1(1)

        @pl.when(s == 3)
        def _():
            ag_stage2(1)

        i = chunk_of(s)
        r = pl.ds(i * chunk, chunk)
        row_id = lax.broadcasted_iota(jnp.int32, (chunk, seq), 0) + i * chunk
        keep = row_id >= lax.broadcasted_iota(jnp.int32, (chunk, seq), 1)
        for h in range(heads):
            hc = pl.ds(h * head_dim, head_dim)
            sc = dot(qf[r, hc], kv[:, 0:head_dim], NT) * scale
            sc = jnp.where(keep, sc, -jnp.inf)
            ex = jnp.exp(sc - jnp.max(sc, axis=-1, keepdims=True))
            pr = ex * (1.0 / jnp.sum(ex, axis=-1, keepdims=True))
            prob[h, r, :] = pr
            of[r, hc] = dot(pr.astype(BF16), kv[:, head_dim:], NN).astype(BF16)

    ag_stage1(2)
    ag_partner(1, cx)
    ag_partner(2, cx)

    @pl.loop(0, chips)
    def _(s):
        @pl.when(s == 1)
        def _():
            with jax.named_scope('b1'):
                ag_stage2(2)
                for arr in (1, 2):
                    ag_partner(arr, xright)

        @pl.when(s == 2)
        def _():
            with jax.named_scope('b2'):
                ag_stage3(1)
                for arr in (1, 2):
                    ag_partner(arr, xleft)

        @pl.when(s == 3)
        def _():
            with jax.named_scope('b3'):
                dd_add(xright)
                for cl in range(2):
                    x_copy(0, 0, cl).start()
                ag_stage3(2)
                ag_partner(1, xfar)
            with jax.named_scope('b3y'):
                y_first(0)
            with jax.named_scope('b3w'):
                dd_add(xleft)
                for cl in range(2):
                    x_copy(1, 0, cl).start()
                ag_partner(2, xfar)

        with jax.named_scope('b_comp'):
            i = chunk_of(s)
            r = pl.ds(i * chunk, chunk)
            oc = of[r, :]
            do = dot(yf[r, :], wo[...], NT).astype(BF16)
            dof[r, :] = do
            od = do.astype(F32) * oc.astype(F32)
            for h in range(heads):
                hs = slice(h * head_dim, (h + 1) * head_dim)
                dp = dot(do[:, hs], kv[:, head_dim:], NT)
                ds = (prob[h, r, :] * (dp - jnp.sum(od[:, hs], axis=-1, keepdims=True))).astype(BF16)
                dsf[h, r, :] = ds
                dqf[r, hs] = (dot(ds, kv[:, 0:head_dim], NN) * scale).astype(BF16)
            dq = dqf[r, :]
            for j in range(pieces):
                dxp[pl.ds(2 * i, 2), :, j * pcol:(j + 1) * pcol] = dot(dq, wq[j * pcol:(j + 1) * pcol, :], NT).reshape(2, tok, pcol)
        dd_copy(i).start()

    with jax.named_scope('t00_dkv'):
        for kc in range(chips):
            ks = slice(kc * chunk, (kc + 1) * chunk)
            qs = slice(kc * chunk, seq)
            dk = jnp.zeros((chunk, head_dim), F32)
            dv = jnp.zeros((chunk, head_dim), F32)
            for h in range(heads):
                hs = slice(h * head_dim, (h + 1) * head_dim)
                dk = dk + dot(dsf[h, qs, ks], qf[qs, hs], TN)
                dv = dv + dot(prob[h, qs, ks].astype(BF16), dof[qs, hs], TN)
            kvp[2 * kc:2 * kc + 2, :, 0:head_dim] = (dk * scale).reshape(2, tok, head_dim)
            kvp[2 * kc:2 * kc + 2, :, head_dim:] = dv.reshape(2, tok, head_dim)
            if kc == 1:
                dd_add(xfar)
                for side in range(2):
                    x_copy(side, 1, 0).start()
        for xc in range(chips):
            kd_copy(xc).start()

    def x_send(kind, cl):
        for side in range(2):
            x_copy(side, kind, cl).start()

    own = cx * 2 + cc

    def dx_final(cl):
        cols = slice(cl * pcol, (cl + 1) * pcol)
        kv_term = dot(kvb[own_rows, :], wkv[cols, :], NT)
        for side in range(2):
            x_copy(side, 0, cl).wait_recv()
            x_copy(side, 2, cl).wait_recv()
        dx_ref[0:half, cols] = (kv_term[0:half] + dxp[own, 0:half, cols] + xr[1, 0, cl] + xr[0, 2, cl]).astype(BF16)
        dx_ref[half:, cols] = (kv_term[half:] + dxp[own, half:, cols] + xr[0, 0, cl] + xr[1, 2, cl]).astype(BF16)

    with jax.named_scope('t02_y1'):
        y_first(1)
    with jax.named_scope('t03_kd'):
        for xc in range(chips):
            kd_copy(xc).wait_recv()
            blk = xc * 2 + cc
            kvp[blk] = kvp[blk] + kvr[xc]
        for kind in (1, 0):
            for side in range(2):
                k_copy(side, kind).start()
        x_send(0, 2)
    with jax.named_scope('t04_y0'):
        y_rest(0)
        y_pass(0)
    with jax.named_scope('t05_y1r'):
        y_rest(1)
        dd_add(cx)
    with jax.named_scope('t06_kpass'):
        k_pass()
        x_send(1, 1)
    with jax.named_scope('t08_xp0'):
        x_pass(0)
    with jax.named_scope('t07_kfin'):
        for side in range(2):
            k_copy(side, 0).wait_recv()
            k_copy(side, 2).wait_recv()
        kvb[pl.ds(me * tok, half), :] = (kvp[own, 0:half, :] + kr[1, 0] + kr[0, 2]).astype(BF16)
        kvb[pl.ds(me * tok + half, half), :] = (kvp[own, half:, :] + kr[0, 0] + kr[1, 2]).astype(BF16)
        for cp_ in ag_own(3):
            cp_.start()
        x_send(1, 2)
    with jax.named_scope('t09_xp1'):
        x_pass(1)
    with jax.named_scope('t09_y1'):
        y_pass(1)
    with jax.named_scope('t10_ag'):
        ag_stage1(3)
        x_send(1, 3)
        x_send(0, 3)
        ag_stage2(3)
    with jax.named_scope('t11_ag'):
        ag_stage3(3)
        for xc in (cx, xright, xleft, xfar):
            ag_partner(3, xc)
    mrow = width // (2 * chips)
    krow = mrow // rows
    with jax.named_scope('t12_wk'):
        part = dot(xf[:, pl.ds(pl.multiple_of(me * mrow, mrow), mrow)], kvb[...], TN)
        wkp[...] = part.reshape(rows, krow, 2 * head_dim)

    def wk_copy(idx, blk, dev):
        return rcopy(wkp.at[blk], wkr.at[idx], wk_s.at[idx], wk_r.at[idx], dev)

    wk_copies = [wk_copy(0, yup, to_u), wk_copy(1, ydn, to_d), wk_copy(2, yfar, to_f)]
    for cp_ in wk_copies:
        cp_.start()
    with jax.named_scope('t14_xp2'):
        x_pass(2)
    with jax.named_scope('t15_y0f'):
        first, second = y_final(0)
        dwo_ref[:, 0:wcol] = first
        dwo_ref[:, wcol:] = second
        dx_final(0)
    with jax.named_scope('t16_xp3'):
        x_pass(3)
    with jax.named_scope('t17_y1f'):
        for idx, val in enumerate(y_final(1)):
            val = val.T
            for h in range(heads):
                dwq_ref[pl.ds(idx * wcol * heads + h, wcol, stride=heads), :] = val[:, h * head_dim:(h + 1) * head_dim]
        for cp_ in wk_copies:
            cp_.wait_recv()
        wk_sum = wkp[my] + wkr[0] + wkr[1] + wkr[2]
        dwk_ref[...] = wk_sum[:, 0:head_dim]
        dwv_ref[...] = wk_sum[:, head_dim:]
    for cl in range(1, pieces):
        with jax.named_scope('t18_dx%d' % cl):
            dx_final(cl)

    with jax.named_scope('t19_sends'):
        for arr in range(4):
            for cp_ in ag_all_sends(arr):
                cp_.wait_send()
        for xc in range(chips):
            dd_copy(xc).wait_send()
            kd_copy(xc).wait_send()
        for side in range(2):
            for kind in range(3):
                k_copy(side, kind).wait_send()
                for cl in range(pieces):
                    x_copy(side, kind, cl).wait_send()
                for w in range(2):
                    y_copy(w, side, kind).wait_send()
        for cp_ in wk_copies:
            cp_.wait_send()


def copy_out(*refs):
    n = (len(refs) - 1) // 2
    sem = refs[-1]
    copies = [pltpu.make_async_copy(refs[k], refs[n + k], sem.at[k]) for k in range(n)]
    for cp_ in copies:
        cp_.start()
    for cp_ in copies:
        cp_.wait()


VMEM_LIMIT = 60 * 1000 * 1000


def solution(mesh):
    model_size = mesh.shape['model']
    data_size = mesh.shape['data']
    tok_spec = P(('pod', 'data'), 'model', None)
    chips = model_size // 2

    def device_step(x_loc, dy_loc, w_q, w_k, w_v, w_o):
        tok, width = x_loc.shape[1:]
        head_dim = w_k.shape[2]
        head_cols = w_q.shape[1] * head_dim
        assert chips == 4 and data_size == 4 and w_k.shape[0] == 1 and x_loc.shape[0] == 1
        seq = model_size * tok
        half = tok // 2
        heads = head_cols // head_dim
        wcol = width // (2 * data_size)
        krow = width // (model_size * data_size)
        cfg = (tok, width, head_cols, head_dim, chips, data_size)
        vm = pltpu.VMEM
        dma = pltpu.SemaphoreType.DMA
        pieces = 4
        scratch = [
            vm((seq, width), BF16), vm((seq, width), BF16), vm((width, head_cols), BF16), vm((head_cols, width), BF16),
            vm((width, 2 * head_dim), BF16), vm((heads * width, head_dim), BF16), vm((heads * width, head_dim), F32),
            vm((seq, head_cols), BF16), vm((seq, 2 * head_dim), BF16), vm((seq, head_cols), BF16),
            vm((heads, seq, seq), F32), vm((heads, seq, seq), BF16), vm((seq, head_cols), BF16), vm((seq, head_cols), BF16),
            vm((seq, 2 * head_dim), BF16),
            vm((model_size, tok, width), F32), vm((chips, tok, width), F32), vm((2, 3, pieces, half, width // pieces), F32),
            vm((model_size, tok, 2 * head_dim), F32), vm((chips, tok, 2 * head_dim), F32), vm((2, 3, half, 2 * head_dim), F32),
            vm((2, 2 * data_size, head_cols, wcol), F32), vm((2, 2, 3, head_cols, wcol), F32),
            vm((data_size, krow, 2 * head_dim), F32), vm((3, krow, 2 * head_dim), F32),
            dma((20,)), dma((4, 14)), dma((4, 16)), dma((chips,)), dma((chips,)), dma((2, 3, pieces)), dma((2, 3, pieces)),
            dma((chips,)), dma((chips,)), dma((2, 3)), dma((2, 3)), dma((2, 2, 3)), dma((2, 2, 3)), dma((3,)), dma((3,)),
        ]
        anyspec = pl.BlockSpec(memory_space=pl.ANY)
        vspec = pl.BlockSpec(memory_space=pltpu.VMEM)
        shapes = (jax.ShapeDtypeStruct((tok, width), BF16), jax.ShapeDtypeStruct((heads * 2 * wcol, head_dim), F32),
                  jax.ShapeDtypeStruct((krow, head_dim), F32), jax.ShapeDtypeStruct((krow, head_dim), F32),
                  jax.ShapeDtypeStruct((head_cols, 2 * wcol), F32))
        outs = pl.pallas_call(
            functools.partial(body, cfg),
            out_shape=tuple(pltpu.VMEM(a.shape, a.dtype) for a in shapes),
            in_specs=[anyspec] * 6,
            out_specs=(vspec,) * 5,
            scratch_shapes=scratch,
            compiler_params=pltpu.CompilerParams(collective_id=0, has_side_effects=True, vmem_limit_bytes=VMEM_LIMIT),
            name='attn_bwd',
        )(x_loc[0], dy_loc[0], w_q.reshape(width * heads, head_dim), w_o.reshape(head_cols, width), w_k[0], w_v[0])
        dx, dwq, dwk, dwv, dwo = pl.pallas_call(
            copy_out,
            out_shape=shapes,
            in_specs=[vspec] * 5,
            out_specs=(anyspec,) * 5,
            scratch_shapes=[dma((5,))],
            compiler_params=pltpu.CompilerParams(vmem_limit_bytes=4 * 1024 * 1024),
            name='copy_out',
        )(*outs)
        return (dx[None], dwq.reshape(2 * wcol, heads, head_dim), dwk, dwv, dwo.reshape(heads, head_dim, 2 * wcol))

    kv_rows = P(('pod', 'model', 'data'), None)
    return jax.shard_map(device_step, mesh=mesh,
                         in_specs=(tok_spec, tok_spec, P(None, 'model', None), P(), P(), P('model', None, None)),
                         out_specs=(tok_spec, P(('pod', 'data'), 'model', None), kv_rows, kv_rows, P(('pod', 'model'), None, 'data')),
                         check_vma=False)
```

```python
import functools

import jax
import jax.numpy as jnp
from jax import lax
from jax.experimental import pallas as pl
from jax.experimental.pallas import tpu as pltpu
from jax.sharding import PartitionSpec as P

F32 = jnp.float32
BF16 = jnp.bfloat16
NN = (((1,), (0,)), ((), ()))
NT = (((1,), (1,)), ((), ()))
TN = (((0,), (0,)), ((), ()))


def dot(a, b, dims):
    return lax.dot_general(a, b, dims, preferred_element_type=F32)


def body(cfg, x_hbm, dy_hbm, wq_hbm, wo_hbm, wk_hbm, wv_hbm,
         dx_out, dwq_out, dwk_out, dwv_out, dwo_out,
         xf, yf, wqs, wo, wkv, wq2, wq2f, qf, kv, of, prob, dsf, dqf, dof, kvb, dqa,
         kvp, kvr, kr, dwa, yr, wkp, wkr, dx_ref, dwq_ref, dwk_ref, dwv_ref, dwo_ref,
         load_sem, out_sem, ag_s, ag_r, wy_s, wy_r, wd_s, wd_r, dq_s, dq_r,
         kd_s, kd_r, kr_s, kr_r, yr_s, yr_r, wk_s, wk_r):
    tok, width, head_cols, head_dim, chips, rows = cfg
    half = tok // 2
    chunk = 2 * tok
    seq = chips * chunk
    heads = head_cols // head_dim
    wcol = width // (2 * rows)
    hcol = width // 2
    qrow = width // 8
    scale = head_dim ** -0.5

    me = lax.axis_index('model')
    cx = me // 2
    cc = me % 2
    cp = 1 - cc
    xright = (cx + 1) % chips
    xleft = (cx + chips - 1) % chips
    xfar = (cx + 2) % chips
    my = lax.axis_index('data')
    yup = (my + 1) % rows
    ydn = (my + rows - 1) % rows
    yfar = (my + 2) % rows
    to_r = {'model': xright * 2 + cc}
    to_l = {'model': xleft * 2 + cc}
    to_p = {'model': cx * 2 + cp}
    to_u = {'data': yup}
    to_d = {'data': ydn}
    to_f = {'data': yfar}

    def rcopy(src, dst, ssem, rsem, dev):
        return pltpu.make_async_remote_copy(src_ref=src, dst_ref=dst, send_sem=ssem, recv_sem=rsem,
                                            device_id=dev, device_id_type=pl.DeviceIdType.MESH)

    def piece(arr, xc, core, h, base):
        r = pl.ds((xc * 2 + core) * tok + h * half, half)
        if arr == 0:
            return xf.at[r, :]
        if arr == 3:
            return kvb.at[r, :]
        slot = (xc + chips - base) % chips
        if arr == 4:
            return wqs.at[core, slot, pl.ds(my * qrow + h * (qrow // 2), qrow // 2), :]
        if arr == 5:
            return wqs.at[core, slot, pl.ds(hcol + h * (hcol // 2), hcol // 2), :]
        return yf.at[r, pl.ds((arr - 1) * hcol, hcol)]

    def ag_copy(arr, idx, xc, core, h, dev):
        base = {'r': xright, 'l': xleft, 'p': cx}[dev]
        return rcopy(piece(arr, xc, core, h, cx), piece(arr, xc, core, h, base), ag_s.at[arr, idx],
                     ag_r.at[arr, (xc * 2 + core) * 2 + h], {'r': to_r, 'l': to_l, 'p': to_p}[dev])

    def ag_ring_first(arr):
        return [ag_copy(arr, 0, cx, cc, 0, 'r'), ag_copy(arr, 2, cx, cc, 1, 'l')]

    def ag_first(arr):
        return ag_ring_first(arr) + [ag_copy(arr, 4, cx, cc, 0, 'p'), ag_copy(arr, 5, cx, cc, 1, 'p')]

    def ag_second(arr):
        return [ag_copy(arr, 1, cx, cc, 1, 'r'), ag_copy(arr, 3, cx, cc, 0, 'l')]

    def ag_own(arr):
        return ag_first(arr) + ag_second(arr)

    def ag_relay(arr):
        return [ag_copy(arr, 6, xleft, cc, 0, 'r'), ag_copy(arr, 7, xright, cc, 1, 'l')]

    def ag_cross(arr, idx, xc, h):
        return ag_copy(arr, idx, xc, cc, h, 'p')

    def ag_all_sends(arr):
        out = ag_own(arr) + ag_relay(arr)
        for idx, xc, h in ((8, xleft, 0), (9, xleft, 1), (10, xright, 0), (11, xright, 1), (12, xfar, 0), (13, xfar, 1)):
            out.append(ag_cross(arr, idx, xc, h))
        return out

    def ag_wait(arr, xc, core, h):
        p = piece(arr, xc, core, h, cx)
        rcopy(p, p, ag_s.at[arr, 0], ag_r.at[arr, (xc * 2 + core) * 2 + h], to_p).wait_recv()

    def ag_relays(arr):
        relays = ag_relay(arr)
        ag_wait(arr, xleft, cc, 0)
        relays[0].start()
        ag_wait(arr, xright, cc, 1)
        relays[1].start()

    def ag_stage1(arr):
        ag_relays(arr)
        ag_cross(arr, 8, xleft, 0).start()
        ag_cross(arr, 11, xright, 1).start()

    def ag_stage2(arr):
        ag_wait(arr, xright, cc, 0)
        ag_cross(arr, 10, xright, 0).start()
        ag_wait(arr, xleft, cc, 1)
        ag_cross(arr, 9, xleft, 1).start()

    def ag_stage3(arr):
        ag_wait(arr, xfar, cc, 0)
        ag_cross(arr, 12, xfar, 0).start()
        ag_wait(arr, xfar, cc, 1)
        ag_cross(arr, 13, xfar, 1).start()

    def ag_partner(arr, xc):
        ag_wait(arr, xc, cp, 0)
        ag_wait(arr, xc, cp, 1)

    def wy_copy(idx, q, h, dev):
        p = wqs.at[cc, pl.ds(1, chips - 1), pl.ds(q * qrow + h * (qrow // 2), qrow // 2), :]
        return rcopy(p, p, wy_s.at[idx], wy_r.at[q, h], dev)

    wy_own = [wy_copy(0, my, 0, to_u), wy_copy(1, my, 1, to_d), wy_copy(2, my, 1, to_u), wy_copy(3, my, 0, to_d)]
    wy_relay = [wy_copy(4, ydn, 0, to_u), wy_copy(5, yup, 1, to_d)]

    def wy_pass():
        wy_copy(0, ydn, 0, to_u).wait_recv()
        wy_relay[0].start()
        wy_copy(0, yup, 1, to_u).wait_recv()
        wy_relay[1].start()

    wd_own = rcopy(wqs.at[cc, 0, pl.ds(0, hcol), :], wqs.at[cc, 0, pl.ds(0, hcol), :], wd_s.at[0], wd_r.at[0], to_p)
    wd_rest = rcopy(wqs.at[cc, pl.ds(1, chips - 1), pl.ds(0, hcol), :], wqs.at[cc, pl.ds(1, chips - 1), pl.ds(0, hcol), :],
                    wd_s.at[1], wd_r.at[1], to_p)

    def wy_end():
        for q, h in ((ydn, 1), (yup, 0), (yfar, 0), (yfar, 1)):
            wy_copy(0, q, h, to_u).wait_recv()
        wd_rest.start()

    def dq_copy(s, xc, core):
        return rcopy(dqf.at[pl.ds((xc * 2 + core) * tok, tok), :], dqa.at[(cx + chips - xc) % chips, cc],
                     dq_s.at[s, core], dq_r.at[(cx + chips - xc) % chips, cc], {'model': xc * 2 + core})

    def dq_wait(slot, core):
        rcopy(dqa.at[slot, core], dqa.at[slot, core], dq_s.at[0, 0], dq_r.at[slot, core], to_p).wait_recv()

    def kd_copy(xc):
        return rcopy(kvp.at[xc * 2 + cp], kvr.at[xc], kd_s.at[xc], kd_r.at[xc], to_p)

    def kpart(xc, h):
        return kvp.at[xc * 2 + cc, pl.ds(h * half, half), :]

    def ring_src(kind, side):
        if kind == 0:
            return (xright, 1) if side == 0 else (xleft, 0)
        if kind == 1:
            return (xfar, 0) if side == 0 else (xfar, 1)
        return (xright, 0) if side == 0 else (xleft, 1)

    def k_copy(side, kind):
        xc, h = ring_src(kind, side)
        return rcopy(kpart(xc, h), kr.at[side, kind], kr_s.at[side, kind], kr_r.at[side, kind],
                     to_r if side == 0 else to_l)

    def k_pass():
        for side in range(2):
            k_copy(side, 1).wait_recv()
            xc, h = ring_src(2, side)
            ref = kpart(xc, h)
            ref[...] = ref[...] + kr[side, 1]
            k_copy(side, 2).start()

    order = ((yfar, 0), (yfar, 1), (yup, 1), (ydn, 0), (yup, 0), (ydn, 1), (my, 0), (my, 1))

    def y_blk(w, kind, side):
        pos = {(1, 0): 0, (1, 1): 1, (0, 0): 2, (0, 1): 3, (2, 0): 4, (2, 1): 5, (3, 0): 6, (3, 1): 7}[kind, side]
        if w == 0:
            return pos
        return order[pos][0] * 2 + order[pos][1]

    def y_copy(w, side, kind):
        return rcopy(dwa.at[w, y_blk(w, kind, side)], yr.at[w, side, kind], yr_s.at[w, side, kind], yr_r.at[w, side, kind],
                     to_u if side == 0 else to_d)

    def dw_block(w, kind, side):
        blk = y_blk(w, kind, side)
        if w == 0:
            dwa[0, blk] = dot(of[...], yf[:, blk * wcol:(blk + 1) * wcol], TN)
        else:
            dwa[1, blk] = dot(dqf[...], xf[:, pl.ds(pl.multiple_of(blk * wcol, wcol), wcol)], TN)

    def y_first(w):
        for kind in (1, 0):
            for side in range(2):
                dw_block(w, kind, side)
                y_copy(w, side, kind).start()

    def y_rest(w):
        for kind in (2, 3):
            for side in range(2):
                dw_block(w, kind, side)

    def y_pass(w):
        for side in range(2):
            y_copy(w, side, 1).wait_recv()
            blk = y_blk(w, 2, side)
            dwa[w, blk] = dwa[w, blk] + yr[w, side, 1]
            y_copy(w, side, 2).start()

    def y_final(w):
        for side in range(2):
            y_copy(w, side, 0).wait_recv()
            y_copy(w, side, 2).wait_recv()
        first = dwa[w, y_blk(w, 3, 0)] + yr[w, 1, 0] + yr[w, 0, 2]
        second = dwa[w, y_blk(w, 3, 1)] + yr[w, 0, 0] + yr[w, 1, 2]
        return first, second

    own_rows = pl.ds(me * tok, tok)
    loads = [pltpu.make_async_copy(x_hbm, xf.at[own_rows, :], load_sem.at[0]),
             pltpu.make_async_copy(wq_hbm, wq2, load_sem.at[1]),
             pltpu.make_async_copy(wk_hbm, wkv.at[:, pl.ds(0, head_dim)], load_sem.at[2]),
             pltpu.make_async_copy(wv_hbm, wkv.at[:, pl.ds(head_dim, head_dim)], load_sem.at[3])]
    for pos, (dest, part) in enumerate(order):
        src = pl.ds(pl.multiple_of((dest * 2 + part) * wcol, wcol), wcol)
        dst = pl.ds(pos * wcol, wcol)
        loads.append(pltpu.make_async_copy(dy_hbm.at[:, src], yf.at[own_rows, dst], load_sem.at[4 + pos]))
        loads.append(pltpu.make_async_copy(wo_hbm.at[:, src], wo.at[:, dst], load_sem.at[12 + pos]))
    for cp_ in loads:
        cp_.start()
    barrier = pltpu.get_barrier_semaphore()
    peers = [{'model': (me + k) % (2 * chips)} for k in range(1, 2 * chips)]
    for dev in peers + [to_u, to_d, to_f]:
        pl.semaphore_signal(barrier, inc=1, device_id=dev, device_id_type=pl.DeviceIdType.MESH)
    with jax.named_scope('barrier'):
        pl.semaphore_wait(barrier, 2 * chips + 2)
    loads[0].wait()
    for cp_ in ag_first(0):
        cp_.start()
    with jax.named_scope('loadw'):
        for cp_ in loads[1:]:
            cp_.wait()
        step = 2 * width // 8

        @pl.loop(0, 8)
        def _(b):
            r2 = pl.ds(pl.multiple_of(b * step, step), step)
            wq2f[r2, :] = wq2[r2, :].astype(F32)
            r1 = pl.ds(pl.multiple_of(b * (step // 2), step // 2), step // 2)
            for h in range(heads):
                wqs[cc, 0, r1, h * head_dim:(h + 1) * head_dim] = wq2f[pl.ds(b * step + h, step // 2, stride=heads), :].astype(BF16)

    for cp_ in ag_ring_first(4) + ag_second(4) + ag_second(0):
        cp_.start()
    wd_own.start()

    def chunk_of(s):
        return (cx + s + s // 2 - 2 * (s // 3)) % chips

    @pl.loop(0, chips)
    def _(s):
        @pl.when(s == 0)
        def _():
            ag_partner(0, cx)

        @pl.when(s == 1)
        def _():
            with jax.named_scope('q1'):
                ag_relays(4)
                ag_stage1(0)
                for cp_ in ag_own(1):
                    cp_.start()
                ag_stage2(0)
            with jax.named_scope('q1w'):
                for xc, h in ((xleft, 1), (xright, 0), (xfar, 0), (xfar, 1)):
                    ag_wait(4, xc, cc, h)
                for cp_ in wy_own:
                    cp_.start()
            ag_partner(0, xright)

        @pl.when(s == 2)
        def _():
            ag_partner(0, xleft)

        @pl.when(s == 3)
        def _():
            ag_stage3(0)
            ag_partner(0, xfar)

        r = pl.ds(chunk_of(s) * chunk, chunk)
        xc = xf[r, :]
        qf[r, :] = dot(xc, wqs[cc, 0], NN).astype(BF16)
        kv[r, :] = dot(xc, wkv[...], NN).astype(BF16)

    @pl.loop(0, chips)
    def _(s):
        @pl.when(s == 0)
        def _():
            with jax.named_scope('f0'):
                wy_pass()

        @pl.when(s == 1)
        def _():
            with jax.named_scope('f1'):
                ag_stage1(1)
                for cp_ in ag_own(2):
                    cp_.start()

        @pl.when(s == 2)
        def _():
            with jax.named_scope('f2'):
                ag_stage2(1)

        i = chunk_of(s)
        r = pl.ds(i * chunk, chunk)
        row_id = lax.broadcasted_iota(jnp.int32, (chunk, seq), 0) + i * chunk
        keep = row_id >= lax.broadcasted_iota(jnp.int32, (chunk, seq), 1)
        for h in range(heads):
            hc = pl.ds(h * head_dim, head_dim)
            sc = dot(qf[r, hc], kv[:, 0:head_dim], NT) * scale
            sc = jnp.where(keep, sc, -jnp.inf)
            ex = jnp.exp(sc - jnp.max(sc, axis=-1, keepdims=True))
            pr = ex * (1.0 / jnp.sum(ex, axis=-1, keepdims=True))
            prob[h, r, :] = pr
            of[r, hc] = dot(pr.astype(BF16), kv[:, head_dim:], NN).astype(BF16)

    with jax.named_scope('b0'):
        ag_stage3(1)
        ag_partner(1, cx)
        ag_partner(2, cx)

    @pl.loop(0, chips)
    def _(s):
        @pl.when(s == 1)
        def _():
            with jax.named_scope('b1'):
                for xc in (xright, xleft, xfar):
                    ag_partner(1, xc)
            with jax.named_scope('b1y'):
                y_first(0)
            with jax.named_scope('b1s'):
                ag_stage1(2)
                for cp_ in ag_first(5):
                    cp_.start()
                wy_end()
            with jax.named_scope('b1w'):
                ag_stage2(2)
                ag_partner(2, xright)

        @pl.when(s == 2)
        def _():
            with jax.named_scope('b2'):
                ag_stage3(2)
                ag_partner(2, xleft)

        @pl.when(s == 3)
        def _():
            with jax.named_scope('b3'):
                ag_partner(2, xfar)

        with jax.named_scope('b_comp'):
            i = chunk_of(s)
            r = pl.ds(i * chunk, chunk)
            oc = of[r, :]
            do = dot(yf[r, :], wo[...], NT).astype(BF16)
            dof[r, :] = do
            od = do.astype(F32) * oc.astype(F32)
            for h in range(heads):
                hs = slice(h * head_dim, (h + 1) * head_dim)
                dp = dot(do[:, hs], kv[:, head_dim:], NT)
                ds = (prob[h, r, :] * (dp - jnp.sum(od[:, hs], axis=-1, keepdims=True))).astype(BF16)
                dsf[h, r, :] = ds
                dqf[r, hs] = (dot(ds, kv[:, 0:head_dim], NN) * scale).astype(BF16)

        @pl.when(s == 0)
        def _():
            dqa[0, cc] = dqf[own_rows, :]
            dq_copy(0, cx, cp).start()

        @pl.when(s > 0)
        def _():
            for core in range(2):
                dq_copy(s, i, core).start()

    for cp_ in ag_second(5):
        cp_.start()
    with jax.named_scope('t00_y1'):
        y_first(1)

    with jax.named_scope('t00_dkv'):
        for kc in range(chips):
            ks = slice(kc * chunk, (kc + 1) * chunk)
            qs = slice(kc * chunk, seq)
            dk = jnp.zeros((chunk, head_dim), F32)
            dv = jnp.zeros((chunk, head_dim), F32)
            for h in range(heads):
                hs = slice(h * head_dim, (h + 1) * head_dim)
                dk = dk + dot(dsf[h, qs, ks], qf[qs, hs], TN)
                dv = dv + dot(prob[h, qs, ks].astype(BF16), dof[qs, hs], TN)
            kvp[2 * kc:2 * kc + 2, :, 0:head_dim] = (dk * scale).reshape(2, tok, head_dim)
            kvp[2 * kc:2 * kc + 2, :, head_dim:] = dv.reshape(2, tok, head_dim)
        for xc in range(chips):
            kd_copy(xc).start()

    own = cx * 2 + cc

    def dx_part(j):
        cols = slice(j * (hcol // 2), (j + 1) * (hcol // 2))
        acc = dot(kvb[own_rows, :], wkv[cols, :], NT)
        for slot in range(chips):
            for core in range(2):
                acc = acc + dot(dqa[slot, core], wqs[core, slot, cols, :], NT)
        dx_ref[:, cols] = acc.astype(BF16)

    def out_copy(k, src, dst):
        return pltpu.make_async_copy(src, dst, out_sem.at[k])

    outs = [out_copy(0, dx_ref, dx_out), out_copy(1, dwq_ref, dwq_out), out_copy(2, dwk_ref, dwk_out),
            out_copy(3, dwv_ref, dwv_out), out_copy(4, dwo_ref, dwo_out)]

    with jax.named_scope('t03_kd'):
        for xc in range(chips):
            kd_copy(xc).wait_recv()
            blk = xc * 2 + cc
            kvp[blk] = kvp[blk] + kvr[xc]
        for kind in (1, 0):
            for side in range(2):
                k_copy(side, kind).start()
    with jax.named_scope('t04_ag5'):
        ag_stage1(5)
    with jax.named_scope('t05_y0'):
        y_rest(0)
        y_pass(0)
        y_rest(1)
    with jax.named_scope('t06_ag5'):
        ag_stage2(5)
    with jax.named_scope('t07_kpass'):
        k_pass()
    with jax.named_scope('t08_y1'):
        y_pass(1)
    with jax.named_scope('t09_ag5'):
        ag_stage3(5)
    with jax.named_scope('t10_kfin'):
        for side in range(2):
            k_copy(side, 0).wait_recv()
            k_copy(side, 2).wait_recv()
        kvb[pl.ds(me * tok, half), :] = (kvp[own, 0:half, :] + kr[1, 0] + kr[0, 2]).astype(BF16)
        kvb[pl.ds(me * tok + half, half), :] = (kvp[own, half:, :] + kr[0, 0] + kr[1, 2]).astype(BF16)
        for cp_ in ag_own(3):
            cp_.start()
    with jax.named_scope('t11_dqw'):
        for slot in range(chips):
            for core in range(2):
                if slot > 0:
                    dq_wait(slot, core)
        dq_wait(0, cp)
        wd_own.wait_recv()
        wd_rest.wait_recv()
    with jax.named_scope('t12_dxa'):
        dx_part(0)
    with jax.named_scope('t13_ag3'):
        ag_stage1(3)
    with jax.named_scope('t14_dxa'):
        dx_part(1)
    with jax.named_scope('t15_ag3'):
        ag_stage2(3)
        ag_stage3(3)
    with jax.named_scope('t16_ag5'):
        for xc in (cx, xright, xleft, xfar):
            ag_partner(5, xc)
        for j in (2, 3):
            dx_part(j)
        outs[0].start()
    with jax.named_scope('t17_ag3'):
        for xc in (cx, xright, xleft, xfar):
            ag_partner(3, xc)
    mrow = width // (2 * chips)
    krow = mrow // rows
    with jax.named_scope('t18_wk'):
        part = dot(xf[:, pl.ds(pl.multiple_of(me * mrow, mrow), mrow)], kvb[...], TN)
        wkp[...] = part.reshape(rows, krow, 2 * head_dim)

    def wk_copy(idx, blk, dev):
        return rcopy(wkp.at[blk], wkr.at[idx], wk_s.at[idx], wk_r.at[idx], dev)

    wk_copies = [wk_copy(0, yup, to_u), wk_copy(1, ydn, to_d), wk_copy(2, yfar, to_f)]
    for cp_ in wk_copies:
        cp_.start()
    with jax.named_scope('t19_y0f'):
        first, second = y_final(0)
        dwo_ref[:, 0:wcol] = first
        dwo_ref[:, wcol:] = second
        outs[4].start()
    with jax.named_scope('t20_y1f'):
        for idx, val in enumerate(y_final(1)):
            val = val.T
            for h in range(heads):
                dwq_ref[pl.ds(idx * wcol * heads + h, wcol, stride=heads), :] = val[:, h * head_dim:(h + 1) * head_dim]
        outs[1].start()
    with jax.named_scope('t21_wkf'):
        for cp_ in wk_copies:
            cp_.wait_recv()
        wk_sum = wkp[my] + wkr[0] + wkr[1] + wkr[2]
        dwk_ref[...] = wk_sum[:, 0:head_dim]
        dwv_ref[...] = wk_sum[:, head_dim:]
        outs[2].start()
        outs[3].start()

    with jax.named_scope('t22_sends'):
        for arr in (0, 1, 2, 3, 5):
            for cp_ in ag_all_sends(arr):
                cp_.wait_send()
        for cp_ in ag_ring_first(4) + ag_second(4) + ag_relay(4) + wy_own + wy_relay + [wd_own, wd_rest]:
            cp_.wait_send()
        dq_copy(0, cx, cp).wait_send()
        for s, xc in ((1, xright), (2, xleft), (3, xfar)):
            for core in range(2):
                dq_copy(s, xc, core).wait_send()
        for xc in range(chips):
            kd_copy(xc).wait_send()
        for side in range(2):
            for kind in range(3):
                k_copy(side, kind).wait_send()
                for w in range(2):
                    y_copy(w, side, kind).wait_send()
        for cp_ in wk_copies:
            cp_.wait_send()
        for cp_ in outs:
            cp_.wait()


def copy_out(*refs):
    n = (len(refs) - 1) // 2
    sem = refs[-1]
    copies = [pltpu.make_async_copy(refs[k], refs[n + k], sem.at[k]) for k in range(n)]
    for cp_ in copies:
        cp_.start()
    for cp_ in copies:
        cp_.wait()


VMEM_LIMIT = 60 * 1000 * 1000


def solution(mesh):
    model_size = mesh.shape['model']
    data_size = mesh.shape['data']
    tok_spec = P(('pod', 'data'), 'model', None)
    chips = model_size // 2

    def device_step(x_loc, dy_loc, w_q, w_k, w_v, w_o):
        tok, width = x_loc.shape[1:]
        head_dim = w_k.shape[2]
        head_cols = w_q.shape[1] * head_dim
        assert chips == 4 and data_size == 4 and w_k.shape[0] == 1 and x_loc.shape[0] == 1
        seq = model_size * tok
        half = tok // 2
        heads = head_cols // head_dim
        wcol = width // (2 * data_size)
        krow = width // (model_size * data_size)
        cfg = (tok, width, head_cols, head_dim, chips, data_size)
        vm = pltpu.VMEM
        dma = pltpu.SemaphoreType.DMA
        scratch = [
            vm((seq, width), BF16), vm((seq, width), BF16), vm((2, chips, width, head_cols), BF16), vm((head_cols, width), BF16),
            vm((width, 2 * head_dim), BF16), vm((heads * width, head_dim), BF16), vm((heads * width, head_dim), F32),
            vm((seq, head_cols), BF16), vm((seq, 2 * head_dim), BF16), vm((seq, head_cols), BF16),
            vm((heads, seq, seq), F32), vm((heads, seq, seq), BF16), vm((seq, head_cols), BF16), vm((seq, head_cols), BF16),
            vm((seq, 2 * head_dim), BF16), vm((chips, 2, tok, head_cols), BF16),
            vm((model_size, tok, 2 * head_dim), F32), vm((chips, tok, 2 * head_dim), F32), vm((2, 3, half, 2 * head_dim), F32),
            vm((2, 2 * data_size, head_cols, wcol), F32), vm((2, 2, 3, head_cols, wcol), F32),
            vm((data_size, krow, 2 * head_dim), F32), vm((3, krow, 2 * head_dim), F32),
            vm((tok, width), BF16), vm((heads * 2 * wcol, head_dim), F32), vm((krow, head_dim), F32), vm((krow, head_dim), F32),
            vm((head_cols, 2 * wcol), F32),
            dma((20,)), dma((5,)), dma((6, 14)), dma((6, 16)), dma((6,)), dma((data_size, 2)), dma((2,)), dma((2,)),
            dma((chips, 2)), dma((chips, 2)),
            dma((chips,)), dma((chips,)), dma((2, 3)), dma((2, 3)), dma((2, 2, 3)), dma((2, 2, 3)), dma((3,)), dma((3,)),
        ]
        anyspec = pl.BlockSpec(memory_space=pl.ANY)
        vspec = pl.BlockSpec(memory_space=pltpu.VMEM)
        shapes = (jax.ShapeDtypeStruct((tok, width), BF16), jax.ShapeDtypeStruct((heads * 2 * wcol, head_dim), F32),
                  jax.ShapeDtypeStruct((krow, head_dim), F32), jax.ShapeDtypeStruct((krow, head_dim), F32),
                  jax.ShapeDtypeStruct((head_cols, 2 * wcol), F32))
        outs = pl.pallas_call(
            functools.partial(body, cfg),
            out_shape=tuple(pltpu.VMEM(a.shape, a.dtype) for a in shapes),
            in_specs=[anyspec] * 6,
            out_specs=(anyspec,) * 5,
            scratch_shapes=scratch,
            compiler_params=pltpu.CompilerParams(collective_id=0, has_side_effects=True, vmem_limit_bytes=VMEM_LIMIT),
            name='attn_bwd',
        )(x_loc[0], dy_loc[0], w_q.reshape(width * heads, head_dim), w_o.reshape(head_cols, width), w_k[0], w_v[0])
        dx, dwq, dwk, dwv, dwo = pl.pallas_call(
            copy_out,
            out_shape=shapes,
            in_specs=[vspec] * 5,
            out_specs=(anyspec,) * 5,
            scratch_shapes=[dma((5,))],
            compiler_params=pltpu.CompilerParams(vmem_limit_bytes=4 * 1024 * 1024),
            name='copy_out',
        )(*outs)
        return (dx[None], dwq.reshape(2 * wcol, heads, head_dim), dwk, dwv, dwo.reshape(heads, head_dim, 2 * wcol))

    kv_rows = P(('pod', 'model', 'data'), None)
    return jax.shard_map(device_step, mesh=mesh,
                         in_specs=(tok_spec, tok_spec, P(None, 'model', None), P(), P(), P('model', None, None)),
                         out_specs=(tok_spec, P(('pod', 'data'), 'model', None), kv_rows, kv_rows, P(('pod', 'model'), None, 'data')),
                         check_vma=False)
```

```python
import functools

import jax
import jax.numpy as jnp
from jax import lax
from jax.experimental import pallas as pl
from jax.experimental.pallas import tpu as pltpu
from jax.sharding import PartitionSpec as P

F32 = jnp.float32
BF16 = jnp.bfloat16
NN = (((1,), (0,)), ((), ()))
NT = (((1,), (1,)), ((), ()))
TN = (((0,), (0,)), ((), ()))


def dot(a, b, dims):
    return lax.dot_general(a, b, dims, preferred_element_type=F32)


def body(cfg, x_hbm, dy_hbm, wq_hbm, wo_hbm, wk_hbm, wv_hbm,
         dx_out, dwq_out, dwk_out, dwv_out, dwo_out,
         xf, yf, wqs, wo, wkv, wq2, wq2f, qf, kv, of, prob, dsf, dqf, dof, kvb, dqa,
         kvp, kvr, kr, dwa, yr, wkp, wkr, dx_ref, dwq_ref, dwk_ref, dwv_ref, dwo_ref,
         load_sem, out_sem, ag_s, ag_r, wy_s, wy_r, wd_s, wd_r, dq_s, dq_r,
         kd_s, kd_r, kr_s, kr_r, yr_s, yr_r, wk_s, wk_r):
    tok, width, head_cols, head_dim, chips, rows = cfg
    half = tok // 2
    chunk = 2 * tok
    seq = chips * chunk
    heads = head_cols // head_dim
    wcol = width // (2 * rows)
    hcol = width // 2
    qrow = width // 8
    scale = head_dim ** -0.5

    me = lax.axis_index('model')
    cx = me // 2
    cc = me % 2
    cp = 1 - cc
    xright = (cx + 1) % chips
    xleft = (cx + chips - 1) % chips
    xfar = (cx + 2) % chips
    my = lax.axis_index('data')
    yup = (my + 1) % rows
    ydn = (my + rows - 1) % rows
    yfar = (my + 2) % rows
    to_r = {'model': xright * 2 + cc}
    to_l = {'model': xleft * 2 + cc}
    to_p = {'model': cx * 2 + cp}
    to_u = {'data': yup}
    to_d = {'data': ydn}
    to_f = {'data': yfar}

    def rcopy(src, dst, ssem, rsem, dev):
        return pltpu.make_async_remote_copy(src_ref=src, dst_ref=dst, send_sem=ssem, recv_sem=rsem,
                                            device_id=dev, device_id_type=pl.DeviceIdType.MESH)

    def piece(arr, xc, core, h, base):
        r = pl.ds((xc * 2 + core) * tok + h * half, half)
        if arr == 0:
            return xf.at[r, :]
        if arr == 3:
            return kvb.at[r, :]
        slot = (xc + chips - base) % chips
        if arr == 4:
            return wqs.at[core, slot, pl.ds(my * qrow + h * (qrow // 2), qrow // 2), :]
        if arr >= 5:
            return wqs.at[core, slot, pl.ds((arr - 3) * (hcol // 2) + h * (hcol // 4), hcol // 4), :]
        return yf.at[r, pl.ds((arr - 1) * hcol, hcol)]

    def ag_copy(arr, idx, xc, core, h, dev):
        base = {'r': xright, 'l': xleft, 'p': cx}[dev]
        return rcopy(piece(arr, xc, core, h, cx), piece(arr, xc, core, h, base), ag_s.at[arr, idx],
                     ag_r.at[arr, (xc * 2 + core) * 2 + h], {'r': to_r, 'l': to_l, 'p': to_p}[dev])

    def ag_ring_first(arr):
        return [ag_copy(arr, 0, cx, cc, 0, 'r'), ag_copy(arr, 2, cx, cc, 1, 'l')]

    def ag_first(arr):
        return ag_ring_first(arr) + [ag_copy(arr, 4, cx, cc, 0, 'p'), ag_copy(arr, 5, cx, cc, 1, 'p')]

    def ag_second(arr):
        return [ag_copy(arr, 1, cx, cc, 1, 'r'), ag_copy(arr, 3, cx, cc, 0, 'l')]

    def ag_own(arr):
        return ag_first(arr) + ag_second(arr)

    def ag_relay(arr):
        return [ag_copy(arr, 6, xleft, cc, 0, 'r'), ag_copy(arr, 7, xright, cc, 1, 'l')]

    def ag_cross(arr, idx, xc, h):
        return ag_copy(arr, idx, xc, cc, h, 'p')

    def ag_all_sends(arr):
        out = ag_own(arr) + ag_relay(arr)
        for idx, xc, h in ((8, xleft, 0), (9, xleft, 1), (10, xright, 0), (11, xright, 1), (12, xfar, 0), (13, xfar, 1)):
            out.append(ag_cross(arr, idx, xc, h))
        return out

    def ag_wait(arr, xc, core, h):
        p = piece(arr, xc, core, h, cx)
        rcopy(p, p, ag_s.at[arr, 0], ag_r.at[arr, (xc * 2 + core) * 2 + h], to_p).wait_recv()

    def ag_relays(arr):
        relays = ag_relay(arr)
        ag_wait(arr, xleft, cc, 0)
        relays[0].start()
        ag_wait(arr, xright, cc, 1)
        relays[1].start()

    def ag_stage1(arr):
        ag_relays(arr)
        ag_cross(arr, 8, xleft, 0).start()
        ag_cross(arr, 11, xright, 1).start()

    def ag_stage2(arr):
        ag_wait(arr, xright, cc, 0)
        ag_cross(arr, 10, xright, 0).start()
        ag_wait(arr, xleft, cc, 1)
        ag_cross(arr, 9, xleft, 1).start()

    def ag_stage3(arr):
        ag_wait(arr, xfar, cc, 0)
        ag_cross(arr, 12, xfar, 0).start()
        ag_wait(arr, xfar, cc, 1)
        ag_cross(arr, 13, xfar, 1).start()

    def ag_partner(arr, xc):
        ag_wait(arr, xc, cp, 0)
        ag_wait(arr, xc, cp, 1)

    def wy_copy(idx, q, h, dev):
        p = wqs.at[cc, pl.ds(1, chips - 1), pl.ds(q * qrow + h * (qrow // 2), qrow // 2), :]
        return rcopy(p, p, wy_s.at[idx], wy_r.at[q, h], dev)

    wy_own = [wy_copy(0, my, 0, to_u), wy_copy(1, my, 1, to_d), wy_copy(2, my, 1, to_u), wy_copy(3, my, 0, to_d)]
    wy_relay = [wy_copy(4, ydn, 0, to_u), wy_copy(5, yup, 1, to_d)]

    def wy_pass():
        wy_copy(0, ydn, 0, to_u).wait_recv()
        wy_relay[0].start()
        wy_copy(0, yup, 1, to_u).wait_recv()
        wy_relay[1].start()

    wd_own = rcopy(wqs.at[cc, 0, pl.ds(0, hcol), :], wqs.at[cc, 0, pl.ds(0, hcol), :], wd_s.at[0], wd_r.at[0], to_p)
    wd_rest = rcopy(wqs.at[cc, pl.ds(1, chips - 1), pl.ds(0, hcol), :], wqs.at[cc, pl.ds(1, chips - 1), pl.ds(0, hcol), :],
                    wd_s.at[1], wd_r.at[1], to_p)

    def wy_end():
        for q, h in ((ydn, 1), (yup, 0), (yfar, 0), (yfar, 1)):
            wy_copy(0, q, h, to_u).wait_recv()
        wd_rest.start()

    def dq_copy(s, xc, core):
        return rcopy(dqf.at[pl.ds((xc * 2 + core) * tok, tok), :], dqa.at[(cx + chips - xc) % chips, cc],
                     dq_s.at[s, core], dq_r.at[(cx + chips - xc) % chips, cc], {'model': xc * 2 + core})

    def dq_wait(slot, core):
        rcopy(dqa.at[slot, core], dqa.at[slot, core], dq_s.at[0, 0], dq_r.at[slot, core], to_p).wait_recv()

    def kd_copy(xc):
        return rcopy(kvp.at[xc * 2 + cp], kvr.at[xc], kd_s.at[xc], kd_r.at[xc], to_p)

    def kpart(xc, h):
        return kvp.at[xc * 2 + cc, pl.ds(h * half, half), :]

    def ring_src(kind, side):
        if kind == 0:
            return (xright, 1) if side == 0 else (xleft, 0)
        if kind == 1:
            return (xfar, 0) if side == 0 else (xfar, 1)
        return (xright, 0) if side == 0 else (xleft, 1)

    def k_copy(side, kind):
        xc, h = ring_src(kind, side)
        return rcopy(kpart(xc, h), kr.at[side, kind], kr_s.at[side, kind], kr_r.at[side, kind],
                     to_r if side == 0 else to_l)

    def k_pass():
        for side in range(2):
            k_copy(side, 1).wait_recv()
            xc, h = ring_src(2, side)
            ref = kpart(xc, h)
            ref[...] = ref[...] + kr[side, 1]
            k_copy(side, 2).start()

    order = ((yfar, 0), (yfar, 1), (yup, 1), (ydn, 0), (yup, 0), (ydn, 1), (my, 0), (my, 1))

    def y_blk(w, kind, side):
        pos = {(1, 0): 0, (1, 1): 1, (0, 0): 2, (0, 1): 3, (2, 0): 4, (2, 1): 5, (3, 0): 6, (3, 1): 7}[kind, side]
        if w == 0:
            return pos
        return order[pos][0] * 2 + order[pos][1]

    def y_copy(w, side, kind):
        return rcopy(dwa.at[w, y_blk(w, kind, side)], yr.at[w, side, kind], yr_s.at[w, side, kind], yr_r.at[w, side, kind],
                     to_u if side == 0 else to_d)

    def dw_block(w, kind, side):
        blk = y_blk(w, kind, side)
        if w == 0:
            dwa[0, blk] = dot(of[...], yf[:, blk * wcol:(blk + 1) * wcol], TN)
        else:
            dwa[1, blk] = dot(dqf[...], xf[:, pl.ds(pl.multiple_of(blk * wcol, wcol), wcol)], TN)

    def y_first(w):
        for kind in (1, 0):
            for side in range(2):
                dw_block(w, kind, side)
                y_copy(w, side, kind).start()

    def y_rest(w):
        for kind in (2, 3):
            for side in range(2):
                dw_block(w, kind, side)

    def y_pass(w):
        for side in range(2):
            y_copy(w, side, 1).wait_recv()
            blk = y_blk(w, 2, side)
            dwa[w, blk] = dwa[w, blk] + yr[w, side, 1]
            y_copy(w, side, 2).start()

    def y_final(w):
        for side in range(2):
            y_copy(w, side, 0).wait_recv()
            y_copy(w, side, 2).wait_recv()
        first = dwa[w, y_blk(w, 3, 0)] + yr[w, 1, 0] + yr[w, 0, 2]
        second = dwa[w, y_blk(w, 3, 1)] + yr[w, 0, 0] + yr[w, 1, 2]
        return first, second

    own_rows = pl.ds(me * tok, tok)
    loads = [pltpu.make_async_copy(x_hbm, xf.at[own_rows, :], load_sem.at[0]),
             pltpu.make_async_copy(wq_hbm, wq2, load_sem.at[1]),
             pltpu.make_async_copy(wk_hbm, wkv.at[:, pl.ds(0, head_dim)], load_sem.at[2]),
             pltpu.make_async_copy(wv_hbm, wkv.at[:, pl.ds(head_dim, head_dim)], load_sem.at[3])]
    for pos, (dest, part) in enumerate(order):
        src = pl.ds(pl.multiple_of((dest * 2 + part) * wcol, wcol), wcol)
        dst = pl.ds(pos * wcol, wcol)
        loads.append(pltpu.make_async_copy(dy_hbm.at[:, src], yf.at[own_rows, dst], load_sem.at[4 + pos]))
        loads.append(pltpu.make_async_copy(wo_hbm.at[:, src], wo.at[:, dst], load_sem.at[12 + pos]))
    for cp_ in loads:
        cp_.start()
    barrier = pltpu.get_barrier_semaphore()
    peers = [{'model': (me + k) % (2 * chips)} for k in range(1, 2 * chips)]
    for dev in peers + [to_u, to_d, to_f]:
        pl.semaphore_signal(barrier, inc=1, device_id=dev, device_id_type=pl.DeviceIdType.MESH)
    with jax.named_scope('barrier'):
        pl.semaphore_wait(barrier, 2 * chips + 2)
    loads[0].wait()
    for cp_ in ag_first(0):
        cp_.start()
    with jax.named_scope('loadw'):
        for cp_ in loads[1:]:
            cp_.wait()
        step = 2 * width // 8

        @pl.loop(0, 8)
        def _(b):
            r2 = pl.ds(pl.multiple_of(b * step, step), step)
            wq2f[r2, :] = wq2[r2, :].astype(F32)
            r1 = pl.ds(pl.multiple_of(b * (step // 2), step // 2), step // 2)
            for h in range(heads):
                wqs[cc, 0, r1, h * head_dim:(h + 1) * head_dim] = wq2f[pl.ds(b * step + h, step // 2, stride=heads), :].astype(BF16)

    for cp_ in ag_ring_first(4) + ag_second(4) + ag_second(0):
        cp_.start()
    wd_own.start()

    def chunk_of(s):
        return (cx + s + s // 2 - 2 * (s // 3)) % chips

    @pl.loop(0, chips)
    def _(s):
        @pl.when(s == 0)
        def _():
            ag_partner(0, cx)

        @pl.when(s == 1)
        def _():
            with jax.named_scope('q1'):
                ag_relays(4)
                ag_stage1(0)
                for cp_ in ag_own(1) + ag_first(2):
                    cp_.start()
                ag_stage2(0)
            with jax.named_scope('q1w'):
                for xc, h in ((xleft, 1), (xright, 0), (xfar, 0), (xfar, 1)):
                    ag_wait(4, xc, cc, h)
                for cp_ in wy_own:
                    cp_.start()
            ag_partner(0, xright)

        @pl.when(s == 2)
        def _():
            ag_partner(0, xleft)

        @pl.when(s == 3)
        def _():
            ag_stage3(0)
            ag_partner(0, xfar)

        r = pl.ds(chunk_of(s) * chunk, chunk)
        xc = xf[r, :]
        qf[r, :] = dot(xc, wqs[cc, 0], NN).astype(BF16)
        kv[r, :] = dot(xc, wkv[...], NN).astype(BF16)

    @pl.loop(0, chips)
    def _(s):
        @pl.when(s == 1)
        def _():
            with jax.named_scope('f1'):
                ag_stage1(1)
                for cp_ in ag_second(2):
                    cp_.start()

        @pl.when(s == 2)
        def _():
            with jax.named_scope('f2'):
                ag_stage2(1)

        @pl.when(s == 3)
        def _():
            with jax.named_scope('f3'):
                wy_pass()

        i = chunk_of(s)
        r = pl.ds(i * chunk, chunk)
        row_id = lax.broadcasted_iota(jnp.int32, (chunk, seq), 0) + i * chunk
        keep = row_id >= lax.broadcasted_iota(jnp.int32, (chunk, seq), 1)
        for h in range(heads):
            hc = pl.ds(h * head_dim, head_dim)
            sc = dot(qf[r, hc], kv[:, 0:head_dim], NT) * scale
            sc = jnp.where(keep, sc, -jnp.inf)
            ex = jnp.exp(sc - jnp.max(sc, axis=-1, keepdims=True))
            pr = ex * (1.0 / jnp.sum(ex, axis=-1, keepdims=True))
            prob[h, r, :] = pr
            of[r, hc] = dot(pr.astype(BF16), kv[:, head_dim:], NN).astype(BF16)

    with jax.named_scope('b0'):
        ag_stage3(1)
        ag_partner(1, cx)
        ag_partner(2, cx)

    @pl.loop(0, chips)
    def _(s):
        @pl.when(s == 1)
        def _():
            with jax.named_scope('b1'):
                for xc in (xright, xleft, xfar):
                    ag_partner(1, xc)
            with jax.named_scope('b1y'):
                y_first(0)
            with jax.named_scope('b1s'):
                ag_stage1(2)
                for cp_ in ag_own(5):
                    cp_.start()
                wy_end()
            with jax.named_scope('b1w'):
                ag_stage2(2)
                ag_partner(2, xright)

        @pl.when(s == 2)
        def _():
            with jax.named_scope('b2'):
                ag_stage3(2)
                ag_partner(2, xleft)

        @pl.when(s == 3)
        def _():
            with jax.named_scope('b3'):
                ag_partner(2, xfar)

        with jax.named_scope('b_comp'):
            i = chunk_of(s)
            r = pl.ds(i * chunk, chunk)
            oc = of[r, :]
            do = dot(yf[r, :], wo[...], NT).astype(BF16)
            dof[r, :] = do
            od = do.astype(F32) * oc.astype(F32)
            for h in range(heads):
                hs = slice(h * head_dim, (h + 1) * head_dim)
                dp = dot(do[:, hs], kv[:, head_dim:], NT)
                ds = (prob[h, r, :] * (dp - jnp.sum(od[:, hs], axis=-1, keepdims=True))).astype(BF16)
                dsf[h, r, :] = ds
                dqf[r, hs] = (dot(ds, kv[:, 0:head_dim], NN) * scale).astype(BF16)

        @pl.when(s == 0)
        def _():
            dqa[0, cc] = dqf[own_rows, :]
            dq_copy(0, cx, cp).start()

        @pl.when(s > 0)
        def _():
            for core in range(2):
                dq_copy(s, i, core).start()

    with jax.named_scope('t00_dkv'):
        for kc in range(chips):
            ks = slice(kc * chunk, (kc + 1) * chunk)
            qs = slice(kc * chunk, seq)
            dk = jnp.zeros((chunk, head_dim), F32)
            dv = jnp.zeros((chunk, head_dim), F32)
            for h in range(heads):
                hs = slice(h * head_dim, (h + 1) * head_dim)
                dk = dk + dot(dsf[h, qs, ks], qf[qs, hs], TN)
                dv = dv + dot(prob[h, qs, ks].astype(BF16), dof[qs, hs], TN)
            kvp[2 * kc:2 * kc + 2, :, 0:head_dim] = (dk * scale).reshape(2, tok, head_dim)
            kvp[2 * kc:2 * kc + 2, :, head_dim:] = dv.reshape(2, tok, head_dim)
        for xc in range(chips):
            kd_copy(xc).start()
    with jax.named_scope('t00_y1'):
        y_first(1)

    own = cx * 2 + cc

    def dx_part(j):
        cols = slice(j * (hcol // 2), (j + 1) * (hcol // 2))
        acc = dot(kvb[own_rows, :], wkv[cols, :], NT)
        for slot in range(chips):
            for core in range(2):
                acc = acc + dot(dqa[slot, core], wqs[core, slot, cols, :], NT)
        dx_ref[:, cols] = acc.astype(BF16)

    def out_copy(k, src, dst):
        return pltpu.make_async_copy(src, dst, out_sem.at[k])

    outs = [out_copy(0, dx_ref, dx_out), out_copy(1, dwq_ref, dwq_out), out_copy(2, dwk_ref, dwk_out),
            out_copy(3, dwv_ref, dwv_out), out_copy(4, dwo_ref, dwo_out)]

    with jax.named_scope('t03_kd'):
        for xc in range(chips):
            kd_copy(xc).wait_recv()
            blk = xc * 2 + cc
            kvp[blk] = kvp[blk] + kvr[xc]
        for kind in (1, 0):
            for side in range(2):
                k_copy(side, kind).start()
    with jax.named_scope('t04_ag5'):
        ag_stage1(5)
    with jax.named_scope('t05_y0'):
        y_rest(0)
        y_pass(0)
    with jax.named_scope('t06_ag5'):
        ag_stage2(5)
    with jax.named_scope('t07_kpass'):
        k_pass()
        for cp_ in ag_first(6):
            cp_.start()
    with jax.named_scope('t08_y1'):
        y_rest(1)
        y_pass(1)
    with jax.named_scope('t09_ag5'):
        ag_stage3(5)
    with jax.named_scope('t10_kfin'):
        for side in range(2):
            k_copy(side, 0).wait_recv()
            k_copy(side, 2).wait_recv()
        kvb[pl.ds(me * tok, half), :] = (kvp[own, 0:half, :] + kr[1, 0] + kr[0, 2]).astype(BF16)
        kvb[pl.ds(me * tok + half, half), :] = (kvp[own, half:, :] + kr[0, 0] + kr[1, 2]).astype(BF16)
        for cp_ in ag_own(3) + ag_second(6):
            cp_.start()
    with jax.named_scope('t11_dqw'):
        for slot in range(chips):
            for core in range(2):
                if slot > 0:
                    dq_wait(slot, core)
        dq_wait(0, cp)
        wd_own.wait_recv()
        wd_rest.wait_recv()
    with jax.named_scope('t12_dxa'):
        dx_part(0)
    with jax.named_scope('t13_ag3'):
        ag_stage1(3)
        ag_stage1(6)
    with jax.named_scope('t14_dxa'):
        dx_part(1)
    with jax.named_scope('t15_ag3'):
        ag_stage2(3)
        ag_stage2(6)
    with jax.named_scope('t16_ag3'):
        ag_stage3(3)
        for xc in (cx, xright, xleft, xfar):
            ag_partner(3, xc)
    mrow = width // (2 * chips)
    krow = mrow // rows
    with jax.named_scope('t18_wk'):
        part = dot(xf[:, pl.ds(pl.multiple_of(me * mrow, mrow), mrow)], kvb[...], TN)
        wkp[...] = part.reshape(rows, krow, 2 * head_dim)

    def wk_copy(idx, blk, dev):
        return rcopy(wkp.at[blk], wkr.at[idx], wk_s.at[idx], wk_r.at[idx], dev)

    wk_copies = [wk_copy(0, yup, to_u), wk_copy(1, ydn, to_d), wk_copy(2, yfar, to_f)]
    for cp_ in wk_copies:
        cp_.start()
    with jax.named_scope('t19_dx2'):
        for xc in (cx, xright, xleft, xfar):
            ag_partner(5, xc)
        dx_part(2)
    with jax.named_scope('t19_ag6'):
        ag_stage3(6)
        for xc in (cx, xright, xleft, xfar):
            ag_partner(6, xc)
        dx_part(3)
        outs[0].start()
    with jax.named_scope('t19_y0f'):
        first, second = y_final(0)
        dwo_ref[:, 0:wcol] = first
        dwo_ref[:, wcol:] = second
        outs[4].start()
    with jax.named_scope('t20_y1f'):
        for idx, val in enumerate(y_final(1)):
            val = val.T
            for h in range(heads):
                dwq_ref[pl.ds(idx * wcol * heads + h, wcol, stride=heads), :] = val[:, h * head_dim:(h + 1) * head_dim]
        outs[1].start()
    with jax.named_scope('t21_wkf'):
        for cp_ in wk_copies:
            cp_.wait_recv()
        wk_sum = wkp[my] + wkr[0] + wkr[1] + wkr[2]
        dwk_ref[...] = wk_sum[:, 0:head_dim]
        dwv_ref[...] = wk_sum[:, head_dim:]
        outs[2].start()
        outs[3].start()

    with jax.named_scope('t22_sends'):
        for arr in (0, 1, 2, 3, 5, 6):
            for cp_ in ag_all_sends(arr):
                cp_.wait_send()
        for cp_ in ag_ring_first(4) + ag_second(4) + ag_relay(4) + wy_own + wy_relay + [wd_own, wd_rest]:
            cp_.wait_send()
        dq_copy(0, cx, cp).wait_send()
        for s, xc in ((1, xright), (2, xleft), (3, xfar)):
            for core in range(2):
                dq_copy(s, xc, core).wait_send()
        for xc in range(chips):
            kd_copy(xc).wait_send()
        for side in range(2):
            for kind in range(3):
                k_copy(side, kind).wait_send()
                for w in range(2):
                    y_copy(w, side, kind).wait_send()
        for cp_ in wk_copies:
            cp_.wait_send()
        for cp_ in outs:
            cp_.wait()


def copy_out(*refs):
    n = (len(refs) - 1) // 2
    sem = refs[-1]
    copies = [pltpu.make_async_copy(refs[k], refs[n + k], sem.at[k]) for k in range(n)]
    for cp_ in copies:
        cp_.start()
    for cp_ in copies:
        cp_.wait()


VMEM_LIMIT = 60 * 1000 * 1000


def solution(mesh):
    model_size = mesh.shape['model']
    data_size = mesh.shape['data']
    tok_spec = P(('pod', 'data'), 'model', None)
    chips = model_size // 2

    def device_step(x_loc, dy_loc, w_q, w_k, w_v, w_o):
        tok, width = x_loc.shape[1:]
        head_dim = w_k.shape[2]
        head_cols = w_q.shape[1] * head_dim
        assert chips == 4 and data_size == 4 and w_k.shape[0] == 1 and x_loc.shape[0] == 1
        seq = model_size * tok
        half = tok // 2
        heads = head_cols // head_dim
        wcol = width // (2 * data_size)
        krow = width // (model_size * data_size)
        cfg = (tok, width, head_cols, head_dim, chips, data_size)
        vm = pltpu.VMEM
        dma = pltpu.SemaphoreType.DMA
        scratch = [
            vm((seq, width), BF16), vm((seq, width), BF16), vm((2, chips, width, head_cols), BF16), vm((head_cols, width), BF16),
            vm((width, 2 * head_dim), BF16), vm((heads * width, head_dim), BF16), vm((heads * width, head_dim), F32),
            vm((seq, head_cols), BF16), vm((seq, 2 * head_dim), BF16), vm((seq, head_cols), BF16),
            vm((heads, seq, seq), F32), vm((heads, seq, seq), BF16), vm((seq, head_cols), BF16), vm((seq, head_cols), BF16),
            vm((seq, 2 * head_dim), BF16), vm((chips, 2, tok, head_cols), BF16),
            vm((model_size, tok, 2 * head_dim), F32), vm((chips, tok, 2 * head_dim), F32), vm((2, 3, half, 2 * head_dim), F32),
            vm((2, 2 * data_size, head_cols, wcol), F32), vm((2, 2, 3, head_cols, wcol), F32),
            vm((data_size, krow, 2 * head_dim), F32), vm((3, krow, 2 * head_dim), F32),
            vm((tok, width), BF16), vm((heads * 2 * wcol, head_dim), F32), vm((krow, head_dim), F32), vm((krow, head_dim), F32),
            vm((head_cols, 2 * wcol), F32),
            dma((20,)), dma((5,)), dma((7, 14)), dma((7, 16)), dma((6,)), dma((data_size, 2)), dma((2,)), dma((2,)),
            dma((chips, 2)), dma((chips, 2)),
            dma((chips,)), dma((chips,)), dma((2, 3)), dma((2, 3)), dma((2, 2, 3)), dma((2, 2, 3)), dma((3,)), dma((3,)),
        ]
        anyspec = pl.BlockSpec(memory_space=pl.ANY)
        vspec = pl.BlockSpec(memory_space=pltpu.VMEM)
        shapes = (jax.ShapeDtypeStruct((tok, width), BF16), jax.ShapeDtypeStruct((heads * 2 * wcol, head_dim), F32),
                  jax.ShapeDtypeStruct((krow, head_dim), F32), jax.ShapeDtypeStruct((krow, head_dim), F32),
                  jax.ShapeDtypeStruct((head_cols, 2 * wcol), F32))
        outs = pl.pallas_call(
            functools.partial(body, cfg),
            out_shape=tuple(pltpu.VMEM(a.shape, a.dtype) for a in shapes),
            in_specs=[anyspec] * 6,
            out_specs=(anyspec,) * 5,
            scratch_shapes=scratch,
            compiler_params=pltpu.CompilerParams(collective_id=0, has_side_effects=True, vmem_limit_bytes=VMEM_LIMIT),
            name='attn_bwd',
        )(x_loc[0], dy_loc[0], w_q.reshape(width * heads, head_dim), w_o.reshape(head_cols, width), w_k[0], w_v[0])
        dx, dwq, dwk, dwv, dwo = pl.pallas_call(
            copy_out,
            out_shape=shapes,
            in_specs=[vspec] * 5,
            out_specs=(anyspec,) * 5,
            scratch_shapes=[dma((5,))],
            compiler_params=pltpu.CompilerParams(vmem_limit_bytes=4 * 1024 * 1024),
            name='copy_out',
        )(*outs)
        return (dx[None], dwq.reshape(2 * wcol, heads, head_dim), dwk, dwv, dwo.reshape(heads, head_dim, 2 * wcol))

    kv_rows = P(('pod', 'model', 'data'), None)
    return jax.shard_map(device_step, mesh=mesh,
                         in_specs=(tok_spec, tok_spec, P(None, 'model', None), P(), P(), P('model', None, None)),
                         out_specs=(tok_spec, P(('pod', 'data'), 'model', None), kv_rows, kv_rows, P(('pod', 'model'), None, 'data')),
                         check_vma=False)
```

```python
import functools

import jax
import jax.numpy as jnp
from jax import lax
from jax.experimental import pallas as pl
from jax.experimental.pallas import tpu as pltpu
from jax.sharding import PartitionSpec as P

F32 = jnp.float32
BF16 = jnp.bfloat16
NN = (((1,), (0,)), ((), ()))
NT = (((1,), (1,)), ((), ()))
TN = (((0,), (0,)), ((), ()))


def dot(a, b, dims):
    return lax.dot_general(a, b, dims, preferred_element_type=F32)


def body(cfg, x_hbm, dy_hbm, wq_hbm, wo_hbm, wk_hbm, wv_hbm,
         dx_out, dwq_out, dwk_out, dwv_out, dwo_out,
         xf, yf, wqs, wo, wkv, wq2, wq2f, qf, kv, of, prob, dsf, dqf, dof, kvb, dqa,
         kvp, kvr, kr, dwa, yr, wkp, wkr, dx_ref, dwq_ref, dwk_ref, dwv_ref, dwo_ref,
         load_sem, out_sem, ag_s, ag_r, wy_s, wy_r, wd_s, wd_r, dq_s, dq_r,
         kd_s, kd_r, kr_s, kr_r, yr_s, yr_r, wk_s, wk_r):
    tok, width, head_cols, head_dim, chips, rows = cfg
    half = tok // 2
    chunk = 2 * tok
    seq = chips * chunk
    heads = head_cols // head_dim
    wcol = width // (2 * rows)
    hcol = width // 2
    qrow = width // 8
    scale = head_dim ** -0.5

    me = lax.axis_index('model')
    cx = me // 2
    cc = me % 2
    cp = 1 - cc
    xright = (cx + 1) % chips
    xleft = (cx + chips - 1) % chips
    xfar = (cx + 2) % chips
    my = lax.axis_index('data')
    yup = (my + 1) % rows
    ydn = (my + rows - 1) % rows
    yfar = (my + 2) % rows
    to_r = {'model': xright * 2 + cc}
    to_l = {'model': xleft * 2 + cc}
    to_p = {'model': cx * 2 + cp}
    to_u = {'data': yup}
    to_d = {'data': ydn}
    to_f = {'data': yfar}

    def rcopy(src, dst, ssem, rsem, dev):
        return pltpu.make_async_remote_copy(src_ref=src, dst_ref=dst, send_sem=ssem, recv_sem=rsem,
                                            device_id=dev, device_id_type=pl.DeviceIdType.MESH)

    def piece(arr, xc, core, h, base):
        r = pl.ds((xc * 2 + core) * tok + h * half, half)
        if arr == 0:
            return xf.at[r, :]
        if arr == 3:
            return kvb.at[r, :]
        slot = (xc + chips - base) % chips
        if arr == 4:
            return wqs.at[core, slot, pl.ds(my * qrow + h * (qrow // 2), qrow // 2), :]
        if arr >= 5:
            return wqs.at[core, slot, pl.ds((arr - 3) * (hcol // 2) + h * (hcol // 4), hcol // 4), :]
        return yf.at[r, pl.ds((arr - 1) * hcol, hcol)]

    def ag_copy(arr, idx, xc, core, h, dev):
        base = {'r': xright, 'l': xleft, 'p': cx}[dev]
        return rcopy(piece(arr, xc, core, h, cx), piece(arr, xc, core, h, base), ag_s.at[arr, idx],
                     ag_r.at[arr, (xc * 2 + core) * 2 + h], {'r': to_r, 'l': to_l, 'p': to_p}[dev])

    def ag_ring_first(arr):
        return [ag_copy(arr, 0, cx, cc, 0, 'r'), ag_copy(arr, 2, cx, cc, 1, 'l')]

    def ag_first(arr):
        return ag_ring_first(arr) + [ag_copy(arr, 4, cx, cc, 0, 'p'), ag_copy(arr, 5, cx, cc, 1, 'p')]

    def ag_second(arr):
        return [ag_copy(arr, 1, cx, cc, 1, 'r'), ag_copy(arr, 3, cx, cc, 0, 'l')]

    def ag_own(arr):
        return ag_first(arr) + ag_second(arr)

    def ag_relay(arr):
        return [ag_copy(arr, 6, xleft, cc, 0, 'r'), ag_copy(arr, 7, xright, cc, 1, 'l')]

    def ag_cross(arr, idx, xc, h):
        return ag_copy(arr, idx, xc, cc, h, 'p')

    def ag_all_sends(arr):
        out = ag_own(arr) + ag_relay(arr)
        for idx, xc, h in ((8, xleft, 0), (9, xleft, 1), (10, xright, 0), (11, xright, 1), (12, xfar, 0), (13, xfar, 1)):
            out.append(ag_cross(arr, idx, xc, h))
        return out

    def ag_wait(arr, xc, core, h):
        p = piece(arr, xc, core, h, cx)
        rcopy(p, p, ag_s.at[arr, 0], ag_r.at[arr, (xc * 2 + core) * 2 + h], to_p).wait_recv()

    def ag_relays(arr):
        relays = ag_relay(arr)
        ag_wait(arr, xleft, cc, 0)
        relays[0].start()
        ag_wait(arr, xright, cc, 1)
        relays[1].start()

    def ag_stage1(arr):
        ag_relays(arr)
        ag_cross(arr, 8, xleft, 0).start()
        ag_cross(arr, 11, xright, 1).start()

    def ag_stage2(arr):
        ag_wait(arr, xright, cc, 0)
        ag_cross(arr, 10, xright, 0).start()
        ag_wait(arr, xleft, cc, 1)
        ag_cross(arr, 9, xleft, 1).start()

    def ag_stage3(arr):
        ag_wait(arr, xfar, cc, 0)
        ag_cross(arr, 12, xfar, 0).start()
        ag_wait(arr, xfar, cc, 1)
        ag_cross(arr, 13, xfar, 1).start()

    def ag_partner(arr, xc):
        ag_wait(arr, xc, cp, 0)
        ag_wait(arr, xc, cp, 1)

    def wy_copy(idx, q, h, dev):
        p = wqs.at[cc, pl.ds(1, chips - 1), pl.ds(q * qrow + h * (qrow // 2), qrow // 2), :]
        return rcopy(p, p, wy_s.at[idx], wy_r.at[q, h], dev)

    wy_own = [wy_copy(0, my, 0, to_u), wy_copy(1, my, 1, to_d), wy_copy(2, my, 1, to_u), wy_copy(3, my, 0, to_d)]
    wy_relay = [wy_copy(4, ydn, 0, to_u), wy_copy(5, yup, 1, to_d)]

    def wy_pass():
        wy_copy(0, ydn, 0, to_u).wait_recv()
        wy_relay[0].start()
        wy_copy(0, yup, 1, to_u).wait_recv()
        wy_relay[1].start()

    wd_own = rcopy(wqs.at[cc, 0, pl.ds(0, hcol), :], wqs.at[cc, 0, pl.ds(0, hcol), :], wd_s.at[0], wd_r.at[0], to_p)
    wd_rest = rcopy(wqs.at[cc, pl.ds(1, chips - 1), pl.ds(0, hcol), :], wqs.at[cc, pl.ds(1, chips - 1), pl.ds(0, hcol), :],
                    wd_s.at[1], wd_r.at[1], to_p)

    def wy_end():
        for q, h in ((ydn, 1), (yup, 0), (yfar, 0), (yfar, 1)):
            wy_copy(0, q, h, to_u).wait_recv()
        wd_rest.start()

    def dq_copy(s, xc, core):
        return rcopy(dqf.at[pl.ds((xc * 2 + core) * tok, tok), :], dqa.at[(cx + chips - xc) % chips, cc],
                     dq_s.at[s, core], dq_r.at[(cx + chips - xc) % chips, cc], {'model': xc * 2 + core})

    def dq_wait(slot, core):
        rcopy(dqa.at[slot, core], dqa.at[slot, core], dq_s.at[0, 0], dq_r.at[slot, core], to_p).wait_recv()

    def kd_copy(xc):
        return rcopy(kvp.at[xc * 2 + cp], kvr.at[xc], kd_s.at[xc], kd_r.at[xc], to_p)

    def kpart(xc, h):
        return kvp.at[xc * 2 + cc, pl.ds(h * half, half), :]

    def ring_src(kind, side):
        if kind == 0:
            return (xright, 1) if side == 0 else (xleft, 0)
        if kind == 1:
            return (xfar, 0) if side == 0 else (xfar, 1)
        return (xright, 0) if side == 0 else (xleft, 1)

    def k_copy(side, kind):
        xc, h = ring_src(kind, side)
        return rcopy(kpart(xc, h), kr.at[side, kind], kr_s.at[side, kind], kr_r.at[side, kind],
                     to_r if side == 0 else to_l)

    def k_pass():
        for side in range(2):
            k_copy(side, 1).wait_recv()
            xc, h = ring_src(2, side)
            ref = kpart(xc, h)
            ref[...] = ref[...] + kr[side, 1]
            k_copy(side, 2).start()

    order = ((yfar, 0), (yfar, 1), (yup, 1), (ydn, 0), (yup, 0), (ydn, 1), (my, 0), (my, 1))

    def y_blk(w, kind, side):
        pos = {(1, 0): 0, (1, 1): 1, (0, 0): 2, (0, 1): 3, (2, 0): 4, (2, 1): 5, (3, 0): 6, (3, 1): 7}[kind, side]
        if w == 0:
            return pos
        return order[pos][0] * 2 + order[pos][1]

    def y_copy(w, side, kind):
        return rcopy(dwa.at[w, y_blk(w, kind, side)], yr.at[w, side, kind], yr_s.at[w, side, kind], yr_r.at[w, side, kind],
                     to_u if side == 0 else to_d)

    def dw_block(w, kind, side):
        blk = y_blk(w, kind, side)
        if w == 0:
            dwa[0, blk] = dot(of[...], yf[:, blk * wcol:(blk + 1) * wcol], TN)
        else:
            dwa[1, blk] = dot(dqf[...], xf[:, pl.ds(pl.multiple_of(blk * wcol, wcol), wcol)], TN)

    def y_first(w, between=lambda: None):
        for kind in (1, 0):
            for side in range(2):
                dw_block(w, kind, side)
                y_copy(w, side, kind).start()
            if kind == 1:
                between()

    def y_rest(w):
        for kind in (2, 3):
            for side in range(2):
                dw_block(w, kind, side)

    def y_pass(w):
        for side in range(2):
            y_copy(w, side, 1).wait_recv()
            blk = y_blk(w, 2, side)
            dwa[w, blk] = dwa[w, blk] + yr[w, side, 1]
            y_copy(w, side, 2).start()

    def y_final(w):
        for side in range(2):
            y_copy(w, side, 0).wait_recv()
            y_copy(w, side, 2).wait_recv()
        first = dwa[w, y_blk(w, 3, 0)] + yr[w, 1, 0] + yr[w, 0, 2]
        second = dwa[w, y_blk(w, 3, 1)] + yr[w, 0, 0] + yr[w, 1, 2]
        return first, second

    own_rows = pl.ds(me * tok, tok)
    loads = [pltpu.make_async_copy(x_hbm, xf.at[own_rows, :], load_sem.at[0]),
             pltpu.make_async_copy(wq_hbm, wq2, load_sem.at[1]),
             pltpu.make_async_copy(wk_hbm, wkv.at[:, pl.ds(0, head_dim)], load_sem.at[2]),
             pltpu.make_async_copy(wv_hbm, wkv.at[:, pl.ds(head_dim, head_dim)], load_sem.at[3])]
    for pos, (dest, part) in enumerate(order):
        src = pl.ds(pl.multiple_of((dest * 2 + part) * wcol, wcol), wcol)
        dst = pl.ds(pos * wcol, wcol)
        loads.append(pltpu.make_async_copy(dy_hbm.at[:, src], yf.at[own_rows, dst], load_sem.at[4 + pos]))
        loads.append(pltpu.make_async_copy(wo_hbm.at[:, src], wo.at[:, dst], load_sem.at[12 + pos]))
    for cp_ in loads:
        cp_.start()
    barrier = pltpu.get_barrier_semaphore()
    peers = [{'model': (me + k) % (2 * chips)} for k in range(1, 2 * chips)]
    for dev in peers + [to_u, to_d, to_f]:
        pl.semaphore_signal(barrier, inc=1, device_id=dev, device_id_type=pl.DeviceIdType.MESH)
    with jax.named_scope('barrier'):
        pl.semaphore_wait(barrier, 2 * chips + 2)
    loads[0].wait()
    for cp_ in ag_first(0):
        cp_.start()
    with jax.named_scope('loadw'):
        for cp_ in loads[1:]:
            cp_.wait()
        step = 2 * width // 8

        @pl.loop(0, 8)
        def _(b):
            r2 = pl.ds(pl.multiple_of(b * step, step), step)
            wq2f[r2, :] = wq2[r2, :].astype(F32)
            r1 = pl.ds(pl.multiple_of(b * (step // 2), step // 2), step // 2)
            for h in range(heads):
                wqs[cc, 0, r1, h * head_dim:(h + 1) * head_dim] = wq2f[pl.ds(b * step + h, step // 2, stride=heads), :].astype(BF16)

    for cp_ in ag_ring_first(4) + ag_second(4) + ag_second(0):
        cp_.start()
    wd_own.start()

    def chunk_of(s):
        return (cx + s + s // 2 - 2 * (s // 3)) % chips

    @pl.loop(0, chips)
    def _(s):
        @pl.when(s == 0)
        def _():
            ag_partner(0, cx)

        @pl.when(s == 1)
        def _():
            with jax.named_scope('q1'):
                ag_relays(4)
                ag_stage1(0)
                for cp_ in ag_own(1) + ag_first(2):
                    cp_.start()
                ag_stage2(0)
            with jax.named_scope('q1w'):
                for xc, h in ((xleft, 1), (xright, 0), (xfar, 0), (xfar, 1)):
                    ag_wait(4, xc, cc, h)
                for cp_ in wy_own:
                    cp_.start()
            ag_partner(0, xright)

        @pl.when(s == 2)
        def _():
            ag_partner(0, xleft)

        @pl.when(s == 3)
        def _():
            ag_stage3(0)
            ag_partner(0, xfar)

        r = pl.ds(chunk_of(s) * chunk, chunk)
        xc = xf[r, :]
        qf[r, :] = dot(xc, wqs[cc, 0], NN).astype(BF16)
        kv[r, :] = dot(xc, wkv[...], NN).astype(BF16)

    @pl.loop(0, chips)
    def _(s):
        @pl.when(s == 1)
        def _():
            with jax.named_scope('f1'):
                ag_stage1(1)
                for cp_ in ag_second(2):
                    cp_.start()

        @pl.when(s == 2)
        def _():
            with jax.named_scope('f2'):
                ag_stage2(1)

        @pl.when(s == 3)
        def _():
            with jax.named_scope('f3'):
                wy_pass()

        i = chunk_of(s)
        r = pl.ds(i * chunk, chunk)
        row_id = lax.broadcasted_iota(jnp.int32, (chunk, seq), 0) + i * chunk
        keep = row_id >= lax.broadcasted_iota(jnp.int32, (chunk, seq), 1)
        for h in range(heads):
            hc = pl.ds(h * head_dim, head_dim)
            sc = dot(qf[r, hc], kv[:, 0:head_dim], NT) * scale
            sc = jnp.where(keep, sc, -jnp.inf)
            ex = jnp.exp(sc - jnp.max(sc, axis=-1, keepdims=True))
            pr = ex * (1.0 / jnp.sum(ex, axis=-1, keepdims=True))
            prob[h, r, :] = pr
            of[r, hc] = dot(pr.astype(BF16), kv[:, head_dim:], NN).astype(BF16)

    with jax.named_scope('b0'):
        ag_stage1(2)
        for cp_ in ag_own(5):
            cp_.start()
        ag_stage3(1)
        ag_partner(1, cx)
        ag_partner(2, cx)

    @pl.loop(0, chips)
    def _(s):
        @pl.when(s == 1)
        def _():
            with jax.named_scope('b1'):
                for xc in (xright, xleft, xfar):
                    ag_partner(1, xc)
            with jax.named_scope('b1y'):
                y_first(0, lambda: ag_stage2(2))
            with jax.named_scope('b1s'):
                wy_end()
            with jax.named_scope('b1w'):
                ag_partner(2, xright)

        @pl.when(s == 2)
        def _():
            with jax.named_scope('b2'):
                ag_stage3(2)
                ag_partner(2, xleft)

        @pl.when(s == 3)
        def _():
            with jax.named_scope('b3'):
                ag_partner(2, xfar)

        with jax.named_scope('b_comp'):
            i = chunk_of(s)
            r = pl.ds(i * chunk, chunk)
            oc = of[r, :]
            do = dot(yf[r, :], wo[...], NT).astype(BF16)
            dof[r, :] = do
            od = do.astype(F32) * oc.astype(F32)
            for h in range(heads):
                hs = slice(h * head_dim, (h + 1) * head_dim)
                dp = dot(do[:, hs], kv[:, head_dim:], NT)
                ds = (prob[h, r, :] * (dp - jnp.sum(od[:, hs], axis=-1, keepdims=True))).astype(BF16)
                dsf[h, r, :] = ds
                dqf[r, hs] = (dot(ds, kv[:, 0:head_dim], NN) * scale).astype(BF16)

        @pl.when(s == 0)
        def _():
            dqa[0, cc] = dqf[own_rows, :]
            dq_copy(0, cx, cp).start()

        @pl.when(s > 0)
        def _():
            for core in range(2):
                dq_copy(s, i, core).start()

    with jax.named_scope('t00_dkv'):
        for kc in range(chips):
            ks = slice(kc * chunk, (kc + 1) * chunk)
            qs = slice(kc * chunk, seq)
            dk = jnp.zeros((chunk, head_dim), F32)
            dv = jnp.zeros((chunk, head_dim), F32)
            for h in range(heads):
                hs = slice(h * head_dim, (h + 1) * head_dim)
                dk = dk + dot(dsf[h, qs, ks], qf[qs, hs], TN)
                dv = dv + dot(prob[h, qs, ks].astype(BF16), dof[qs, hs], TN)
            kvp[2 * kc:2 * kc + 2, :, 0:head_dim] = (dk * scale).reshape(2, tok, head_dim)
            kvp[2 * kc:2 * kc + 2, :, head_dim:] = dv.reshape(2, tok, head_dim)
        for xc in range(chips):
            kd_copy(xc).start()
    with jax.named_scope('t00_y1'):
        y_first(1)

    own = cx * 2 + cc

    def dx_part(j):
        cols = slice(j * (hcol // 2), (j + 1) * (hcol // 2))
        acc = dot(kvb[own_rows, :], wkv[cols, :], NT)
        for slot in range(chips):
            for core in range(2):
                acc = acc + dot(dqa[slot, core], wqs[core, slot, cols, :], NT)
        dx_ref[:, cols] = acc.astype(BF16)

    def out_copy(k, src, dst):
        return pltpu.make_async_copy(src, dst, out_sem.at[k])

    outs = [out_copy(0, dx_ref, dx_out), out_copy(1, dwq_ref, dwq_out), out_copy(2, dwk_ref, dwk_out),
            out_copy(3, dwv_ref, dwv_out), out_copy(4, dwo_ref, dwo_out)]

    with jax.named_scope('t03_kd'):
        for xc in range(chips):
            kd_copy(xc).wait_recv()
            blk = xc * 2 + cc
            kvp[blk] = kvp[blk] + kvr[xc]
        for kind in (1, 0):
            for side in range(2):
                k_copy(side, kind).start()
    with jax.named_scope('t04_ag5'):
        ag_stage1(5)
    with jax.named_scope('t05_y0'):
        y_rest(0)
        y_pass(0)
    with jax.named_scope('t06_ag5'):
        ag_stage2(5)
    with jax.named_scope('t07_kpass'):
        k_pass()
        for cp_ in ag_first(6):
            cp_.start()
    with jax.named_scope('t08_y1'):
        y_rest(1)
        y_pass(1)
    with jax.named_scope('t09_ag5'):
        ag_stage3(5)
    with jax.named_scope('t10_kfin'):
        for side in range(2):
            k_copy(side, 0).wait_recv()
            k_copy(side, 2).wait_recv()
        kvb[pl.ds(me * tok, half), :] = (kvp[own, 0:half, :] + kr[1, 0] + kr[0, 2]).astype(BF16)
        kvb[pl.ds(me * tok + half, half), :] = (kvp[own, half:, :] + kr[0, 0] + kr[1, 2]).astype(BF16)
        for cp_ in ag_own(3) + ag_second(6):
            cp_.start()
    with jax.named_scope('t11_dqw'):
        for slot in range(chips):
            for core in range(2):
                if slot > 0:
                    dq_wait(slot, core)
        dq_wait(0, cp)
        wd_own.wait_recv()
        wd_rest.wait_recv()
    with jax.named_scope('t12_dxa'):
        dx_part(0)
    with jax.named_scope('t13_ag3'):
        ag_stage1(3)
        ag_stage1(6)
    with jax.named_scope('t14_dxa'):
        dx_part(1)
    with jax.named_scope('t15_ag3'):
        ag_stage2(3)
        ag_stage2(6)
    with jax.named_scope('t16_ag3'):
        ag_stage3(3)
        for xc in (cx, xright, xleft, xfar):
            ag_partner(3, xc)
    mrow = width // (2 * chips)
    krow = mrow // rows
    with jax.named_scope('t18_wk'):
        part = dot(xf[:, pl.ds(pl.multiple_of(me * mrow, mrow), mrow)], kvb[...], TN)
        wkp[...] = part.reshape(rows, krow, 2 * head_dim)

    def wk_copy(idx, blk, dev):
        return rcopy(wkp.at[blk], wkr.at[idx], wk_s.at[idx], wk_r.at[idx], dev)

    wk_copies = [wk_copy(0, yup, to_u), wk_copy(1, ydn, to_d), wk_copy(2, yfar, to_f)]
    for cp_ in wk_copies:
        cp_.start()
    with jax.named_scope('t19_dx2'):
        for xc in (cx, xright, xleft, xfar):
            ag_partner(5, xc)
        dx_part(2)
    with jax.named_scope('t19_ag6'):
        ag_stage3(6)
        for xc in (cx, xright, xleft, xfar):
            ag_partner(6, xc)
        dx_part(3)
        outs[0].start()
    with jax.named_scope('t19_y0f'):
        first, second = y_final(0)
        dwo_ref[:, 0:wcol] = first
        dwo_ref[:, wcol:] = second
        outs[4].start()
    with jax.named_scope('t20_y1f'):
        for idx, val in enumerate(y_final(1)):
            val = val.T
            for h in range(heads):
                dwq_ref[pl.ds(idx * wcol * heads + h, wcol, stride=heads), :] = val[:, h * head_dim:(h + 1) * head_dim]
        outs[1].start()
    with jax.named_scope('t21_wkf'):
        for cp_ in wk_copies:
            cp_.wait_recv()
        wk_sum = wkp[my] + wkr[0] + wkr[1] + wkr[2]
        dwk_ref[...] = wk_sum[:, 0:head_dim]
        dwv_ref[...] = wk_sum[:, head_dim:]
        outs[2].start()
        outs[3].start()

    with jax.named_scope('t22_sends'):
        for arr in (0, 1, 2, 3, 5, 6):
            for cp_ in ag_all_sends(arr):
                cp_.wait_send()
        for cp_ in ag_ring_first(4) + ag_second(4) + ag_relay(4) + wy_own + wy_relay + [wd_own, wd_rest]:
            cp_.wait_send()
        dq_copy(0, cx, cp).wait_send()
        for s, xc in ((1, xright), (2, xleft), (3, xfar)):
            for core in range(2):
                dq_copy(s, xc, core).wait_send()
        for xc in range(chips):
            kd_copy(xc).wait_send()
        for side in range(2):
            for kind in range(3):
                k_copy(side, kind).wait_send()
                for w in range(2):
                    y_copy(w, side, kind).wait_send()
        for cp_ in wk_copies:
            cp_.wait_send()
        for cp_ in outs:
            cp_.wait()


def copy_out(*refs):
    n = (len(refs) - 1) // 2
    sem = refs[-1]
    copies = [pltpu.make_async_copy(refs[k], refs[n + k], sem.at[k]) for k in range(n)]
    for cp_ in copies:
        cp_.start()
    for cp_ in copies:
        cp_.wait()


VMEM_LIMIT = 60 * 1000 * 1000


def solution(mesh):
    model_size = mesh.shape['model']
    data_size = mesh.shape['data']
    tok_spec = P(('pod', 'data'), 'model', None)
    chips = model_size // 2

    def device_step(x_loc, dy_loc, w_q, w_k, w_v, w_o):
        tok, width = x_loc.shape[1:]
        head_dim = w_k.shape[2]
        head_cols = w_q.shape[1] * head_dim
        assert chips == 4 and data_size == 4 and w_k.shape[0] == 1 and x_loc.shape[0] == 1
        seq = model_size * tok
        half = tok // 2
        heads = head_cols // head_dim
        wcol = width // (2 * data_size)
        krow = width // (model_size * data_size)
        cfg = (tok, width, head_cols, head_dim, chips, data_size)
        vm = pltpu.VMEM
        dma = pltpu.SemaphoreType.DMA
        scratch = [
            vm((seq, width), BF16), vm((seq, width), BF16), vm((2, chips, width, head_cols), BF16), vm((head_cols, width), BF16),
            vm((width, 2 * head_dim), BF16), vm((heads * width, head_dim), BF16), vm((heads * width, head_dim), F32),
            vm((seq, head_cols), BF16), vm((seq, 2 * head_dim), BF16), vm((seq, head_cols), BF16),
            vm((heads, seq, seq), F32), vm((heads, seq, seq), BF16), vm((seq, head_cols), BF16), vm((seq, head_cols), BF16),
            vm((seq, 2 * head_dim), BF16), vm((chips, 2, tok, head_cols), BF16),
            vm((model_size, tok, 2 * head_dim), F32), vm((chips, tok, 2 * head_dim), F32), vm((2, 3, half, 2 * head_dim), F32),
            vm((2, 2 * data_size, head_cols, wcol), F32), vm((2, 2, 3, head_cols, wcol), F32),
            vm((data_size, krow, 2 * head_dim), F32), vm((3, krow, 2 * head_dim), F32),
            vm((tok, width), BF16), vm((heads * 2 * wcol, head_dim), F32), vm((krow, head_dim), F32), vm((krow, head_dim), F32),
            vm((head_cols, 2 * wcol), F32),
            dma((20,)), dma((5,)), dma((7, 14)), dma((7, 16)), dma((6,)), dma((data_size, 2)), dma((2,)), dma((2,)),
            dma((chips, 2)), dma((chips, 2)),
            dma((chips,)), dma((chips,)), dma((2, 3)), dma((2, 3)), dma((2, 2, 3)), dma((2, 2, 3)), dma((3,)), dma((3,)),
        ]
        anyspec = pl.BlockSpec(memory_space=pl.ANY)
        vspec = pl.BlockSpec(memory_space=pltpu.VMEM)
        shapes = (jax.ShapeDtypeStruct((tok, width), BF16), jax.ShapeDtypeStruct((heads * 2 * wcol, head_dim), F32),
                  jax.ShapeDtypeStruct((krow, head_dim), F32), jax.ShapeDtypeStruct((krow, head_dim), F32),
                  jax.ShapeDtypeStruct((head_cols, 2 * wcol), F32))
        outs = pl.pallas_call(
            functools.partial(body, cfg),
            out_shape=tuple(pltpu.VMEM(a.shape, a.dtype) for a in shapes),
            in_specs=[anyspec] * 6,
            out_specs=(anyspec,) * 5,
            scratch_shapes=scratch,
            compiler_params=pltpu.CompilerParams(collective_id=0, has_side_effects=True, vmem_limit_bytes=VMEM_LIMIT),
            name='attn_bwd',
        )(x_loc[0], dy_loc[0], w_q.reshape(width * heads, head_dim), w_o.reshape(head_cols, width), w_k[0], w_v[0])
        dx, dwq, dwk, dwv, dwo = pl.pallas_call(
            copy_out,
            out_shape=shapes,
            in_specs=[vspec] * 5,
            out_specs=(anyspec,) * 5,
            scratch_shapes=[dma((5,))],
            compiler_params=pltpu.CompilerParams(vmem_limit_bytes=4 * 1024 * 1024),
            name='copy_out',
        )(*outs)
        return (dx[None], dwq.reshape(2 * wcol, heads, head_dim), dwk, dwv, dwo.reshape(heads, head_dim, 2 * wcol))

    kv_rows = P(('pod', 'model', 'data'), None)
    return jax.shard_map(device_step, mesh=mesh,
                         in_specs=(tok_spec, tok_spec, P(None, 'model', None), P(), P(), P('model', None, None)),
                         out_specs=(tok_spec, P(('pod', 'data'), 'model', None), kv_rows, kv_rows, P(('pod', 'model'), None, 'data')),
                         check_vma=False)
```

```python
import functools

import jax
import jax.numpy as jnp
from jax import lax
from jax.experimental import pallas as pl
from jax.experimental.pallas import tpu as pltpu
from jax.sharding import PartitionSpec as P

F32 = jnp.float32
BF16 = jnp.bfloat16
NN = (((1,), (0,)), ((), ()))
NT = (((1,), (1,)), ((), ()))
TN = (((0,), (0,)), ((), ()))


def dot(a, b, dims):
    return lax.dot_general(a, b, dims, preferred_element_type=F32)


def body(cfg, x_hbm, dy_hbm, wq_hbm, wo_hbm, wk_hbm, wv_hbm,
         dx_out, dwq_out, dwk_out, dwv_out, dwo_out,
         xf, yf, wqs, wo, wkv, wq2, wq2f, qf, kv, of, prob, dsf, dqf, dof, kvb, dqa,
         kvp, kvr, kr, dwa, yr, wkp, wkr, dx_ref, dwq_ref, dwk_ref, dwv_ref, dwo_ref,
         load_sem, out_sem, ag_s, ag_r, wy_s, wy_r, wd_s, wd_r, dq_s, dq_r,
         kd_s, kd_r, kr_s, kr_r, yr_s, yr_r, wk_s, wk_r):
    tok, width, head_cols, head_dim, chips, rows = cfg
    half = tok // 2
    chunk = 2 * tok
    seq = chips * chunk
    heads = head_cols // head_dim
    wcol = width // (2 * rows)
    hcol = width // 2
    qrow = width // 8
    scale = head_dim ** -0.5

    me = lax.axis_index('model')
    cx = me // 2
    cc = me % 2
    cp = 1 - cc
    xright = (cx + 1) % chips
    xleft = (cx + chips - 1) % chips
    xfar = (cx + 2) % chips
    my = lax.axis_index('data')
    yup = (my + 1) % rows
    ydn = (my + rows - 1) % rows
    yfar = (my + 2) % rows
    to_r = {'model': xright * 2 + cc}
    to_l = {'model': xleft * 2 + cc}
    to_p = {'model': cx * 2 + cp}
    to_u = {'data': yup}
    to_d = {'data': ydn}
    to_f = {'data': yfar}

    def rcopy(src, dst, ssem, rsem, dev):
        return pltpu.make_async_remote_copy(src_ref=src, dst_ref=dst, send_sem=ssem, recv_sem=rsem,
                                            device_id=dev, device_id_type=pl.DeviceIdType.MESH)

    def piece(arr, xc, core, h, base):
        r = pl.ds((xc * 2 + core) * tok + h * half, half)
        if arr == 0:
            return xf.at[r, :]
        if arr == 3:
            return kvb.at[r, :]
        slot = (xc + chips - base) % chips
        if arr == 4:
            return wqs.at[core, slot, pl.ds(my * qrow + h * (qrow // 2), qrow // 2), :]
        if arr >= 5:
            return wqs.at[core, slot, pl.ds((arr - 3) * (hcol // 2) + h * (hcol // 4), hcol // 4), :]
        return yf.at[r, pl.ds((arr - 1) * hcol, hcol)]

    def ag_slot(xc, base, h, cross):
        away = (xc + chips - base) % chips
        return 2 * chips - 2 + away if cross else 2 * away - 2 + h

    def ag_copy(arr, idx, xc, core, h, dev):
        base = {'r': xright, 'l': xleft, 'p': cx}[dev]
        return rcopy(piece(arr, xc, core, h, cx), piece(arr, xc, core, h, base), ag_s.at[arr],
                     ag_r.at[arr, ag_slot(xc, base, h, dev == 'p')], {'r': to_r, 'l': to_l, 'p': to_p}[dev])

    def ag_ring_first(arr):
        return [ag_copy(arr, 0, cx, cc, 0, 'r'), ag_copy(arr, 2, cx, cc, 1, 'l')]

    def ag_first(arr):
        return ag_ring_first(arr) + [ag_copy(arr, 4, cx, cc, 0, 'p'), ag_copy(arr, 5, cx, cc, 1, 'p')]

    def ag_second(arr):
        return [ag_copy(arr, 1, cx, cc, 1, 'r'), ag_copy(arr, 3, cx, cc, 0, 'l')]

    def ag_own(arr):
        return ag_first(arr) + ag_second(arr)

    def ag_relay(arr):
        return [ag_copy(arr, 6, xleft, cc, 0, 'r'), ag_copy(arr, 7, xright, cc, 1, 'l')]

    def ag_cross(arr, idx, xc, h):
        return ag_copy(arr, idx, xc, cc, h, 'p')

    def ag_wait(arr, xc, core, h):
        p = piece(arr, xc, core, h, cx)
        rcopy(p, p, ag_s.at[arr], ag_r.at[arr, ag_slot(xc, cx, h, False)], to_p).wait_recv()

    def ag_relays(arr):
        relays = ag_relay(arr)
        ag_wait(arr, xleft, cc, 0)
        relays[0].start()
        ag_wait(arr, xright, cc, 1)
        relays[1].start()

    def ag_stage1(arr):
        ag_relays(arr)
        ag_cross(arr, 8, xleft, 0).start()
        ag_cross(arr, 11, xright, 1).start()

    def ag_stage2(arr):
        ag_wait(arr, xright, cc, 0)
        ag_cross(arr, 10, xright, 0).start()
        ag_wait(arr, xleft, cc, 1)
        ag_cross(arr, 9, xleft, 1).start()

    def ag_stage3(arr):
        ag_wait(arr, xfar, cc, 0)
        ag_cross(arr, 12, xfar, 0).start()
        ag_wait(arr, xfar, cc, 1)
        ag_cross(arr, 13, xfar, 1).start()

    def ag_partner(arr, xc):
        r = pl.ds((xc * 2 + cp) * tok, tok)
        if arr == 0:
            p = xf.at[r, :]
        elif arr == 3:
            p = kvb.at[r, :]
        elif arr >= 5:
            p = wqs.at[cp, (xc + chips - cx) % chips, pl.ds((arr - 3) * (hcol // 2), hcol // 2), :]
        else:
            p = yf.at[r, pl.ds((arr - 1) * hcol, hcol)]
        rcopy(p, p, ag_s.at[arr], ag_r.at[arr, ag_slot(xc, cx, 0, True)], to_p).wait_recv()

    def ag_sent(arr):
        r = pl.ds(0, 7 * tok)
        p = {0: xf.at[r, :], 1: yf.at[r, pl.ds(0, hcol)], 2: yf.at[r, pl.ds(0, hcol)], 3: kvb.at[r, :],
             4: wqs.at[0, 0, pl.ds(0, 3 * qrow), :], 5: wqs.at[:, 0, pl.ds(0, 7 * qrow), :],
             6: wqs.at[:, 0, pl.ds(0, 7 * qrow), :]}[arr]
        rcopy(p, p, ag_s.at[arr], ag_r.at[arr, 0], to_p).wait_send()

    def wy_copy(idx, q, h, dev):
        p = wqs.at[cc, pl.ds(1, chips - 1), pl.ds(q * qrow + h * (qrow // 2), qrow // 2), :]
        return rcopy(p, p, wy_s.at[0], wy_r.at[idx], dev)

    wy_own = [wy_copy(0, my, 0, to_u), wy_copy(1, my, 1, to_d), wy_copy(2, my, 1, to_u), wy_copy(2, my, 0, to_d)]
    wy_relay = [wy_copy(2, ydn, 0, to_u), wy_copy(2, yup, 1, to_d)]

    def wy_pass():
        wy_copy(0, ydn, 0, to_u).wait_recv()
        wy_relay[0].start()
        wy_copy(1, yup, 1, to_u).wait_recv()
        wy_relay[1].start()

    def wy_total(count):
        p = wqs.at[cc, pl.ds(1, chips - 1), pl.ds(0, count * (qrow // 2)), :]
        return rcopy(p, p, wy_s.at[0], wy_r.at[2], to_u)

    wd_own = rcopy(wqs.at[cc, 0, pl.ds(0, hcol), :], wqs.at[cc, 0, pl.ds(0, hcol), :], wd_s.at[0], wd_r.at[0], to_p)
    wd_rest = rcopy(wqs.at[cc, pl.ds(1, chips - 1), pl.ds(0, hcol), :], wqs.at[cc, pl.ds(1, chips - 1), pl.ds(0, hcol), :],
                    wd_s.at[1], wd_r.at[1], to_p)

    def wy_end():
        wy_total(4).wait_recv()
        wd_rest.start()

    def dq_copy(xc, core):
        return rcopy(dqf.at[pl.ds((xc * 2 + core) * tok, tok), :], dqa.at[(cx + chips - xc) % chips, cc],
                     dq_s.at[0], dq_r.at[0], {'model': xc * 2 + core})

    dq_total = rcopy(dqf.at[pl.ds(0, 7 * tok), :], dqf.at[pl.ds(0, 7 * tok), :], dq_s.at[0], dq_r.at[0], to_p)

    def kd_copy(xc):
        return rcopy(kvp.at[xc * 2 + cp], kvr.at[xc], kd_s.at[0], kd_r.at[0], to_p)

    kd_total = rcopy(kvr, kvr, kd_s.at[0], kd_r.at[0], to_p)

    def kpart(xc, h):
        return kvp.at[xc * 2 + cc, pl.ds(h * half, half), :]

    def ring_src(kind, side):
        if kind == 0:
            return (xright, 1) if side == 0 else (xleft, 0)
        if kind == 1:
            return (xfar, 0) if side == 0 else (xfar, 1)
        return (xright, 0) if side == 0 else (xleft, 1)

    def k_copy(side, kind):
        xc, h = ring_src(kind, side)
        return rcopy(kpart(xc, h), kr.at[side, kind], kr_s.at[0], kr_r.at[side if kind == 1 else 2],
                     to_r if side == 0 else to_l)

    def k_pass():
        for side in range(2):
            k_copy(side, 1).wait_recv()
            xc, h = ring_src(2, side)
            ref = kpart(xc, h)
            ref[...] = ref[...] + kr[side, 1]
            k_copy(side, 2).start()

    order = ((yfar, 0), (yfar, 1), (yup, 1), (ydn, 0), (yup, 0), (ydn, 1), (my, 0), (my, 1))

    def y_blk(w, kind, side):
        pos = {(1, 0): 0, (1, 1): 1, (0, 0): 2, (0, 1): 3, (2, 0): 4, (2, 1): 5, (3, 0): 6, (3, 1): 7}[kind, side]
        if w == 0:
            return pos
        return order[pos][0] * 2 + order[pos][1]

    def y_copy(w, side, kind):
        return rcopy(dwa.at[w, y_blk(w, kind, side)], yr.at[w, side, kind], yr_s.at[0], yr_r.at[w, side if kind == 1 else 2],
                     to_u if side == 0 else to_d)

    def dw_block(w, kind, side):
        blk = y_blk(w, kind, side)
        if w == 0:
            dwa[0, blk] = dot(of[...], yf[:, blk * wcol:(blk + 1) * wcol], TN)
        else:
            dwa[1, blk] = dot(dqf[...], xf[:, pl.ds(pl.multiple_of(blk * wcol, wcol), wcol)], TN)

    def y_first(w, between=lambda: None):
        for kind in (1, 0):
            for side in range(2):
                dw_block(w, kind, side)
                y_copy(w, side, kind).start()
            if kind == 1:
                between()

    def y_rest(w):
        for kind in (2, 3):
            for side in range(2):
                dw_block(w, kind, side)

    def y_pass(w):
        for side in range(2):
            y_copy(w, side, 1).wait_recv()
            blk = y_blk(w, 2, side)
            dwa[w, blk] = dwa[w, blk] + yr[w, side, 1]
            y_copy(w, side, 2).start()

    def y_final(w):
        p = yr.at[w, :, pl.ds(0, 2)]
        rcopy(p, p, yr_s.at[0], yr_r.at[w, 2], to_u).wait_recv()
        first = dwa[w, y_blk(w, 3, 0)] + yr[w, 1, 0] + yr[w, 0, 2]
        second = dwa[w, y_blk(w, 3, 1)] + yr[w, 0, 0] + yr[w, 1, 2]
        return first, second

    own_rows = pl.ds(me * tok, tok)
    loads = [pltpu.make_async_copy(x_hbm, xf.at[own_rows, :], load_sem.at[0]),
             pltpu.make_async_copy(wq_hbm, wq2, load_sem.at[1]),
             pltpu.make_async_copy(wk_hbm, wkv.at[:, pl.ds(0, head_dim)], load_sem.at[2]),
             pltpu.make_async_copy(wv_hbm, wkv.at[:, pl.ds(head_dim, head_dim)], load_sem.at[2])]
    for pos, (dest, part) in enumerate(order):
        src = pl.ds(pl.multiple_of((dest * 2 + part) * wcol, wcol), wcol)
        dst = pl.ds(pos * wcol, wcol)
        loads.append(pltpu.make_async_copy(dy_hbm.at[:, src], yf.at[own_rows, dst], load_sem.at[3]))
        loads.append(pltpu.make_async_copy(wo_hbm.at[:, src], wo.at[:, dst], load_sem.at[4]))
    for cp_ in loads:
        cp_.start()
    barrier = pltpu.get_barrier_semaphore()
    peers = [{'model': (me + k) % (2 * chips)} for k in range(1, 2 * chips)]
    for dev in peers + [to_u, to_d, to_f]:
        pl.semaphore_signal(barrier, inc=1, device_id=dev, device_id_type=pl.DeviceIdType.MESH)
    with jax.named_scope('barrier'):
        pl.semaphore_wait(barrier, 2 * chips + 2)
    loads[0].wait()
    for cp_ in ag_first(0):
        cp_.start()
    with jax.named_scope('loadw'):
        loads[1].wait()
        for k, ref in ((2, wkv), (3, yf.at[own_rows, :]), (4, wo)):
            pltpu.make_async_copy(ref, ref, load_sem.at[k]).wait()
        step = 2 * width // 8

        @pl.loop(0, 8)
        def _(b):
            r2 = pl.ds(pl.multiple_of(b * step, step), step)
            wq2f[r2, :] = wq2[r2, :].astype(F32)
            r1 = pl.ds(pl.multiple_of(b * (step // 2), step // 2), step // 2)
            for h in range(heads):
                wqs[cc, 0, r1, h * head_dim:(h + 1) * head_dim] = wq2f[pl.ds(b * step + h, step // 2, stride=heads), :].astype(BF16)

    for cp_ in ag_ring_first(4) + ag_second(4) + ag_second(0):
        cp_.start()
    wd_own.start()

    def chunk_of(s):
        return (cx + s + s // 2 - 2 * (s // 3)) % chips

    @pl.loop(0, chips)
    def _(s):
        @pl.when(s == 0)
        def _():
            ag_partner(0, cx)

        @pl.when(s == 1)
        def _():
            with jax.named_scope('q1'):
                ag_relays(4)
                ag_stage1(0)
                for cp_ in ag_own(1):
                    cp_.start()
                ag_stage2(0)
            with jax.named_scope('q1w'):
                for xc, h in ((xleft, 1), (xright, 0), (xfar, 0), (xfar, 1)):
                    ag_wait(4, xc, cc, h)
                for cp_ in wy_own:
                    cp_.start()
            ag_partner(0, xright)

        @pl.when(s == 2)
        def _():
            ag_partner(0, xleft)

        @pl.when(s == 3)
        def _():
            ag_stage3(0)
            ag_partner(0, xfar)

        r = pl.ds(chunk_of(s) * chunk, chunk)
        xc = xf[r, :]
        qf[r, :] = dot(xc, wqs[cc, 0], NN).astype(BF16)
        kv[r, :] = dot(xc, wkv[...], NN).astype(BF16)

    @pl.loop(0, chips)
    def _(s):
        @pl.when(s == 1)
        def _():
            with jax.named_scope('f1'):
                ag_stage1(1)
                for cp_ in ag_own(2):
                    cp_.start()

        @pl.when(s == 2)
        def _():
            with jax.named_scope('f2'):
                wy_pass()
                ag_stage2(1)

        i = chunk_of(s)
        r = pl.ds(i * chunk, chunk)
        row_id = lax.broadcasted_iota(jnp.int32, (chunk, seq), 0) + i * chunk
        keep = row_id >= lax.broadcasted_iota(jnp.int32, (chunk, seq), 1)
        for h in range(heads):
            hc = pl.ds(h * head_dim, head_dim)
            sc = dot(qf[r, hc], kv[:, 0:head_dim], NT) * scale
            sc = jnp.where(keep, sc, -jnp.inf)
            ex = jnp.exp(sc - jnp.max(sc, axis=-1, keepdims=True))
            pr = ex * (1.0 / jnp.sum(ex, axis=-1, keepdims=True))
            prob[h, r, :] = pr
            of[r, hc] = dot(pr.astype(BF16), kv[:, head_dim:], NN).astype(BF16)

    def mid_relays():
        ag_stage1(2)
        for cp_ in ag_own(5):
            cp_.start()

    with jax.named_scope('b0'):
        ag_stage3(1)
        ag_partner(1, cx)
        ag_partner(2, cx)

    @pl.loop(0, chips)
    def _(s):
        @pl.when(s == 1)
        def _():
            with jax.named_scope('b1'):
                for xc in (xright, xleft, xfar):
                    ag_partner(1, xc)
            with jax.named_scope('b1y'):
                y_first(0, mid_relays)
            with jax.named_scope('b1w'):
                ag_stage2(2)
                wy_end()
                ag_partner(2, xright)

        @pl.when(s == 2)
        def _():
            with jax.named_scope('b2'):
                ag_stage3(2)
                ag_partner(2, xleft)

        @pl.when(s == 3)
        def _():
            with jax.named_scope('b3'):
                ag_partner(2, xfar)

        with jax.named_scope('b_comp'):
            i = chunk_of(s)
            r = pl.ds(i * chunk, chunk)
            oc = of[r, :]
            do = dot(yf[r, :], wo[...], NT).astype(BF16)
            dof[r, :] = do
            od = do.astype(F32) * oc.astype(F32)
            for h in range(heads):
                hs = slice(h * head_dim, (h + 1) * head_dim)
                dp = dot(do[:, hs], kv[:, head_dim:], NT)
                ds = (prob[h, r, :] * (dp - jnp.sum(od[:, hs], axis=-1, keepdims=True))).astype(BF16)
                dsf[h, r, :] = ds
                dqf[r, hs] = (dot(ds, kv[:, 0:head_dim], NN) * scale).astype(BF16)

        @pl.when(s == 0)
        def _():
            dqa[0, cc] = dqf[own_rows, :]
            dq_copy(cx, cp).start()

        @pl.when(s > 0)
        def _():
            for core in range(2):
                dq_copy(i, core).start()

    with jax.named_scope('t00_dkv'):
        for kc in range(chips):
            ks = slice(kc * chunk, (kc + 1) * chunk)
            qs = slice(kc * chunk, seq)
            dk = jnp.zeros((chunk, head_dim), F32)
            dv = jnp.zeros((chunk, head_dim), F32)
            for h in range(heads):
                hs = slice(h * head_dim, (h + 1) * head_dim)
                dk = dk + dot(dsf[h, qs, ks], qf[qs, hs], TN)
                dv = dv + dot(prob[h, qs, ks].astype(BF16), dof[qs, hs], TN)
            kvp[2 * kc:2 * kc + 2, :, 0:head_dim] = (dk * scale).reshape(2, tok, head_dim)
            kvp[2 * kc:2 * kc + 2, :, head_dim:] = dv.reshape(2, tok, head_dim)
        for xc in range(chips):
            kd_copy(xc).start()
    with jax.named_scope('t00_y1'):
        y_first(1)

    own = cx * 2 + cc

    def dx_part(j):
        cols = slice(j * (hcol // 2), (j + 1) * (hcol // 2))
        acc = dot(kvb[own_rows, :], wkv[cols, :], NT)
        for slot in range(chips):
            for core in range(2):
                acc = acc + dot(dqa[slot, core], wqs[core, slot, cols, :], NT)
        dx_ref[:, cols] = acc.astype(BF16)

    def out_copy(k, src, dst):
        return pltpu.make_async_copy(src, dst, out_sem.at[k])

    outs = [out_copy(0, dx_ref, dx_out), out_copy(1, dwq_ref, dwq_out), out_copy(2, dwk_ref, dwk_out),
            out_copy(3, dwv_ref, dwv_out), out_copy(4, dwo_ref, dwo_out)]

    with jax.named_scope('t03_kd'):
        kd_total.wait_recv()
        for xc in range(chips):
            blk = xc * 2 + cc
            kvp[blk] = kvp[blk] + kvr[xc]
        for kind in (1, 0):
            for side in range(2):
                k_copy(side, kind).start()
    with jax.named_scope('t04_ag5'):
        ag_stage1(5)
    with jax.named_scope('t05_y0'):
        y_rest(0)
        y_pass(0)
    with jax.named_scope('t06_ag5'):
        ag_stage2(5)
    with jax.named_scope('t07_kpass'):
        k_pass()
        for cp_ in ag_first(6):
            cp_.start()
    with jax.named_scope('t08_y1'):
        y_rest(1)
        y_pass(1)
    with jax.named_scope('t09_ag5'):
        ag_stage3(5)
    with jax.named_scope('t10_kfin'):
        p = kr.at[:, pl.ds(0, 2)]
        rcopy(p, p, kr_s.at[0], kr_r.at[2], to_r).wait_recv()
        kvb[pl.ds(me * tok, half), :] = (kvp[own, 0:half, :] + kr[1, 0] + kr[0, 2]).astype(BF16)
        kvb[pl.ds(me * tok + half, half), :] = (kvp[own, half:, :] + kr[0, 0] + kr[1, 2]).astype(BF16)
        for cp_ in ag_own(3) + ag_second(6):
            cp_.start()
    with jax.named_scope('t11_dqw'):
        dq_total.wait_recv()
        wd_own.wait_recv()
        wd_rest.wait_recv()
    with jax.named_scope('t12_dxa'):
        dx_part(0)
    with jax.named_scope('t13_ag3'):
        ag_stage1(3)
        ag_stage1(6)
    with jax.named_scope('t14_dxa'):
        dx_part(1)
    with jax.named_scope('t15_ag3'):
        ag_stage2(3)
        ag_stage2(6)
    with jax.named_scope('t16_ag3'):
        ag_stage3(3)
        for xc in (cx, xright, xleft, xfar):
            ag_partner(3, xc)
    mrow = width // (2 * chips)
    krow = mrow // rows
    with jax.named_scope('t18_wk'):
        part = dot(xf[:, pl.ds(pl.multiple_of(me * mrow, mrow), mrow)], kvb[...], TN)
        wkp[...] = part.reshape(rows, krow, 2 * head_dim)

    def wk_copy(idx, blk, dev):
        return rcopy(wkp.at[blk], wkr.at[idx], wk_s.at[0], wk_r.at[0], dev)

    wk_total = rcopy(wkr, wkr, wk_s.at[0], wk_r.at[0], to_u)

    wk_copies = [wk_copy(0, yup, to_u), wk_copy(1, ydn, to_d), wk_copy(2, yfar, to_f)]
    for cp_ in wk_copies:
        cp_.start()
    with jax.named_scope('t19_dx2'):
        for xc in (cx, xright, xleft, xfar):
            ag_partner(5, xc)
        dx_part(2)
    with jax.named_scope('t19_ag6'):
        ag_stage3(6)
        for xc in (cx, xright, xleft, xfar):
            ag_partner(6, xc)
        dx_part(3)
        outs[0].start()
    with jax.named_scope('t19_y0f'):
        first, second = y_final(0)
        dwo_ref[:, 0:wcol] = first
        dwo_ref[:, wcol:] = second
        outs[4].start()
    with jax.named_scope('t20_y1f'):
        for idx, val in enumerate(y_final(1)):
            val = val.T
            for h in range(heads):
                dwq_ref[pl.ds(idx * wcol * heads + h, wcol, stride=heads), :] = val[:, h * head_dim:(h + 1) * head_dim]
        outs[1].start()
    with jax.named_scope('t21_wkf'):
        wk_total.wait_recv()
        wk_sum = wkp[my] + wkr[0] + wkr[1] + wkr[2]
        dwk_ref[...] = wk_sum[:, 0:head_dim]
        dwv_ref[...] = wk_sum[:, head_dim:]
        outs[2].start()
        outs[3].start()

    with jax.named_scope('t22_sends'):
        for arr in range(7):
            ag_sent(arr)
        wd_own.wait_send()
        wd_rest.wait_send()
        wy_total(6).wait_send()
        dq_total.wait_send()
        kd_total.wait_send()
        rcopy(kvp.at[pl.ds(0, 3)], kvp.at[pl.ds(0, 3)], kr_s.at[0], kr_r.at[0], to_r).wait_send()
        rcopy(dwa.at[:, pl.ds(0, 6)], dwa.at[:, pl.ds(0, 6)], yr_s.at[0], yr_r.at[0, 0], to_u).wait_send()
        wk_total.wait_send()
        for cp_ in outs:
            cp_.wait()


def copy_out(*refs):
    n = (len(refs) - 1) // 2
    sem = refs[-1]
    copies = [pltpu.make_async_copy(refs[k], refs[n + k], sem.at[k]) for k in range(n)]
    for cp_ in copies:
        cp_.start()
    for cp_ in copies:
        cp_.wait()


VMEM_LIMIT = 60 * 1000 * 1000


def solution(mesh):
    model_size = mesh.shape['model']
    data_size = mesh.shape['data']
    tok_spec = P(('pod', 'data'), 'model', None)
    chips = model_size // 2

    def device_step(x_loc, dy_loc, w_q, w_k, w_v, w_o):
        tok, width = x_loc.shape[1:]
        head_dim = w_k.shape[2]
        head_cols = w_q.shape[1] * head_dim
        assert chips == 4 and data_size == 4 and w_k.shape[0] == 1 and x_loc.shape[0] == 1
        seq = model_size * tok
        half = tok // 2
        heads = head_cols // head_dim
        wcol = width // (2 * data_size)
        krow = width // (model_size * data_size)
        cfg = (tok, width, head_cols, head_dim, chips, data_size)
        vm = pltpu.VMEM
        dma = pltpu.SemaphoreType.DMA
        scratch = [
            vm((seq, width), BF16), vm((seq, width), BF16), vm((2, chips, width, head_cols), BF16), vm((head_cols, width), BF16),
            vm((width, 2 * head_dim), BF16), vm((heads * width, head_dim), BF16), vm((heads * width, head_dim), F32),
            vm((seq, head_cols), BF16), vm((seq, 2 * head_dim), BF16), vm((seq, head_cols), BF16),
            vm((heads, seq, seq), F32), vm((heads, seq, seq), BF16), vm((seq, head_cols), BF16), vm((seq, head_cols), BF16),
            vm((seq, 2 * head_dim), BF16), vm((chips, 2, tok, head_cols), BF16),
            vm((model_size, tok, 2 * head_dim), F32), vm((chips, tok, 2 * head_dim), F32), vm((2, 3, half, 2 * head_dim), F32),
            vm((2, 2 * data_size, head_cols, wcol), F32), vm((2, 2, 3, head_cols, wcol), F32),
            vm((data_size, krow, 2 * head_dim), F32), vm((3, krow, 2 * head_dim), F32),
            vm((tok, width), BF16), vm((heads * 2 * wcol, head_dim), F32), vm((krow, head_dim), F32), vm((krow, head_dim), F32),
            vm((head_cols, 2 * wcol), F32),
            dma((5,)), dma((5,)), dma((7,)), dma((7, 10)), dma((1,)), dma((3,)), dma((2,)), dma((2,)),
            dma((1,)), dma((1,)), dma((1,)), dma((1,)), dma((1,)), dma((3,)), dma((1,)), dma((2, 3)), dma((1,)), dma((1,)),
        ]
        anyspec = pl.BlockSpec(memory_space=pl.ANY)
        vspec = pl.BlockSpec(memory_space=pltpu.VMEM)
        shapes = (jax.ShapeDtypeStruct((tok, width), BF16), jax.ShapeDtypeStruct((heads * 2 * wcol, head_dim), F32),
                  jax.ShapeDtypeStruct((krow, head_dim), F32), jax.ShapeDtypeStruct((krow, head_dim), F32),
                  jax.ShapeDtypeStruct((head_cols, 2 * wcol), F32))
        outs = pl.pallas_call(
            functools.partial(body, cfg),
            out_shape=tuple(pltpu.VMEM(a.shape, a.dtype) for a in shapes),
            in_specs=[anyspec] * 6,
            out_specs=(anyspec,) * 5,
            scratch_shapes=scratch,
            compiler_params=pltpu.CompilerParams(collective_id=0, has_side_effects=True, vmem_limit_bytes=VMEM_LIMIT),
            name='attn_bwd',
        )(x_loc[0], dy_loc[0], w_q.reshape(width * heads, head_dim), w_o.reshape(head_cols, width), w_k[0], w_v[0])
        dx, dwq, dwk, dwv, dwo = pl.pallas_call(
            copy_out,
            out_shape=shapes,
            in_specs=[vspec] * 5,
            out_specs=(anyspec,) * 5,
            scratch_shapes=[dma((5,))],
            compiler_params=pltpu.CompilerParams(vmem_limit_bytes=4 * 1024 * 1024),
            name='copy_out',
        )(*outs)
        return (dx[None], dwq.reshape(2 * wcol, heads, head_dim), dwk, dwv, dwo.reshape(heads, head_dim, 2 * wcol))

    kv_rows = P(('pod', 'model', 'data'), None)
    return jax.shard_map(device_step, mesh=mesh,
                         in_specs=(tok_spec, tok_spec, P(None, 'model', None), P(), P(), P('model', None, None)),
                         out_specs=(tok_spec, P(('pod', 'data'), 'model', None), kv_rows, kv_rows, P(('pod', 'model'), None, 'data')),
                         check_vma=False)
```

```python
import functools

import jax
import jax.numpy as jnp
from jax import lax
from jax.experimental import pallas as pl
from jax.experimental.pallas import tpu as pltpu
from jax.sharding import PartitionSpec as P

F32 = jnp.float32
BF16 = jnp.bfloat16
NN = (((1,), (0,)), ((), ()))
NT = (((1,), (1,)), ((), ()))
TN = (((0,), (0,)), ((), ()))


def dot(a, b, dims):
    return lax.dot_general(a, b, dims, preferred_element_type=F32)


def body(cfg, x_hbm, dy_hbm, wq_hbm, wo_hbm, wk_hbm, wv_hbm,
         dx_out, dwq_out, dwk_out, dwv_out, dwo_out,
         xf, yf, wqs, wo, wkv, wq2, wq2f, qf, kv, of, prob, dsf, dqf, dof, kvb, dqa,
         kvp, kvr, kr, dwa, yr, wkp, wkr, dxacc, dx_ref, dwq_ref, dwk_ref, dwv_ref, dwo_ref,
         load_sem, out_sem, ag_s, ag_r, wy_s, wy_r, wd_s, wd_r, dq_s, dq_r,
         kd_s, kd_r, kr_s, kr_r, yr_s, yr_r, wk_s, wk_r):
    tok, width, head_cols, head_dim, chips, rows = cfg
    half = tok // 2
    chunk = 2 * tok
    seq = chips * chunk
    heads = head_cols // head_dim
    wcol = width // (2 * rows)
    hcol = width // 2
    qrow = width // 8
    scale = head_dim ** -0.5

    me = lax.axis_index('model')
    cx = me // 2
    cc = me % 2
    cp = 1 - cc
    xright = (cx + 1) % chips
    xleft = (cx + chips - 1) % chips
    xfar = (cx + 2) % chips
    my = lax.axis_index('data')
    yup = (my + 1) % rows
    ydn = (my + rows - 1) % rows
    yfar = (my + 2) % rows
    to_r = {'model': xright * 2 + cc}
    to_l = {'model': xleft * 2 + cc}
    to_p = {'model': cx * 2 + cp}
    to_u = {'data': yup}
    to_d = {'data': ydn}
    to_f = {'data': yfar}

    def rcopy(src, dst, ssem, rsem, dev):
        return pltpu.make_async_remote_copy(src_ref=src, dst_ref=dst, send_sem=ssem, recv_sem=rsem,
                                            device_id=dev, device_id_type=pl.DeviceIdType.MESH)

    def piece(arr, xc, core, h, base):
        r = pl.ds((xc * 2 + core) * tok + h * half, half)
        if arr == 0:
            return xf.at[r, :]
        if arr == 3:
            return kvb.at[r, :]
        slot = (xc + chips - base) % chips
        if arr == 4:
            return wqs.at[core, slot, pl.ds(my * qrow + h * (qrow // 2), qrow // 2), :]
        if arr >= 5:
            return wqs.at[core, slot, pl.ds((arr - 3) * (hcol // 2) + h * (hcol // 4), hcol // 4), :]
        return yf.at[r, pl.ds((arr - 1) * hcol, hcol)]

    def ag_slot(xc, base, h, cross):
        away = (xc + chips - base) % chips
        return 2 * chips - 2 + away if cross else 2 * away - 2 + h

    def ag_copy(arr, idx, xc, core, h, dev):
        base = {'r': xright, 'l': xleft, 'p': cx}[dev]
        return rcopy(piece(arr, xc, core, h, cx), piece(arr, xc, core, h, base), ag_s.at[arr],
                     ag_r.at[arr, ag_slot(xc, base, h, dev == 'p')], {'r': to_r, 'l': to_l, 'p': to_p}[dev])

    def ag_ring_first(arr):
        return [ag_copy(arr, 0, cx, cc, 0, 'r'), ag_copy(arr, 2, cx, cc, 1, 'l')]

    def ag_first(arr):
        return ag_ring_first(arr) + [ag_copy(arr, 4, cx, cc, 0, 'p'), ag_copy(arr, 5, cx, cc, 1, 'p')]

    def ag_second(arr):
        return [ag_copy(arr, 1, cx, cc, 1, 'r'), ag_copy(arr, 3, cx, cc, 0, 'l')]

    def ag_own(arr):
        return ag_first(arr) + ag_second(arr)

    def ag_relay(arr):
        return [ag_copy(arr, 6, xleft, cc, 0, 'r'), ag_copy(arr, 7, xright, cc, 1, 'l')]

    def ag_cross(arr, idx, xc, h):
        return ag_copy(arr, idx, xc, cc, h, 'p')

    def ag_wait(arr, xc, core, h):
        p = piece(arr, xc, core, h, cx)
        rcopy(p, p, ag_s.at[arr], ag_r.at[arr, ag_slot(xc, cx, h, False)], to_p).wait_recv()

    def ag_relays(arr):
        relays = ag_relay(arr)
        ag_wait(arr, xleft, cc, 0)
        relays[0].start()
        ag_wait(arr, xright, cc, 1)
        relays[1].start()

    def ag_stage1(arr):
        ag_relays(arr)
        ag_cross(arr, 8, xleft, 0).start()
        ag_cross(arr, 11, xright, 1).start()

    def ag_stage2(arr):
        ag_wait(arr, xright, cc, 0)
        ag_cross(arr, 10, xright, 0).start()
        ag_wait(arr, xleft, cc, 1)
        ag_cross(arr, 9, xleft, 1).start()

    def ag_stage3(arr):
        ag_wait(arr, xfar, cc, 0)
        ag_cross(arr, 12, xfar, 0).start()
        ag_wait(arr, xfar, cc, 1)
        ag_cross(arr, 13, xfar, 1).start()

    def ag_partner(arr, xc):
        r = pl.ds((xc * 2 + cp) * tok, tok)
        if arr == 0:
            p = xf.at[r, :]
        elif arr == 3:
            p = kvb.at[r, :]
        elif arr >= 5:
            p = wqs.at[cp, (xc + chips - cx) % chips, pl.ds((arr - 3) * (hcol // 2), hcol // 2), :]
        else:
            p = yf.at[r, pl.ds((arr - 1) * hcol, hcol)]
        rcopy(p, p, ag_s.at[arr], ag_r.at[arr, ag_slot(xc, cx, 0, True)], to_p).wait_recv()

    def ag_sent(arr):
        r = pl.ds(0, 7 * tok)
        p = {0: xf.at[r, :], 1: yf.at[r, pl.ds(0, hcol)], 2: yf.at[r, pl.ds(0, hcol)], 3: kvb.at[r, :],
             4: wqs.at[0, 0, pl.ds(0, 3 * qrow), :], 5: wqs.at[:, 0, pl.ds(0, 7 * qrow), :],
             6: wqs.at[:, 0, pl.ds(0, 7 * qrow), :]}[arr]
        rcopy(p, p, ag_s.at[arr], ag_r.at[arr, 0], to_p).wait_send()

    def wy_copy(idx, q, h, dev):
        p = wqs.at[cc, pl.ds(1, chips - 1), pl.ds(q * qrow + h * (qrow // 2), qrow // 2), :]
        return rcopy(p, p, wy_s.at[0], wy_r.at[idx], dev)

    wy_own = [wy_copy(0, my, 0, to_u), wy_copy(1, my, 1, to_d), wy_copy(2, my, 1, to_u), wy_copy(2, my, 0, to_d)]
    wy_relay = [wy_copy(2, ydn, 0, to_u), wy_copy(2, yup, 1, to_d)]

    def wy_pass():
        wy_copy(0, ydn, 0, to_u).wait_recv()
        wy_relay[0].start()
        wy_copy(1, yup, 1, to_u).wait_recv()
        wy_relay[1].start()

    def wy_total(count):
        p = wqs.at[cc, pl.ds(1, chips - 1), pl.ds(0, count * (qrow // 2)), :]
        return rcopy(p, p, wy_s.at[0], wy_r.at[2], to_u)

    wd_own = rcopy(wqs.at[cc, 0, pl.ds(0, hcol), :], wqs.at[cc, 0, pl.ds(0, hcol), :], wd_s.at[0], wd_r.at[0], to_p)
    wd_rest = rcopy(wqs.at[cc, pl.ds(1, chips - 1), pl.ds(0, hcol), :], wqs.at[cc, pl.ds(1, chips - 1), pl.ds(0, hcol), :],
                    wd_s.at[1], wd_r.at[1], to_p)

    def wy_end():
        wy_total(4).wait_recv()
        wd_rest.start()

    def dq_copy(xc, core):
        return rcopy(dqf.at[pl.ds((xc * 2 + core) * tok, tok), :], dqa.at[(cx + chips - xc) % chips, cc],
                     dq_s.at[0], dq_r.at[0], {'model': xc * 2 + core})

    dq_total = rcopy(dqf.at[pl.ds(0, 7 * tok), :], dqf.at[pl.ds(0, 7 * tok), :], dq_s.at[0], dq_r.at[0], to_p)

    def kd_copy(xc):
        return rcopy(kvp.at[xc * 2 + cp], kvr.at[xc], kd_s.at[0], kd_r.at[0], to_p)

    kd_total = rcopy(kvr, kvr, kd_s.at[0], kd_r.at[0], to_p)

    def kpart(xc, h):
        return kvp.at[xc * 2 + cc, pl.ds(h * half, half), :]

    def ring_src(kind, side):
        if kind == 0:
            return (xright, 1) if side == 0 else (xleft, 0)
        if kind == 1:
            return (xfar, 0) if side == 0 else (xfar, 1)
        return (xright, 0) if side == 0 else (xleft, 1)

    def k_copy(side, kind):
        xc, h = ring_src(kind, side)
        return rcopy(kpart(xc, h), kr.at[side, kind], kr_s.at[0], kr_r.at[side if kind == 1 else 2],
                     to_r if side == 0 else to_l)

    def k_pass():
        for side in range(2):
            k_copy(side, 1).wait_recv()
            xc, h = ring_src(2, side)
            ref = kpart(xc, h)
            ref[...] = ref[...] + kr[side, 1]
            k_copy(side, 2).start()

    order = ((yfar, 0), (yfar, 1), (yup, 1), (ydn, 0), (yup, 0), (ydn, 1), (my, 0), (my, 1))

    def y_blk(w, kind, side):
        pos = {(1, 0): 0, (1, 1): 1, (0, 0): 2, (0, 1): 3, (2, 0): 4, (2, 1): 5, (3, 0): 6, (3, 1): 7}[kind, side]
        if w == 0:
            return pos
        return order[pos][0] * 2 + order[pos][1]

    def y_copy(w, side, kind):
        return rcopy(dwa.at[w, y_blk(w, kind, side)], yr.at[w, side, kind], yr_s.at[0], yr_r.at[w, side if kind == 1 else 2],
                     to_u if side == 0 else to_d)

    def dw_block(w, kind, side):
        blk = y_blk(w, kind, side)
        if w == 0:
            dwa[0, blk] = dot(of[...], yf[:, blk * wcol:(blk + 1) * wcol], TN)
        else:
            dwa[1, blk] = dot(dqf[...], xf[:, pl.ds(pl.multiple_of(blk * wcol, wcol), wcol)], TN)

    def y_first(w, between=lambda: None):
        for kind in (1, 0):
            for side in range(2):
                dw_block(w, kind, side)
                y_copy(w, side, kind).start()
            if kind == 1:
                between()

    def dw_blocks(w, kind):
        for side in range(2):
            dw_block(w, kind, side)

    def y_pass(w):
        for side in range(2):
            y_copy(w, side, 1).wait_recv()
            blk = y_blk(w, 2, side)
            dwa[w, blk] = dwa[w, blk] + yr[w, side, 1]
            y_copy(w, side, 2).start()

    def y_final(w):
        p = yr.at[w, :, pl.ds(0, 2)]
        rcopy(p, p, yr_s.at[0], yr_r.at[w, 2], to_u).wait_recv()
        first = dwa[w, y_blk(w, 3, 0)] + yr[w, 1, 0] + yr[w, 0, 2]
        second = dwa[w, y_blk(w, 3, 1)] + yr[w, 0, 0] + yr[w, 1, 2]
        return first, second

    own_rows = pl.ds(me * tok, tok)
    loads = [pltpu.make_async_copy(x_hbm, xf.at[own_rows, :], load_sem.at[0]),
             pltpu.make_async_copy(wq_hbm, wq2, load_sem.at[1]),
             pltpu.make_async_copy(wk_hbm, wkv.at[:, pl.ds(0, head_dim)], load_sem.at[2]),
             pltpu.make_async_copy(wv_hbm, wkv.at[:, pl.ds(head_dim, head_dim)], load_sem.at[2])]
    for pos, (dest, part) in enumerate(order):
        src = pl.ds(pl.multiple_of((dest * 2 + part) * wcol, wcol), wcol)
        dst = pl.ds(pos * wcol, wcol)
        loads.append(pltpu.make_async_copy(dy_hbm.at[:, src], yf.at[own_rows, dst], load_sem.at[3]))
        loads.append(pltpu.make_async_copy(wo_hbm.at[:, src], wo.at[:, dst], load_sem.at[4]))
    for cp_ in loads:
        cp_.start()
    barrier = pltpu.get_barrier_semaphore()
    peers = [{'model': (me + k) % (2 * chips)} for k in range(1, 2 * chips)]
    for dev in peers + [to_u, to_d, to_f]:
        pl.semaphore_signal(barrier, inc=1, device_id=dev, device_id_type=pl.DeviceIdType.MESH)
    with jax.named_scope('barrier'):
        pl.semaphore_wait(barrier, 2 * chips + 2)
    loads[0].wait()
    for cp_ in ag_first(0):
        cp_.start()
    with jax.named_scope('loadw'):
        loads[1].wait()
        for k, ref in ((2, wkv), (3, yf.at[own_rows, :]), (4, wo)):
            pltpu.make_async_copy(ref, ref, load_sem.at[k]).wait()
        step = 2 * width // 8

        @pl.loop(0, 8)
        def _(b):
            r2 = pl.ds(pl.multiple_of(b * step, step), step)
            wq2f[r2, :] = wq2[r2, :].astype(F32)
            r1 = pl.ds(pl.multiple_of(b * (step // 2), step // 2), step // 2)
            for h in range(heads):
                wqs[cc, 0, r1, h * head_dim:(h + 1) * head_dim] = wq2f[pl.ds(b * step + h, step // 2, stride=heads), :].astype(BF16)

    for cp_ in ag_ring_first(4) + ag_second(4) + ag_second(0):
        cp_.start()
    wd_own.start()

    def chunk_of(s):
        return (cx + s + s // 2 - 2 * (s // 3)) % chips

    @pl.loop(0, chips)
    def _(s):
        @pl.when(s == 0)
        def _():
            ag_partner(0, cx)

        @pl.when(s == 1)
        def _():
            with jax.named_scope('q1'):
                ag_relays(4)
                ag_stage1(0)
                for cp_ in ag_own(1):
                    cp_.start()
                ag_stage2(0)
            with jax.named_scope('q1w'):
                for xc, h in ((xleft, 1), (xright, 0), (xfar, 0), (xfar, 1)):
                    ag_wait(4, xc, cc, h)
                for cp_ in wy_own:
                    cp_.start()
            ag_partner(0, xright)

        @pl.when(s == 2)
        def _():
            ag_partner(0, xleft)

        @pl.when(s == 3)
        def _():
            ag_stage3(0)
            ag_partner(0, xfar)

        r = pl.ds(chunk_of(s) * chunk, chunk)
        xc = xf[r, :]
        qf[r, :] = dot(xc, wqs[cc, 0], NN).astype(BF16)
        kv[r, :] = dot(xc, wkv[...], NN).astype(BF16)

    @pl.loop(0, chips)
    def _(s):
        @pl.when(s == 1)
        def _():
            with jax.named_scope('f1'):
                ag_stage1(1)
                for cp_ in ag_own(2):
                    cp_.start()

        @pl.when(s == 2)
        def _():
            with jax.named_scope('f2'):
                wy_pass()
                ag_stage2(1)

        i = chunk_of(s)
        r = pl.ds(i * chunk, chunk)
        row_id = lax.broadcasted_iota(jnp.int32, (chunk, seq), 0) + i * chunk
        keep = row_id >= lax.broadcasted_iota(jnp.int32, (chunk, seq), 1)
        for h in range(heads):
            hc = pl.ds(h * head_dim, head_dim)
            sc = dot(qf[r, hc], kv[:, 0:head_dim], NT) * scale
            sc = jnp.where(keep, sc, -jnp.inf)
            ex = jnp.exp(sc - jnp.max(sc, axis=-1, keepdims=True))
            pr = ex * (1.0 / jnp.sum(ex, axis=-1, keepdims=True))
            prob[h, r, :] = pr
            of[r, hc] = dot(pr.astype(BF16), kv[:, head_dim:], NN).astype(BF16)

    def mid_relays():
        ag_stage1(2)
        for cp_ in ag_own(5):
            cp_.start()

    with jax.named_scope('b0'):
        ag_stage3(1)
        ag_partner(1, cx)
        ag_partner(2, cx)

    @pl.loop(0, chips)
    def _(s):
        @pl.when(s == 1)
        def _():
            with jax.named_scope('b1'):
                for xc in (xright, xleft, xfar):
                    ag_partner(1, xc)
            with jax.named_scope('b1y'):
                y_first(0, mid_relays)
            with jax.named_scope('b1w'):
                ag_stage2(2)
                wy_end()
                ag_partner(2, xright)

        @pl.when(s == 2)
        def _():
            with jax.named_scope('b2'):
                ag_stage3(2)
                ag_partner(2, xleft)

        @pl.when(s == 3)
        def _():
            with jax.named_scope('b3'):
                ag_partner(2, xfar)

        with jax.named_scope('b_comp'):
            i = chunk_of(s)
            r = pl.ds(i * chunk, chunk)
            oc = of[r, :]
            do = dot(yf[r, :], wo[...], NT).astype(BF16)
            dof[r, :] = do
            od = do.astype(F32) * oc.astype(F32)
            for h in range(heads):
                hs = slice(h * head_dim, (h + 1) * head_dim)
                dp = dot(do[:, hs], kv[:, head_dim:], NT)
                ds = (prob[h, r, :] * (dp - jnp.sum(od[:, hs], axis=-1, keepdims=True))).astype(BF16)
                dsf[h, r, :] = ds
                dqf[r, hs] = (dot(ds, kv[:, 0:head_dim], NN) * scale).astype(BF16)

        @pl.when(s == 0)
        def _():
            dqa[0, cc] = dqf[own_rows, :]
            dq_copy(cx, cp).start()

        @pl.when(s > 0)
        def _():
            for core in range(2):
                dq_copy(i, core).start()

    with jax.named_scope('t00_y0'):
        dw_blocks(0, 2)
        y_pass(0)
    with jax.named_scope('t00_dkv'):
        for kc in range(chips):
            ks = slice(kc * chunk, (kc + 1) * chunk)
            qs = slice(kc * chunk, seq)
            dk = jnp.zeros((chunk, head_dim), F32)
            dv = jnp.zeros((chunk, head_dim), F32)
            for h in range(heads):
                hs = slice(h * head_dim, (h + 1) * head_dim)
                dk = dk + dot(dsf[h, qs, ks], qf[qs, hs], TN)
                dv = dv + dot(prob[h, qs, ks].astype(BF16), dof[qs, hs], TN)
            kvp[2 * kc:2 * kc + 2, :, 0:head_dim] = (dk * scale).reshape(2, tok, head_dim)
            kvp[2 * kc:2 * kc + 2, :, head_dim:] = dv.reshape(2, tok, head_dim)
        for xc in range(chips):
            kd_copy(xc).start()

    def kd_ring():
        kd_total.wait_recv()
        for xc in range(chips):
            blk = xc * 2 + cc
            kvp[blk] = kvp[blk] + kvr[xc]
        for kind in (1, 0):
            for side in range(2):
                k_copy(side, kind).start()

    with jax.named_scope('t00_y1'):
        y_first(1, kd_ring)

    own = cx * 2 + cc

    def dx_near(j):
        cols = slice(j * (hcol // 2), (j + 1) * (hcol // 2))
        acc = dot(kvb[own_rows, :], wkv[cols, :], NT)
        for slot in (0, 1, chips - 1):
            for core in range(2):
                acc = acc + dot(dqa[slot, core], wqs[core, slot, cols, :], NT)
        return acc

    def dx_far(j, acc):
        cols = slice(j * (hcol // 2), (j + 1) * (hcol // 2))
        for core in range(2):
            acc = acc + dot(dqa[2, core], wqs[core, 2, cols, :], NT)
        dx_ref[:, cols] = acc.astype(BF16)

    def dx_part(j):
        dx_far(j, dx_near(j))

    def out_copy(k, src, dst):
        return pltpu.make_async_copy(src, dst, out_sem.at[k])

    outs = [out_copy(0, dx_ref, dx_out), out_copy(1, dwq_ref, dwq_out), out_copy(2, dwk_ref, dwk_out),
            out_copy(3, dwv_ref, dwv_out), out_copy(4, dwo_ref, dwo_out)]

    with jax.named_scope('t04_ag5'):
        ag_stage1(5)
    with jax.named_scope('t05_y0'):
        dw_blocks(0, 3)
        dw_blocks(1, 2)
    with jax.named_scope('t06_ag5'):
        ag_stage2(5)
    with jax.named_scope('t07_kpass'):
        k_pass()
        for cp_ in ag_first(6):
            cp_.start()
    with jax.named_scope('t08_y1'):
        dw_blocks(1, 3)
        y_pass(1)
    with jax.named_scope('t09_ag5'):
        ag_stage3(5)
    with jax.named_scope('t10_kfin'):
        p = kr.at[:, pl.ds(0, 2)]
        rcopy(p, p, kr_s.at[0], kr_r.at[2], to_r).wait_recv()
        kvb[pl.ds(me * tok, half), :] = (kvp[own, 0:half, :] + kr[1, 0] + kr[0, 2]).astype(BF16)
        kvb[pl.ds(me * tok + half, half), :] = (kvp[own, half:, :] + kr[0, 0] + kr[1, 2]).astype(BF16)
        for cp_ in ag_own(3) + ag_second(6):
            cp_.start()
    with jax.named_scope('t11_dqw'):
        dq_total.wait_recv()
        wd_own.wait_recv()
        wd_rest.wait_recv()
    with jax.named_scope('t12_dxa'):
        dx_part(0)
    with jax.named_scope('t13_ag3'):
        ag_stage1(3)
        ag_stage1(6)
    with jax.named_scope('t14_dxa'):
        dx_part(1)
    with jax.named_scope('t15_ag3'):
        ag_stage2(3)
        ag_stage2(6)
    with jax.named_scope('t16_ag3'):
        ag_stage3(3)
        for xc in (cx, xright, xleft, xfar):
            ag_partner(3, xc)
    mrow = width // (2 * chips)
    krow = mrow // rows
    with jax.named_scope('t18_wk'):
        part = dot(xf[:, pl.ds(pl.multiple_of(me * mrow, mrow), mrow)], kvb[...], TN)
        wkp[...] = part.reshape(rows, krow, 2 * head_dim)

    def wk_copy(idx, blk, dev):
        return rcopy(wkp.at[blk], wkr.at[idx], wk_s.at[0], wk_r.at[0], dev)

    wk_total = rcopy(wkr, wkr, wk_s.at[0], wk_r.at[0], to_u)

    wk_copies = [wk_copy(0, yup, to_u), wk_copy(1, ydn, to_d), wk_copy(2, yfar, to_f)]
    for cp_ in wk_copies:
        cp_.start()
    with jax.named_scope('t19_dx2'):
        for xc in (cx, xright, xleft, xfar):
            ag_partner(5, xc)
        dx_part(2)
    with jax.named_scope('t19_ag6'):
        for xc in (cx, xright, xleft):
            ag_partner(6, xc)
        dxacc[...] = dx_near(3)
    with jax.named_scope('t19_ag6f'):
        ag_stage3(6)
    with jax.named_scope('t19_y0f'):
        first, second = y_final(0)
        dwo_ref[:, 0:wcol] = first
        dwo_ref[:, wcol:] = second
        outs[4].start()
    with jax.named_scope('t19_dx3'):
        ag_partner(6, xfar)
        dx_far(3, dxacc[...])
        outs[0].start()
    with jax.named_scope('t20_y1f'):
        for idx, val in enumerate(y_final(1)):
            val = val.T
            for h in range(heads):
                dwq_ref[pl.ds(idx * wcol * heads + h, wcol, stride=heads), :] = val[:, h * head_dim:(h + 1) * head_dim]
        outs[1].start()
    with jax.named_scope('t21_wkf'):
        wk_total.wait_recv()
        wk_sum = wkp[my] + wkr[0] + wkr[1] + wkr[2]
        dwk_ref[...] = wk_sum[:, 0:head_dim]
        dwv_ref[...] = wk_sum[:, head_dim:]
        outs[2].start()
        outs[3].start()

    with jax.named_scope('t22_sends'):
        for arr in range(7):
            ag_sent(arr)
        wd_own.wait_send()
        wd_rest.wait_send()
        wy_total(6).wait_send()
        dq_total.wait_send()
        kd_total.wait_send()
        rcopy(kvp.at[pl.ds(0, 3)], kvp.at[pl.ds(0, 3)], kr_s.at[0], kr_r.at[0], to_r).wait_send()
        rcopy(dwa.at[:, pl.ds(0, 6)], dwa.at[:, pl.ds(0, 6)], yr_s.at[0], yr_r.at[0, 0], to_u).wait_send()
        wk_total.wait_send()
        for cp_ in outs:
            cp_.wait()


def copy_out(*refs):
    n = (len(refs) - 1) // 2
    sem = refs[-1]
    copies = [pltpu.make_async_copy(refs[k], refs[n + k], sem.at[k]) for k in range(n)]
    for cp_ in copies:
        cp_.start()
    for cp_ in copies:
        cp_.wait()


VMEM_LIMIT = 60 * 1000 * 1000


def solution(mesh):
    model_size = mesh.shape['model']
    data_size = mesh.shape['data']
    tok_spec = P(('pod', 'data'), 'model', None)
    chips = model_size // 2

    def device_step(x_loc, dy_loc, w_q, w_k, w_v, w_o):
        tok, width = x_loc.shape[1:]
        head_dim = w_k.shape[2]
        head_cols = w_q.shape[1] * head_dim
        assert chips == 4 and data_size == 4 and w_k.shape[0] == 1 and x_loc.shape[0] == 1
        seq = model_size * tok
        half = tok // 2
        heads = head_cols // head_dim
        wcol = width // (2 * data_size)
        krow = width // (model_size * data_size)
        cfg = (tok, width, head_cols, head_dim, chips, data_size)
        vm = pltpu.VMEM
        dma = pltpu.SemaphoreType.DMA
        scratch = [
            vm((seq, width), BF16), vm((seq, width), BF16), vm((2, chips, width, head_cols), BF16), vm((head_cols, width), BF16),
            vm((width, 2 * head_dim), BF16), vm((heads * width, head_dim), BF16), vm((heads * width, head_dim), F32),
            vm((seq, head_cols), BF16), vm((seq, 2 * head_dim), BF16), vm((seq, head_cols), BF16),
            vm((heads, seq, seq), F32), vm((heads, seq, seq), BF16), vm((seq, head_cols), BF16), vm((seq, head_cols), BF16),
            vm((seq, 2 * head_dim), BF16), vm((chips, 2, tok, head_cols), BF16),
            vm((model_size, tok, 2 * head_dim), F32), vm((chips, tok, 2 * head_dim), F32), vm((2, 3, half, 2 * head_dim), F32),
            vm((2, 2 * data_size, head_cols, wcol), F32), vm((2, 2, 3, head_cols, wcol), F32),
            vm((data_size, krow, 2 * head_dim), F32), vm((3, krow, 2 * head_dim), F32),
            vm((tok, width // 4), F32), vm((tok, width), BF16), vm((heads * 2 * wcol, head_dim), F32), vm((krow, head_dim), F32), vm((krow, head_dim), F32),
            vm((head_cols, 2 * wcol), F32),
            dma((5,)), dma((5,)), dma((7,)), dma((7, 10)), dma((1,)), dma((3,)), dma((2,)), dma((2,)),
            dma((1,)), dma((1,)), dma((1,)), dma((1,)), dma((1,)), dma((3,)), dma((1,)), dma((2, 3)), dma((1,)), dma((1,)),
        ]
        anyspec = pl.BlockSpec(memory_space=pl.ANY)
        vspec = pl.BlockSpec(memory_space=pltpu.VMEM)
        shapes = (jax.ShapeDtypeStruct((tok, width), BF16), jax.ShapeDtypeStruct((heads * 2 * wcol, head_dim), F32),
                  jax.ShapeDtypeStruct((krow, head_dim), F32), jax.ShapeDtypeStruct((krow, head_dim), F32),
                  jax.ShapeDtypeStruct((head_cols, 2 * wcol), F32))
        outs = pl.pallas_call(
            functools.partial(body, cfg),
            out_shape=tuple(pltpu.VMEM(a.shape, a.dtype) for a in shapes),
            in_specs=[anyspec] * 6,
            out_specs=(anyspec,) * 5,
            scratch_shapes=scratch,
            compiler_params=pltpu.CompilerParams(collective_id=0, has_side_effects=True, vmem_limit_bytes=VMEM_LIMIT),
            name='attn_bwd',
        )(x_loc[0], dy_loc[0], w_q.reshape(width * heads, head_dim), w_o.reshape(head_cols, width), w_k[0], w_v[0])
        dx, dwq, dwk, dwv, dwo = pl.pallas_call(
            copy_out,
            out_shape=shapes,
            in_specs=[vspec] * 5,
            out_specs=(anyspec,) * 5,
            scratch_shapes=[dma((5,))],
            compiler_params=pltpu.CompilerParams(vmem_limit_bytes=4 * 1024 * 1024),
            name='copy_out',
        )(*outs)
        return (dx[None], dwq.reshape(2 * wcol, heads, head_dim), dwk, dwv, dwo.reshape(heads, head_dim, 2 * wcol))

    kv_rows = P(('pod', 'model', 'data'), None)
    return jax.shard_map(device_step, mesh=mesh,
                         in_specs=(tok_spec, tok_spec, P(None, 'model', None), P(), P(), P('model', None, None)),
                         out_specs=(tok_spec, P(('pod', 'data'), 'model', None), kv_rows, kv_rows, P(('pod', 'model'), None, 'data')),
                         check_vma=False)
```

```python
import functools

import jax
import jax.numpy as jnp
from jax import lax
from jax.experimental import pallas as pl
from jax.experimental.pallas import tpu as pltpu
from jax.sharding import PartitionSpec as P

F32 = jnp.float32
BF16 = jnp.bfloat16
NN = (((1,), (0,)), ((), ()))
NT = (((1,), (1,)), ((), ()))
TN = (((0,), (0,)), ((), ()))


def dot(a, b, dims):
    return lax.dot_general(a, b, dims, preferred_element_type=F32)


def body(cfg, x_hbm, dy_hbm, wq_hbm, wo_hbm, wk_hbm, wv_hbm,
         dx_out, dwq_out, dwk_out, dwv_out, dwo_out,
         xf, yf, wqs, wo, wkv, wq2, wq2f, qf, kv, of, prob, dsf, dqf, dof, kvb, dqa,
         kvp, kvr, kr, dwa, yr, wkp, wkr, dxacc, dx_ref, dwq_ref, dwk_ref, dwv_ref, dwo_ref,
         load_sem, out_sem, ag_s, ag_r, wy_s, wy_r, wd_s, wd_r, dq_s, dq_r,
         kd_s, kd_r, kr_s, kr_r, yr_s, yr_r, wk_s, wk_r):
    tok, width, head_cols, head_dim, chips, rows = cfg
    half = tok // 2
    chunk = 2 * tok
    seq = chips * chunk
    heads = head_cols // head_dim
    wcol = width // (2 * rows)
    hcol = width // 2
    qrow = 5 * width // 32
    erow = rows * qrow
    brow = (width - erow) // 2
    scale = head_dim ** -0.5

    me = lax.axis_index('model')
    cx = me // 2
    cc = me % 2
    cp = 1 - cc
    xright = (cx + 1) % chips
    xleft = (cx + chips - 1) % chips
    xfar = (cx + 2) % chips
    my = lax.axis_index('data')
    yup = (my + 1) % rows
    ydn = (my + rows - 1) % rows
    yfar = (my + 2) % rows
    to_r = {'model': xright * 2 + cc}
    to_l = {'model': xleft * 2 + cc}
    to_p = {'model': cx * 2 + cp}
    to_u = {'data': yup}
    to_d = {'data': ydn}
    to_f = {'data': yfar}

    def rcopy(src, dst, ssem, rsem, dev):
        return pltpu.make_async_remote_copy(src_ref=src, dst_ref=dst, send_sem=ssem, recv_sem=rsem,
                                            device_id=dev, device_id_type=pl.DeviceIdType.MESH)

    def piece(arr, xc, core, h, base):
        r = pl.ds((xc * 2 + core) * tok + h * half, half)
        if arr == 0:
            return xf.at[r, :]
        if arr == 3:
            return kvb.at[r, :]
        slot = (xc + chips - base) % chips
        if arr == 4:
            return wqs.at[core, slot, pl.ds(my * qrow + h * (qrow // 2), qrow // 2), :]
        if arr >= 5:
            return wqs.at[core, slot, pl.ds(erow + (arr - 5) * brow + h * (brow // 2), brow // 2), :]
        return yf.at[r, pl.ds((arr - 1) * hcol, hcol)]

    def ag_slot(xc, base, h, cross):
        away = (xc + chips - base) % chips
        return 2 * chips - 2 + away if cross else 2 * away - 2 + h

    def ag_copy(arr, idx, xc, core, h, dev):
        base = {'r': xright, 'l': xleft, 'p': cx}[dev]
        return rcopy(piece(arr, xc, core, h, cx), piece(arr, xc, core, h, base), ag_s.at[arr],
                     ag_r.at[arr, ag_slot(xc, base, h, dev == 'p')], {'r': to_r, 'l': to_l, 'p': to_p}[dev])

    def ag_ring_first(arr):
        return [ag_copy(arr, 0, cx, cc, 0, 'r'), ag_copy(arr, 2, cx, cc, 1, 'l')]

    def ag_first(arr):
        return ag_ring_first(arr) + [ag_copy(arr, 4, cx, cc, 0, 'p'), ag_copy(arr, 5, cx, cc, 1, 'p')]

    def ag_second(arr):
        return [ag_copy(arr, 1, cx, cc, 1, 'r'), ag_copy(arr, 3, cx, cc, 0, 'l')]

    def ag_own(arr):
        return ag_first(arr) + ag_second(arr)

    def ag_relay(arr):
        return [ag_copy(arr, 6, xleft, cc, 0, 'r'), ag_copy(arr, 7, xright, cc, 1, 'l')]

    def ag_cross(arr, idx, xc, h):
        return ag_copy(arr, idx, xc, cc, h, 'p')

    def ag_wait(arr, xc, core, h):
        p = piece(arr, xc, core, h, cx)
        rcopy(p, p, ag_s.at[arr], ag_r.at[arr, ag_slot(xc, cx, h, False)], to_p).wait_recv()

    def ag_relays(arr):
        relays = ag_relay(arr)
        ag_wait(arr, xleft, cc, 0)
        relays[0].start()
        ag_wait(arr, xright, cc, 1)
        relays[1].start()

    def ag_stage1(arr):
        ag_relays(arr)
        ag_cross(arr, 8, xleft, 0).start()
        ag_cross(arr, 11, xright, 1).start()

    def ag_stage2(arr):
        ag_wait(arr, xright, cc, 0)
        ag_cross(arr, 10, xright, 0).start()
        ag_wait(arr, xleft, cc, 1)
        ag_cross(arr, 9, xleft, 1).start()

    def ag_stage3(arr):
        ag_wait(arr, xfar, cc, 0)
        ag_cross(arr, 12, xfar, 0).start()
        ag_wait(arr, xfar, cc, 1)
        ag_cross(arr, 13, xfar, 1).start()

    def ag_partner(arr, xc):
        r = pl.ds((xc * 2 + cp) * tok, tok)
        if arr == 0:
            p = xf.at[r, :]
        elif arr == 3:
            p = kvb.at[r, :]
        elif arr >= 5:
            p = wqs.at[cp, (xc + chips - cx) % chips, pl.ds(erow + (arr - 5) * brow, brow), :]
        else:
            p = yf.at[r, pl.ds((arr - 1) * hcol, hcol)]
        rcopy(p, p, ag_s.at[arr], ag_r.at[arr, ag_slot(xc, cx, 0, True)], to_p).wait_recv()

    def ag_sent(arr):
        r = pl.ds(0, 7 * tok)
        p = {0: xf.at[r, :], 1: yf.at[r, pl.ds(0, hcol)], 2: yf.at[r, pl.ds(0, hcol)], 3: kvb.at[r, :],
             4: wqs.at[0, 0, pl.ds(0, 3 * qrow), :], 5: wqs.at[:, 0, pl.ds(0, 7 * brow // 2), :],
             6: wqs.at[:, 0, pl.ds(0, 7 * brow // 2), :]}[arr]
        rcopy(p, p, ag_s.at[arr], ag_r.at[arr, 0], to_p).wait_send()

    def wy_copy(idx, q, h, dev):
        p = wqs.at[cc, pl.ds(1, chips - 1), pl.ds(q * qrow + h * (qrow // 2), qrow // 2), :]
        return rcopy(p, p, wy_s.at[0], wy_r.at[idx], dev)

    wy_own = [wy_copy(0, my, 0, to_u), wy_copy(1, my, 1, to_d), wy_copy(2, my, 1, to_u), wy_copy(2, my, 0, to_d)]
    wy_relay = [wy_copy(2, ydn, 0, to_u), wy_copy(2, yup, 1, to_d)]

    def wy_pass():
        wy_copy(0, ydn, 0, to_u).wait_recv()
        wy_relay[0].start()
        wy_copy(1, yup, 1, to_u).wait_recv()
        wy_relay[1].start()

    def wy_total(count):
        p = wqs.at[cc, pl.ds(1, chips - 1), pl.ds(0, count * (qrow // 2)), :]
        return rcopy(p, p, wy_s.at[0], wy_r.at[2], to_u)

    wd_own = rcopy(wqs.at[cc, 0, pl.ds(0, erow), :], wqs.at[cc, 0, pl.ds(0, erow), :], wd_s.at[0], wd_r.at[0], to_p)
    wd_rest = rcopy(wqs.at[cc, pl.ds(1, chips - 1), pl.ds(0, erow), :], wqs.at[cc, pl.ds(1, chips - 1), pl.ds(0, erow), :],
                    wd_s.at[1], wd_r.at[1], to_p)

    def wy_end():
        wy_total(4).wait_recv()
        wd_rest.start()

    def dq_copy(xc, core):
        return rcopy(dqf.at[pl.ds((xc * 2 + core) * tok, tok), :], dqa.at[(cx + chips - xc) % chips, cc],
                     dq_s.at[0], dq_r.at[0], {'model': xc * 2 + core})

    dq_total = rcopy(dqf.at[pl.ds(0, 7 * tok), :], dqf.at[pl.ds(0, 7 * tok), :], dq_s.at[0], dq_r.at[0], to_p)

    def kd_copy(xc):
        return rcopy(kvp.at[xc * 2 + cp], kvr.at[xc], kd_s.at[0], kd_r.at[0], to_p)

    kd_total = rcopy(kvr, kvr, kd_s.at[0], kd_r.at[0], to_p)

    def kpart(xc, h):
        return kvp.at[xc * 2 + cc, pl.ds(h * half, half), :]

    def ring_src(kind, side):
        if kind == 0:
            return (xright, 1) if side == 0 else (xleft, 0)
        if kind == 1:
            return (xfar, 0) if side == 0 else (xfar, 1)
        return (xright, 0) if side == 0 else (xleft, 1)

    def k_copy(side, kind):
        xc, h = ring_src(kind, side)
        return rcopy(kpart(xc, h), kr.at[side, kind], kr_s.at[0], kr_r.at[side if kind == 1 else 2],
                     to_r if side == 0 else to_l)

    def k_pass():
        for side in range(2):
            k_copy(side, 1).wait_recv()
            xc, h = ring_src(2, side)
            ref = kpart(xc, h)
            ref[...] = ref[...] + kr[side, 1]
            k_copy(side, 2).start()

    order = ((yfar, 0), (yfar, 1), (yup, 1), (ydn, 0), (yup, 0), (ydn, 1), (my, 0), (my, 1))

    def y_blk(w, kind, side):
        pos = {(1, 0): 0, (1, 1): 1, (0, 0): 2, (0, 1): 3, (2, 0): 4, (2, 1): 5, (3, 0): 6, (3, 1): 7}[kind, side]
        if w == 0:
            return pos
        return order[pos][0] * 2 + order[pos][1]

    def y_copy(w, side, kind):
        return rcopy(dwa.at[w, y_blk(w, kind, side)], yr.at[w, side, kind], yr_s.at[0], yr_r.at[w, side if kind == 1 else 2],
                     to_u if side == 0 else to_d)

    def dw_block(w, kind, side):
        blk = y_blk(w, kind, side)
        if w == 0:
            dwa[0, blk] = dot(of[...], yf[:, blk * wcol:(blk + 1) * wcol], TN)
        else:
            dwa[1, blk] = dot(dqf[...], xf[:, pl.ds(pl.multiple_of(blk * wcol, wcol), wcol)], TN)

    def y_first(w, between=lambda: None):
        for kind in (1, 0):
            for side in range(2):
                dw_block(w, kind, side)
                y_copy(w, side, kind).start()
            if kind == 1:
                between()

    def dw_blocks(w, kind):
        for side in range(2):
            dw_block(w, kind, side)

    def y_pass(w):
        for side in range(2):
            y_copy(w, side, 1).wait_recv()
            blk = y_blk(w, 2, side)
            dwa[w, blk] = dwa[w, blk] + yr[w, side, 1]
            y_copy(w, side, 2).start()

    def y_final(w):
        p = yr.at[w, :, pl.ds(0, 2)]
        rcopy(p, p, yr_s.at[0], yr_r.at[w, 2], to_u).wait_recv()
        first = dwa[w, y_blk(w, 3, 0)] + yr[w, 1, 0] + yr[w, 0, 2]
        second = dwa[w, y_blk(w, 3, 1)] + yr[w, 0, 0] + yr[w, 1, 2]
        return first, second

    own_rows = pl.ds(me * tok, tok)
    loads = [pltpu.make_async_copy(x_hbm, xf.at[own_rows, :], load_sem.at[0]),
             pltpu.make_async_copy(wq_hbm, wq2, load_sem.at[1]),
             pltpu.make_async_copy(wk_hbm, wkv.at[:, pl.ds(0, head_dim)], load_sem.at[2]),
             pltpu.make_async_copy(wv_hbm, wkv.at[:, pl.ds(head_dim, head_dim)], load_sem.at[2])]
    for pos, (dest, part) in enumerate(order):
        src = pl.ds(pl.multiple_of((dest * 2 + part) * wcol, wcol), wcol)
        dst = pl.ds(pos * wcol, wcol)
        loads.append(pltpu.make_async_copy(dy_hbm.at[:, src], yf.at[own_rows, dst], load_sem.at[3]))
        loads.append(pltpu.make_async_copy(wo_hbm.at[:, src], wo.at[:, dst], load_sem.at[4]))
    for cp_ in loads:
        cp_.start()
    barrier = pltpu.get_barrier_semaphore()
    peers = [{'model': (me + k) % (2 * chips)} for k in range(1, 2 * chips)]
    for dev in peers + [to_u, to_d, to_f]:
        pl.semaphore_signal(barrier, inc=1, device_id=dev, device_id_type=pl.DeviceIdType.MESH)
    with jax.named_scope('barrier'):
        pl.semaphore_wait(barrier, 2 * chips + 2)
    loads[0].wait()
    for cp_ in ag_first(0):
        cp_.start()
    with jax.named_scope('loadw'):
        loads[1].wait()
        for k, ref in ((2, wkv), (3, yf.at[own_rows, :]), (4, wo)):
            pltpu.make_async_copy(ref, ref, load_sem.at[k]).wait()
        step = 2 * width // 8

        @pl.loop(0, 8)
        def _(b):
            r2 = pl.ds(pl.multiple_of(b * step, step), step)
            wq2f[r2, :] = wq2[r2, :].astype(F32)
            r1 = pl.ds(pl.multiple_of(b * (step // 2), step // 2), step // 2)
            for h in range(heads):
                wqs[cc, 0, r1, h * head_dim:(h + 1) * head_dim] = wq2f[pl.ds(b * step + h, step // 2, stride=heads), :].astype(BF16)

    for cp_ in ag_ring_first(4) + ag_second(4) + ag_second(0):
        cp_.start()
    wd_own.start()

    def chunk_of(s):
        return (cx + s + s // 2 - 2 * (s // 3)) % chips

    @pl.loop(0, chips)
    def _(s):
        @pl.when(s == 0)
        def _():
            ag_partner(0, cx)

        @pl.when(s == 1)
        def _():
            with jax.named_scope('q1'):
                ag_relays(4)
                ag_stage1(0)
                for cp_ in ag_own(1):
                    cp_.start()
                ag_stage2(0)
            with jax.named_scope('q1w'):
                for xc, h in ((xleft, 1), (xright, 0), (xfar, 0), (xfar, 1)):
                    ag_wait(4, xc, cc, h)
                for cp_ in wy_own:
                    cp_.start()
            ag_partner(0, xright)

        @pl.when(s == 2)
        def _():
            ag_partner(0, xleft)

        @pl.when(s == 3)
        def _():
            ag_stage3(0)
            ag_partner(0, xfar)

        r = pl.ds(chunk_of(s) * chunk, chunk)
        xc = xf[r, :]
        qf[r, :] = dot(xc, wqs[cc, 0], NN).astype(BF16)
        kv[r, :] = dot(xc, wkv[...], NN).astype(BF16)

    @pl.loop(0, chips)
    def _(s):
        @pl.when(s == 1)
        def _():
            with jax.named_scope('f1'):
                ag_stage1(1)
                for cp_ in ag_own(2):
                    cp_.start()

        @pl.when(s == 2)
        def _():
            with jax.named_scope('f2'):
                wy_pass()
                ag_stage2(1)

        i = chunk_of(s)
        r = pl.ds(i * chunk, chunk)
        row_id = lax.broadcasted_iota(jnp.int32, (chunk, seq), 0) + i * chunk
        keep = row_id >= lax.broadcasted_iota(jnp.int32, (chunk, seq), 1)
        for h in range(heads):
            hc = pl.ds(h * head_dim, head_dim)
            sc = dot(qf[r, hc], kv[:, 0:head_dim], NT) * scale
            sc = jnp.where(keep, sc, -jnp.inf)
            ex = jnp.exp(sc - jnp.max(sc, axis=-1, keepdims=True))
            pr = ex * (1.0 / jnp.sum(ex, axis=-1, keepdims=True))
            prob[h, r, :] = pr
            of[r, hc] = dot(pr.astype(BF16), kv[:, head_dim:], NN).astype(BF16)

    def mid_relays():
        ag_stage1(2)
        for cp_ in ag_own(5):
            cp_.start()

    with jax.named_scope('b0'):
        ag_stage3(1)
        ag_partner(1, cx)
        ag_partner(2, cx)

    @pl.loop(0, chips)
    def _(s):
        @pl.when(s == 1)
        def _():
            with jax.named_scope('b1'):
                for xc in (xright, xleft, xfar):
                    ag_partner(1, xc)
            with jax.named_scope('b1y'):
                y_first(0, mid_relays)
            with jax.named_scope('b1w'):
                ag_stage2(2)
                wy_end()
                ag_partner(2, xright)

        @pl.when(s == 2)
        def _():
            with jax.named_scope('b2'):
                ag_stage3(2)
                ag_partner(2, xleft)

        @pl.when(s == 3)
        def _():
            with jax.named_scope('b3'):
                ag_partner(2, xfar)

        with jax.named_scope('b_comp'):
            i = chunk_of(s)
            r = pl.ds(i * chunk, chunk)
            oc = of[r, :]
            do = dot(yf[r, :], wo[...], NT).astype(BF16)
            dof[r, :] = do
            od = do.astype(F32) * oc.astype(F32)
            for h in range(heads):
                hs = slice(h * head_dim, (h + 1) * head_dim)
                dp = dot(do[:, hs], kv[:, head_dim:], NT)
                ds = (prob[h, r, :] * (dp - jnp.sum(od[:, hs], axis=-1, keepdims=True))).astype(BF16)
                dsf[h, r, :] = ds
                dqf[r, hs] = (dot(ds, kv[:, 0:head_dim], NN) * scale).astype(BF16)

        @pl.when(s == 0)
        def _():
            dqa[0, cc] = dqf[own_rows, :]
            dq_copy(cx, cp).start()

        @pl.when(s > 0)
        def _():
            for core in range(2):
                dq_copy(i, core).start()

    with jax.named_scope('t00_dkv'):
        for kc in range(chips):
            ks = slice(kc * chunk, (kc + 1) * chunk)
            qs = slice(kc * chunk, seq)
            dk = jnp.zeros((chunk, head_dim), F32)
            dv = jnp.zeros((chunk, head_dim), F32)
            for h in range(heads):
                hs = slice(h * head_dim, (h + 1) * head_dim)
                dk = dk + dot(dsf[h, qs, ks], qf[qs, hs], TN)
                dv = dv + dot(prob[h, qs, ks].astype(BF16), dof[qs, hs], TN)
            kvp[2 * kc:2 * kc + 2, :, 0:head_dim] = (dk * scale).reshape(2, tok, head_dim)
            kvp[2 * kc:2 * kc + 2, :, head_dim:] = dv.reshape(2, tok, head_dim)
        for xc in range(chips):
            kd_copy(xc).start()

    def kd_ring():
        kd_total.wait_recv()
        for xc in range(chips):
            blk = xc * 2 + cc
            kvp[blk] = kvp[blk] + kvr[xc]
        for kind in (1, 0):
            for side in range(2):
                k_copy(side, kind).start()

    with jax.named_scope('t00_y1'):
        y_first(1, kd_ring)

    own = cx * 2 + cc

    cuts = (0, erow // 2, erow, erow + brow, width)

    def dx_near(j):
        cols = slice(cuts[j], cuts[j + 1])
        acc = dot(kvb[own_rows, :], wkv[cols, :], NT)
        for slot in (0, 1, chips - 1):
            for core in range(2):
                acc = acc + dot(dqa[slot, core], wqs[core, slot, cols, :], NT)
        return acc

    def dx_far(j, acc):
        cols = slice(cuts[j], cuts[j + 1])
        for core in range(2):
            acc = acc + dot(dqa[2, core], wqs[core, 2, cols, :], NT)
        dx_ref[:, cols] = acc.astype(BF16)

    def dx_part(j):
        dx_far(j, dx_near(j))

    def out_copy(k, src, dst):
        return pltpu.make_async_copy(src, dst, out_sem.at[k])

    outs = [out_copy(0, dx_ref, dx_out), out_copy(1, dwq_ref, dwq_out), out_copy(2, dwk_ref, dwk_out),
            out_copy(3, dwv_ref, dwv_out), out_copy(4, dwo_ref, dwo_out)]

    with jax.named_scope('t04_ag5'):
        ag_stage1(5)
    with jax.named_scope('t05_y0'):
        dw_blocks(0, 2)
        y_pass(0)
        dw_blocks(0, 3)
        dw_blocks(1, 2)
    with jax.named_scope('t06_ag5'):
        ag_stage2(5)
    with jax.named_scope('t07_kpass'):
        k_pass()
        for cp_ in ag_first(6):
            cp_.start()
    with jax.named_scope('t08_y1'):
        dw_blocks(1, 3)
        y_pass(1)
    with jax.named_scope('t09_ag5'):
        ag_stage3(5)
    with jax.named_scope('t10_kfin'):
        p = kr.at[:, pl.ds(0, 2)]
        rcopy(p, p, kr_s.at[0], kr_r.at[2], to_r).wait_recv()
        kvb[pl.ds(me * tok, half), :] = (kvp[own, 0:half, :] + kr[1, 0] + kr[0, 2]).astype(BF16)
        kvb[pl.ds(me * tok + half, half), :] = (kvp[own, half:, :] + kr[0, 0] + kr[1, 2]).astype(BF16)
        for cp_ in ag_own(3) + ag_second(6):
            cp_.start()
    with jax.named_scope('t11_dqw'):
        dq_total.wait_recv()
        wd_own.wait_recv()
        wd_rest.wait_recv()
    with jax.named_scope('t12_dxa'):
        dx_part(0)
    with jax.named_scope('t13_ag3'):
        ag_stage1(3)
        ag_stage1(6)
    with jax.named_scope('t14_dxa'):
        dx_part(1)
    with jax.named_scope('t15_ag3'):
        ag_stage2(3)
        ag_stage2(6)
    with jax.named_scope('t16_ag3'):
        ag_stage3(3)
        for xc in (cx, xright, xleft, xfar):
            ag_partner(3, xc)
    mrow = width // (2 * chips)
    krow = mrow // rows
    with jax.named_scope('t18_wk'):
        part = dot(xf[:, pl.ds(pl.multiple_of(me * mrow, mrow), mrow)], kvb[...], TN)
        wkp[...] = part.reshape(rows, krow, 2 * head_dim)

    def wk_copy(idx, blk, dev):
        return rcopy(wkp.at[blk], wkr.at[idx], wk_s.at[0], wk_r.at[0], dev)

    wk_total = rcopy(wkr, wkr, wk_s.at[0], wk_r.at[0], to_u)

    wk_copies = [wk_copy(0, yup, to_u), wk_copy(1, ydn, to_d), wk_copy(2, yfar, to_f)]
    for cp_ in wk_copies:
        cp_.start()
    with jax.named_scope('t19_dx2'):
        for xc in (cx, xright, xleft, xfar):
            ag_partner(5, xc)
        dx_part(2)
    with jax.named_scope('t19_ag6'):
        for xc in (cx, xright, xleft):
            ag_partner(6, xc)
        dxacc[...] = dx_near(3)
    with jax.named_scope('t19_ag6f'):
        ag_stage3(6)
    with jax.named_scope('t19_y0f'):
        first, second = y_final(0)
        dwo_ref[:, 0:wcol] = first
        dwo_ref[:, wcol:] = second
        outs[4].start()
    with jax.named_scope('t19_dx3'):
        ag_partner(6, xfar)
        dx_far(3, dxacc[...])
        outs[0].start()
    with jax.named_scope('t20_y1f'):
        for idx, val in enumerate(y_final(1)):
            val = val.T
            for h in range(heads):
                dwq_ref[pl.ds(idx * wcol * heads + h, wcol, stride=heads), :] = val[:, h * head_dim:(h + 1) * head_dim]
        outs[1].start()
    with jax.named_scope('t21_wkf'):
        wk_total.wait_recv()
        wk_sum = wkp[my] + wkr[0] + wkr[1] + wkr[2]
        dwk_ref[...] = wk_sum[:, 0:head_dim]
        dwv_ref[...] = wk_sum[:, head_dim:]
        outs[2].start()
        outs[3].start()

    with jax.named_scope('t22_sends'):
        for arr in range(7):
            ag_sent(arr)
        wd_own.wait_send()
        wd_rest.wait_send()
        wy_total(6).wait_send()
        dq_total.wait_send()
        kd_total.wait_send()
        rcopy(kvp.at[pl.ds(0, 3)], kvp.at[pl.ds(0, 3)], kr_s.at[0], kr_r.at[0], to_r).wait_send()
        rcopy(dwa.at[:, pl.ds(0, 6)], dwa.at[:, pl.ds(0, 6)], yr_s.at[0], yr_r.at[0, 0], to_u).wait_send()
        wk_total.wait_send()
        for cp_ in outs:
            cp_.wait()


def copy_out(*refs):
    n = (len(refs) - 1) // 2
    sem = refs[-1]
    copies = [pltpu.make_async_copy(refs[k], refs[n + k], sem.at[k]) for k in range(n)]
    for cp_ in copies:
        cp_.start()
    for cp_ in copies:
        cp_.wait()


VMEM_LIMIT = 60 * 1000 * 1000


def solution(mesh):
    model_size = mesh.shape['model']
    data_size = mesh.shape['data']
    tok_spec = P(('pod', 'data'), 'model', None)
    chips = model_size // 2

    def device_step(x_loc, dy_loc, w_q, w_k, w_v, w_o):
        tok, width = x_loc.shape[1:]
        head_dim = w_k.shape[2]
        head_cols = w_q.shape[1] * head_dim
        assert chips == 4 and data_size == 4 and w_k.shape[0] == 1 and x_loc.shape[0] == 1
        seq = model_size * tok
        half = tok // 2
        heads = head_cols // head_dim
        wcol = width // (2 * data_size)
        krow = width // (model_size * data_size)
        cfg = (tok, width, head_cols, head_dim, chips, data_size)
        vm = pltpu.VMEM
        dma = pltpu.SemaphoreType.DMA
        scratch = [
            vm((seq, width), BF16), vm((seq, width), BF16), vm((2, chips, width, head_cols), BF16), vm((head_cols, width), BF16),
            vm((width, 2 * head_dim), BF16), vm((heads * width, head_dim), BF16), vm((heads * width, head_dim), F32),
            vm((seq, head_cols), BF16), vm((seq, 2 * head_dim), BF16), vm((seq, head_cols), BF16),
            vm((heads, seq, seq), F32), vm((heads, seq, seq), BF16), vm((seq, head_cols), BF16), vm((seq, head_cols), BF16),
            vm((seq, 2 * head_dim), BF16), vm((chips, 2, tok, head_cols), BF16),
            vm((model_size, tok, 2 * head_dim), F32), vm((chips, tok, 2 * head_dim), F32), vm((2, 3, half, 2 * head_dim), F32),
            vm((2, 2 * data_size, head_cols, wcol), F32), vm((2, 2, 3, head_cols, wcol), F32),
            vm((data_size, krow, 2 * head_dim), F32), vm((3, krow, 2 * head_dim), F32),
            vm((tok, 3 * width // 16), F32), vm((tok, width), BF16), vm((heads * 2 * wcol, head_dim), F32), vm((krow, head_dim), F32), vm((krow, head_dim), F32),
            vm((head_cols, 2 * wcol), F32),
            dma((5,)), dma((5,)), dma((7,)), dma((7, 10)), dma((1,)), dma((3,)), dma((2,)), dma((2,)),
            dma((1,)), dma((1,)), dma((1,)), dma((1,)), dma((1,)), dma((3,)), dma((1,)), dma((2, 3)), dma((1,)), dma((1,)),
        ]
        anyspec = pl.BlockSpec(memory_space=pl.ANY)
        vspec = pl.BlockSpec(memory_space=pltpu.VMEM)
        shapes = (jax.ShapeDtypeStruct((tok, width), BF16), jax.ShapeDtypeStruct((heads * 2 * wcol, head_dim), F32),
                  jax.ShapeDtypeStruct((krow, head_dim), F32), jax.ShapeDtypeStruct((krow, head_dim), F32),
                  jax.ShapeDtypeStruct((head_cols, 2 * wcol), F32))
        outs = pl.pallas_call(
            functools.partial(body, cfg),
            out_shape=tuple(pltpu.VMEM(a.shape, a.dtype) for a in shapes),
            in_specs=[anyspec] * 6,
            out_specs=(anyspec,) * 5,
            scratch_shapes=scratch,
            compiler_params=pltpu.CompilerParams(collective_id=0, has_side_effects=True, vmem_limit_bytes=VMEM_LIMIT),
            name='attn_bwd',
        )(x_loc[0], dy_loc[0], w_q.reshape(width * heads, head_dim), w_o.reshape(head_cols, width), w_k[0], w_v[0])
        dx, dwq, dwk, dwv, dwo = pl.pallas_call(
            copy_out,
            out_shape=shapes,
            in_specs=[vspec] * 5,
            out_specs=(anyspec,) * 5,
            scratch_shapes=[dma((5,))],
            compiler_params=pltpu.CompilerParams(vmem_limit_bytes=4 * 1024 * 1024),
            name='copy_out',
        )(*outs)
        return (dx[None], dwq.reshape(2 * wcol, heads, head_dim), dwk, dwv, dwo.reshape(heads, head_dim, 2 * wcol))

    kv_rows = P(('pod', 'model', 'data'), None)
    return jax.shard_map(device_step, mesh=mesh,
                         in_specs=(tok_spec, tok_spec, P(None, 'model', None), P(), P(), P('model', None, None)),
                         out_specs=(tok_spec, P(('pod', 'data'), 'model', None), kv_rows, kv_rows, P(('pod', 'model'), None, 'data')),
                         check_vma=False)
```

```python
import functools

import jax
import jax.numpy as jnp
from jax import lax
from jax.experimental import pallas as pl
from jax.experimental.pallas import tpu as pltpu
from jax.sharding import PartitionSpec as P

F32 = jnp.float32
BF16 = jnp.bfloat16
NN = (((1,), (0,)), ((), ()))
NT = (((1,), (1,)), ((), ()))
TN = (((0,), (0,)), ((), ()))


def dot(a, b, dims):
    return lax.dot_general(a, b, dims, preferred_element_type=F32)


def body(cfg, x_hbm, dy_hbm, wq_hbm, wo_hbm, wk_hbm, wv_hbm,
         dx_out, dwq_out, dwk_out, dwv_out, dwo_out,
         xf, yf, wqs, wo, wkv, wq2, wq2f, qf, kv, of, prob, dsf, dqf, dof, kvb, dqa,
         kvp, kvr, kr, dwa, yr, wkp, wkr, dxacc, dx_ref, dwq_ref, dwk_ref, dwv_ref, dwo_ref,
         load_sem, out_sem, ag_s, ag_r, wy_s, wy_r, wd_s, wd_r, dq_s, dq_r,
         kd_s, kd_r, kr_s, kr_r, yr_s, yr_r, wk_s, wk_r):
    tok, width, head_cols, head_dim, chips, rows = cfg
    half = tok // 2
    chunk = 2 * tok
    seq = chips * chunk
    heads = head_cols // head_dim
    wcol = width // (2 * rows)
    hcol = width // 2
    qrow = 5 * width // 32
    erow = rows * qrow
    brow = (width - erow) // 2
    scale = head_dim ** -0.5

    me = lax.axis_index('model')
    cx = me // 2
    cc = me % 2
    cp = 1 - cc
    xright = (cx + 1) % chips
    xleft = (cx + chips - 1) % chips
    xfar = (cx + 2) % chips
    my = lax.axis_index('data')
    yup = (my + 1) % rows
    ydn = (my + rows - 1) % rows
    yfar = (my + 2) % rows
    to_r = {'model': xright * 2 + cc}
    to_l = {'model': xleft * 2 + cc}
    to_p = {'model': cx * 2 + cp}
    to_u = {'data': yup}
    to_d = {'data': ydn}
    to_f = {'data': yfar}

    def rcopy(src, dst, ssem, rsem, dev):
        return pltpu.make_async_remote_copy(src_ref=src, dst_ref=dst, send_sem=ssem, recv_sem=rsem,
                                            device_id=dev, device_id_type=pl.DeviceIdType.MESH)

    def piece(arr, xc, core, h, base):
        r = pl.ds((xc * 2 + core) * tok + h * half, half)
        if arr == 0:
            return xf.at[r, :]
        if arr == 3:
            return kvb.at[r, :]
        slot = (xc + chips - base) % chips
        if arr == 4:
            return wqs.at[core, slot, pl.ds(my * qrow + h * (qrow // 2), qrow // 2), :]
        if arr >= 5:
            return wqs.at[core, slot, pl.ds(erow + (arr - 5) * brow + h * (brow // 2), brow // 2), :]
        return yf.at[r, pl.ds((arr - 1) * hcol, hcol)]

    def ag_slot(xc, base, h, cross):
        away = (xc + chips - base) % chips
        return 2 * chips - 2 + away if cross else 2 * away - 2 + h

    def ag_copy(arr, idx, xc, core, h, dev):
        base = {'r': xright, 'l': xleft, 'p': cx}[dev]
        return rcopy(piece(arr, xc, core, h, cx), piece(arr, xc, core, h, base), ag_s.at[arr],
                     ag_r.at[arr, ag_slot(xc, base, h, dev == 'p')], {'r': to_r, 'l': to_l, 'p': to_p}[dev])

    def ag_ring_first(arr):
        return [ag_copy(arr, 0, cx, cc, 0, 'r'), ag_copy(arr, 2, cx, cc, 1, 'l')]

    def ag_first(arr):
        return ag_ring_first(arr) + [ag_copy(arr, 4, cx, cc, 0, 'p'), ag_copy(arr, 5, cx, cc, 1, 'p')]

    def ag_second(arr):
        return [ag_copy(arr, 1, cx, cc, 1, 'r'), ag_copy(arr, 3, cx, cc, 0, 'l')]

    def ag_own(arr):
        return ag_first(arr) + ag_second(arr)

    def ag_relay(arr):
        return [ag_copy(arr, 6, xleft, cc, 0, 'r'), ag_copy(arr, 7, xright, cc, 1, 'l')]

    def ag_cross(arr, idx, xc, h):
        return ag_copy(arr, idx, xc, cc, h, 'p')

    def ag_wait(arr, xc, core, h):
        p = piece(arr, xc, core, h, cx)
        rcopy(p, p, ag_s.at[arr], ag_r.at[arr, ag_slot(xc, cx, h, False)], to_p).wait_recv()

    def ag_relays(arr):
        relays = ag_relay(arr)
        ag_wait(arr, xleft, cc, 0)
        relays[0].start()
        ag_wait(arr, xright, cc, 1)
        relays[1].start()

    def ag_stage1(arr):
        ag_relays(arr)
        ag_cross(arr, 8, xleft, 0).start()
        ag_cross(arr, 11, xright, 1).start()

    def ag_stage2(arr):
        ag_wait(arr, xright, cc, 0)
        ag_cross(arr, 10, xright, 0).start()
        ag_wait(arr, xleft, cc, 1)
        ag_cross(arr, 9, xleft, 1).start()

    def ag_stage3(arr):
        ag_wait(arr, xfar, cc, 0)
        ag_cross(arr, 12, xfar, 0).start()
        ag_wait(arr, xfar, cc, 1)
        ag_cross(arr, 13, xfar, 1).start()

    def ag_partner(arr, xc):
        r = pl.ds((xc * 2 + cp) * tok, tok)
        if arr == 0:
            p = xf.at[r, :]
        elif arr == 3:
            p = kvb.at[r, :]
        elif arr >= 5:
            p = wqs.at[cp, (xc + chips - cx) % chips, pl.ds(erow + (arr - 5) * brow, brow), :]
        else:
            p = yf.at[r, pl.ds((arr - 1) * hcol, hcol)]
        rcopy(p, p, ag_s.at[arr], ag_r.at[arr, ag_slot(xc, cx, 0, True)], to_p).wait_recv()

    def ag_sent(arr):
        r = pl.ds(0, 7 * tok)
        p = {0: xf.at[r, :], 1: yf.at[r, pl.ds(0, hcol)], 2: yf.at[r, pl.ds(0, hcol)], 3: kvb.at[r, :],
             4: wqs.at[0, 0, pl.ds(0, 3 * qrow), :], 5: wqs.at[:, 0, pl.ds(0, 7 * brow // 2), :],
             6: wqs.at[:, 0, pl.ds(0, 7 * brow // 2), :]}[arr]
        rcopy(p, p, ag_s.at[arr], ag_r.at[arr, 0], to_p).wait_send()

    def wy_copy(idx, q, h, dev):
        p = wqs.at[cc, pl.ds(1, chips - 1), pl.ds(q * qrow + h * (qrow // 2), qrow // 2), :]
        return rcopy(p, p, wy_s.at[0], wy_r.at[idx], dev)

    wy_own = [wy_copy(0, my, 0, to_u), wy_copy(1, my, 1, to_d), wy_copy(2, my, 1, to_u), wy_copy(2, my, 0, to_d)]
    wy_relay = [wy_copy(2, ydn, 0, to_u), wy_copy(2, yup, 1, to_d)]

    def wy_pass():
        wy_copy(0, ydn, 0, to_u).wait_recv()
        wy_relay[0].start()
        wy_copy(1, yup, 1, to_u).wait_recv()
        wy_relay[1].start()

    def wy_total(count):
        p = wqs.at[cc, pl.ds(1, chips - 1), pl.ds(0, count * (qrow // 2)), :]
        return rcopy(p, p, wy_s.at[0], wy_r.at[2], to_u)

    wd_own = rcopy(wqs.at[cc, 0, pl.ds(0, erow), :], wqs.at[cc, 0, pl.ds(0, erow), :], wd_s.at[0], wd_r.at[0], to_p)
    wd_rest = rcopy(wqs.at[cc, pl.ds(1, chips - 1), pl.ds(0, erow), :], wqs.at[cc, pl.ds(1, chips - 1), pl.ds(0, erow), :],
                    wd_s.at[1], wd_r.at[1], to_p)

    def wy_end():
        wy_total(4).wait_recv()
        wd_rest.start()

    def dq_copy(xc, core):
        return rcopy(dqf.at[pl.ds((xc * 2 + core) * tok, tok), :], dqa.at[(cx + chips - xc) % chips, cc],
                     dq_s.at[0], dq_r.at[0], {'model': xc * 2 + core})

    dq_total = rcopy(dqf.at[pl.ds(0, 7 * tok), :], dqf.at[pl.ds(0, 7 * tok), :], dq_s.at[0], dq_r.at[0], to_p)

    def kd_copy(xc):
        return rcopy(kvp.at[xc * 2 + cp], kvr.at[xc], kd_s.at[0], kd_r.at[0], to_p)

    kd_total = rcopy(kvr, kvr, kd_s.at[0], kd_r.at[0], to_p)

    def kpart(xc, h):
        return kvp.at[xc * 2 + cc, pl.ds(h * half, half), :]

    def ring_src(kind, side):
        if kind == 0:
            return (xright, 1) if side == 0 else (xleft, 0)
        if kind == 1:
            return (xfar, 0) if side == 0 else (xfar, 1)
        return (xright, 0) if side == 0 else (xleft, 1)

    def k_copy(side, kind):
        xc, h = ring_src(kind, side)
        return rcopy(kpart(xc, h), kr.at[side, kind], kr_s.at[0], kr_r.at[side if kind == 1 else 2],
                     to_r if side == 0 else to_l)

    def k_pass():
        for side in range(2):
            k_copy(side, 1).wait_recv()
            xc, h = ring_src(2, side)
            ref = kpart(xc, h)
            ref[...] = ref[...] + kr[side, 1]
            k_copy(side, 2).start()

    order = ((yfar, 0), (yfar, 1), (yup, 1), (ydn, 0), (yup, 0), (ydn, 1), (my, 0), (my, 1))

    def y_blk(w, kind, side):
        pos = {(1, 0): 0, (1, 1): 1, (0, 0): 2, (0, 1): 3, (2, 0): 4, (2, 1): 5, (3, 0): 6, (3, 1): 7}[kind, side]
        if w == 0:
            return pos
        return order[pos][0] * 2 + order[pos][1]

    def y_copy(w, side, kind):
        return rcopy(dwa.at[w, y_blk(w, kind, side)], yr.at[w, side, kind], yr_s.at[0], yr_r.at[w, side if kind == 1 else 2],
                     to_u if side == 0 else to_d)

    def dw_block(w, kind, side):
        blk = y_blk(w, kind, side)
        if w == 0:
            dwa[0, blk] = dot(of[...], yf[:, blk * wcol:(blk + 1) * wcol], TN)
        else:
            dwa[1, blk] = dot(dqf[...], xf[:, pl.ds(pl.multiple_of(blk * wcol, wcol), wcol)], TN)

    def y_first(w, kind):
        for side in range(2):
            dw_block(w, kind, side)
            y_copy(w, side, kind).start()

    def dw_blocks(w, kind):
        for side in range(2):
            dw_block(w, kind, side)

    def y_pass(w):
        for side in range(2):
            y_copy(w, side, 1).wait_recv()
            blk = y_blk(w, 2, side)
            dwa[w, blk] = dwa[w, blk] + yr[w, side, 1]
            y_copy(w, side, 2).start()

    def y_final(w):
        p = yr.at[w, :, pl.ds(0, 2)]
        rcopy(p, p, yr_s.at[0], yr_r.at[w, 2], to_u).wait_recv()
        first = dwa[w, y_blk(w, 3, 0)] + yr[w, 1, 0] + yr[w, 0, 2]
        second = dwa[w, y_blk(w, 3, 1)] + yr[w, 0, 0] + yr[w, 1, 2]
        return first, second

    own_rows = pl.ds(me * tok, tok)
    loads = [pltpu.make_async_copy(x_hbm, xf.at[own_rows, :], load_sem.at[0]),
             pltpu.make_async_copy(wq_hbm, wq2, load_sem.at[1]),
             pltpu.make_async_copy(wk_hbm, wkv.at[:, pl.ds(0, head_dim)], load_sem.at[2]),
             pltpu.make_async_copy(wv_hbm, wkv.at[:, pl.ds(head_dim, head_dim)], load_sem.at[2])]
    for pos, (dest, part) in enumerate(order):
        src = pl.ds(pl.multiple_of((dest * 2 + part) * wcol, wcol), wcol)
        dst = pl.ds(pos * wcol, wcol)
        loads.append(pltpu.make_async_copy(dy_hbm.at[:, src], yf.at[own_rows, dst], load_sem.at[3]))
        loads.append(pltpu.make_async_copy(wo_hbm.at[:, src], wo.at[:, dst], load_sem.at[4]))
    for cp_ in loads:
        cp_.start()
    barrier = pltpu.get_barrier_semaphore()
    peers = [{'model': (me + k) % (2 * chips)} for k in range(1, 2 * chips)]
    for dev in peers + [to_u, to_d, to_f]:
        pl.semaphore_signal(barrier, inc=1, device_id=dev, device_id_type=pl.DeviceIdType.MESH)
    with jax.named_scope('barrier'):
        pl.semaphore_wait(barrier, 2 * chips + 2)
    loads[0].wait()
    for cp_ in ag_first(0):
        cp_.start()
    with jax.named_scope('loadw'):
        loads[1].wait()
        for k, ref in ((2, wkv), (3, yf.at[own_rows, :]), (4, wo)):
            pltpu.make_async_copy(ref, ref, load_sem.at[k]).wait()
        step = 2 * width // 8

        @pl.loop(0, 8)
        def _(b):
            r2 = pl.ds(pl.multiple_of(b * step, step), step)
            wq2f[r2, :] = wq2[r2, :].astype(F32)
            r1 = pl.ds(pl.multiple_of(b * (step // 2), step // 2), step // 2)
            for h in range(heads):
                wqs[cc, 0, r1, h * head_dim:(h + 1) * head_dim] = wq2f[pl.ds(b * step + h, step // 2, stride=heads), :].astype(BF16)

    for cp_ in ag_ring_first(4) + ag_second(4) + ag_second(0):
        cp_.start()
    wd_own.start()

    def chunk_of(s):
        return (cx + s + s // 2 - 2 * (s // 3)) % chips

    @pl.loop(0, chips)
    def _(s):
        @pl.when(s == 0)
        def _():
            ag_partner(0, cx)

        @pl.when(s == 1)
        def _():
            with jax.named_scope('q1'):
                ag_relays(4)
                ag_stage1(0)
                for cp_ in ag_own(1):
                    cp_.start()
                ag_stage2(0)
            with jax.named_scope('q1w'):
                for xc, h in ((xleft, 1), (xright, 0), (xfar, 0), (xfar, 1)):
                    ag_wait(4, xc, cc, h)
                for cp_ in wy_own:
                    cp_.start()
            ag_partner(0, xright)

        @pl.when(s == 2)
        def _():
            ag_partner(0, xleft)

        @pl.when(s == 3)
        def _():
            ag_stage3(0)
            ag_partner(0, xfar)

        r = pl.ds(chunk_of(s) * chunk, chunk)
        xc = xf[r, :]
        qf[r, :] = dot(xc, wqs[cc, 0], NN).astype(BF16)
        kv[r, :] = dot(xc, wkv[...], NN).astype(BF16)

    @pl.loop(0, chips)
    def _(s):
        @pl.when(s == 1)
        def _():
            with jax.named_scope('f1'):
                ag_stage1(1)
                for cp_ in ag_own(2):
                    cp_.start()

        @pl.when(s == 2)
        def _():
            with jax.named_scope('f2'):
                wy_pass()
                ag_stage2(1)

        i = chunk_of(s)
        r = pl.ds(i * chunk, chunk)
        row_id = lax.broadcasted_iota(jnp.int32, (chunk, seq), 0) + i * chunk
        keep = row_id >= lax.broadcasted_iota(jnp.int32, (chunk, seq), 1)
        for h in range(heads):
            hc = pl.ds(h * head_dim, head_dim)
            sc = dot(qf[r, hc], kv[:, 0:head_dim], NT) * scale
            sc = jnp.where(keep, sc, -jnp.inf)
            ex = jnp.exp(sc - jnp.max(sc, axis=-1, keepdims=True))
            pr = ex * (1.0 / jnp.sum(ex, axis=-1, keepdims=True))
            prob[h, r, :] = pr
            of[r, hc] = dot(pr.astype(BF16), kv[:, head_dim:], NN).astype(BF16)

    def mid_relays():
        ag_stage1(2)
        for cp_ in ag_own(5):
            cp_.start()

    with jax.named_scope('b0'):
        ag_stage3(1)
        ag_partner(1, cx)
        ag_partner(2, cx)

    @pl.loop(0, chips)
    def _(s):
        @pl.when(s == 1)
        def _():
            with jax.named_scope('b1'):
                for xc in (xright, xleft, xfar):
                    ag_partner(1, xc)
            with jax.named_scope('b1y'):
                y_first(0, 1)
                mid_relays()
                y_first(0, 0)
            with jax.named_scope('b1w'):
                ag_stage2(2)
                wy_end()
                ag_partner(2, xright)

        @pl.when(s == 2)
        def _():
            with jax.named_scope('b2'):
                ag_stage3(2)
                ag_partner(2, xleft)

        @pl.when(s == 3)
        def _():
            with jax.named_scope('b3'):
                ag_partner(2, xfar)

        with jax.named_scope('b_comp'):
            i = chunk_of(s)
            r = pl.ds(i * chunk, chunk)
            oc = of[r, :]
            do = dot(yf[r, :], wo[...], NT).astype(BF16)
            dof[r, :] = do
            od = do.astype(F32) * oc.astype(F32)
            for h in range(heads):
                hs = slice(h * head_dim, (h + 1) * head_dim)
                dp = dot(do[:, hs], kv[:, head_dim:], NT)
                ds = (prob[h, r, :] * (dp - jnp.sum(od[:, hs], axis=-1, keepdims=True))).astype(BF16)
                dsf[h, r, :] = ds
                dqf[r, hs] = (dot(ds, kv[:, 0:head_dim], NN) * scale).astype(BF16)

        @pl.when(s == 0)
        def _():
            dqa[0, cc] = dqf[own_rows, :]
            dq_copy(cx, cp).start()

        @pl.when(s > 0)
        def _():
            for core in range(2):
                dq_copy(i, core).start()

    y_first(1, 1)
    with jax.named_scope('t00_dkv'):
        for kc in range(chips):
            ks = slice(kc * chunk, (kc + 1) * chunk)
            qs = slice(kc * chunk, seq)
            dk = jnp.zeros((chunk, head_dim), F32)
            dv = jnp.zeros((chunk, head_dim), F32)
            for h in range(heads):
                hs = slice(h * head_dim, (h + 1) * head_dim)
                dk = dk + dot(dsf[h, qs, ks], qf[qs, hs], TN)
                dv = dv + dot(prob[h, qs, ks].astype(BF16), dof[qs, hs], TN)
            kvp[2 * kc:2 * kc + 2, :, 0:head_dim] = (dk * scale).reshape(2, tok, head_dim)
            kvp[2 * kc:2 * kc + 2, :, head_dim:] = dv.reshape(2, tok, head_dim)
        for xc in range(chips):
            kd_copy(xc).start()

    def kd_ring():
        kd_total.wait_recv()
        for xc in range(chips):
            blk = xc * 2 + cc
            kvp[blk] = kvp[blk] + kvr[xc]
        for kind in (1, 0):
            for side in range(2):
                k_copy(side, kind).start()

    with jax.named_scope('t00_y1'):
        y_first(1, 0)
        kd_ring()

    own = cx * 2 + cc

    cuts = (0, erow // 2, erow, erow + brow, width)

    def dx_near(j):
        cols = slice(cuts[j], cuts[j + 1])
        acc = dot(kvb[own_rows, :], wkv[cols, :], NT)
        for slot in (0, 1, chips - 1):
            for core in range(2):
                acc = acc + dot(dqa[slot, core], wqs[core, slot, cols, :], NT)
        return acc

    def dx_far(j, acc):
        cols = slice(cuts[j], cuts[j + 1])
        for core in range(2):
            acc = acc + dot(dqa[2, core], wqs[core, 2, cols, :], NT)
        dx_ref[:, cols] = acc.astype(BF16)

    def dx_part(j):
        dx_far(j, dx_near(j))

    def out_copy(k, src, dst):
        return pltpu.make_async_copy(src, dst, out_sem.at[k])

    outs = [out_copy(0, dx_ref, dx_out), out_copy(1, dwq_ref, dwq_out), out_copy(2, dwk_ref, dwk_out),
            out_copy(3, dwv_ref, dwv_out), out_copy(4, dwo_ref, dwo_out)]

    with jax.named_scope('t04_ag5'):
        ag_stage1(5)
    with jax.named_scope('t05_y0'):
        dw_blocks(0, 2)
        y_pass(0)
        dw_blocks(0, 3)
        dw_blocks(1, 2)
    with jax.named_scope('t06_ag5'):
        ag_stage2(5)
    with jax.named_scope('t07_kpass'):
        k_pass()
        for cp_ in ag_first(6):
            cp_.start()
    with jax.named_scope('t08_y1'):
        dw_blocks(1, 3)
        y_pass(1)
    with jax.named_scope('t09_ag5'):
        ag_stage3(5)
    with jax.named_scope('t10_kfin'):
        p = kr.at[:, pl.ds(0, 2)]
        rcopy(p, p, kr_s.at[0], kr_r.at[2], to_r).wait_recv()
        kvb[pl.ds(me * tok, half), :] = (kvp[own, 0:half, :] + kr[1, 0] + kr[0, 2]).astype(BF16)
        kvb[pl.ds(me * tok + half, half), :] = (kvp[own, half:, :] + kr[0, 0] + kr[1, 2]).astype(BF16)
        for cp_ in ag_own(3) + ag_second(6):
            cp_.start()
    with jax.named_scope('t11_dqw'):
        dq_total.wait_recv()
        wd_own.wait_recv()
        wd_rest.wait_recv()
    with jax.named_scope('t12_dxa'):
        dx_part(0)
    with jax.named_scope('t13_ag3'):
        ag_stage1(3)
        ag_stage1(6)
    with jax.named_scope('t14_dxa'):
        dx_part(1)
    with jax.named_scope('t15_ag3'):
        ag_stage2(3)
        ag_stage2(6)
    with jax.named_scope('t16_ag3'):
        ag_stage3(3)
        for xc in (cx, xright, xleft, xfar):
            ag_partner(3, xc)
    mrow = width // (2 * chips)
    krow = mrow // rows
    with jax.named_scope('t18_wk'):
        part = dot(xf[:, pl.ds(pl.multiple_of(me * mrow, mrow), mrow)], kvb[...], TN)
        wkp[...] = part.reshape(rows, krow, 2 * head_dim)

    def wk_copy(idx, blk, dev):
        return rcopy(wkp.at[blk], wkr.at[idx], wk_s.at[0], wk_r.at[0], dev)

    wk_total = rcopy(wkr, wkr, wk_s.at[0], wk_r.at[0], to_u)

    wk_copies = [wk_copy(0, yup, to_u), wk_copy(1, ydn, to_d), wk_copy(2, yfar, to_f)]
    for cp_ in wk_copies:
        cp_.start()
    with jax.named_scope('t19_dx2'):
        for xc in (cx, xright, xleft, xfar):
            ag_partner(5, xc)
        dx_part(2)
    with jax.named_scope('t19_ag6'):
        for xc in (cx, xright, xleft):
            ag_partner(6, xc)
        dxacc[...] = dx_near(3)
    with jax.named_scope('t19_ag6f'):
        ag_stage3(6)
    with jax.named_scope('t19_y0f'):
        first, second = y_final(0)
        dwo_ref[:, 0:wcol] = first
        dwo_ref[:, wcol:] = second
        outs[4].start()
    with jax.named_scope('t19_dx3'):
        ag_partner(6, xfar)
        dx_far(3, dxacc[...])
        outs[0].start()
    with jax.named_scope('t20_y1f'):
        for idx, val in enumerate(y_final(1)):
            val = val.T
            for h in range(heads):
                dwq_ref[pl.ds(idx * wcol * heads + h, wcol, stride=heads), :] = val[:, h * head_dim:(h + 1) * head_dim]
        outs[1].start()
    with jax.named_scope('t21_wkf'):
        wk_total.wait_recv()
        wk_sum = wkp[my] + wkr[0] + wkr[1] + wkr[2]
        dwk_ref[...] = wk_sum[:, 0:head_dim]
        dwv_ref[...] = wk_sum[:, head_dim:]
        outs[2].start()
        outs[3].start()

    with jax.named_scope('t22_sends'):
        for arr in range(7):
            ag_sent(arr)
        wd_own.wait_send()
        wd_rest.wait_send()
        wy_total(6).wait_send()
        dq_total.wait_send()
        kd_total.wait_send()
        rcopy(kvp.at[pl.ds(0, 3)], kvp.at[pl.ds(0, 3)], kr_s.at[0], kr_r.at[0], to_r).wait_send()
        rcopy(dwa.at[:, pl.ds(0, 6)], dwa.at[:, pl.ds(0, 6)], yr_s.at[0], yr_r.at[0, 0], to_u).wait_send()
        wk_total.wait_send()
        for cp_ in outs:
            cp_.wait()


def copy_out(*refs):
    n = (len(refs) - 1) // 2
    sem = refs[-1]
    copies = [pltpu.make_async_copy(refs[k], refs[n + k], sem.at[k]) for k in range(n)]
    for cp_ in copies:
        cp_.start()
    for cp_ in copies:
        cp_.wait()


VMEM_LIMIT = 60 * 1000 * 1000


def solution(mesh):
    model_size = mesh.shape['model']
    data_size = mesh.shape['data']
    tok_spec = P(('pod', 'data'), 'model', None)
    chips = model_size // 2

    def device_step(x_loc, dy_loc, w_q, w_k, w_v, w_o):
        tok, width = x_loc.shape[1:]
        head_dim = w_k.shape[2]
        head_cols = w_q.shape[1] * head_dim
        assert chips == 4 and data_size == 4 and w_k.shape[0] == 1 and x_loc.shape[0] == 1
        seq = model_size * tok
        half = tok // 2
        heads = head_cols // head_dim
        wcol = width // (2 * data_size)
        krow = width // (model_size * data_size)
        cfg = (tok, width, head_cols, head_dim, chips, data_size)
        vm = pltpu.VMEM
        dma = pltpu.SemaphoreType.DMA
        scratch = [
            vm((seq, width), BF16), vm((seq, width), BF16), vm((2, chips, width, head_cols), BF16), vm((head_cols, width), BF16),
            vm((width, 2 * head_dim), BF16), vm((heads * width, head_dim), BF16), vm((heads * width, head_dim), F32),
            vm((seq, head_cols), BF16), vm((seq, 2 * head_dim), BF16), vm((seq, head_cols), BF16),
            vm((heads, seq, seq), F32), vm((heads, seq, seq), BF16), vm((seq, head_cols), BF16), vm((seq, head_cols), BF16),
            vm((seq, 2 * head_dim), BF16), vm((chips, 2, tok, head_cols), BF16),
            vm((model_size, tok, 2 * head_dim), F32), vm((chips, tok, 2 * head_dim), F32), vm((2, 3, half, 2 * head_dim), F32),
            vm((2, 2 * data_size, head_cols, wcol), F32), vm((2, 2, 3, head_cols, wcol), F32),
            vm((data_size, krow, 2 * head_dim), F32), vm((3, krow, 2 * head_dim), F32),
            vm((tok, 3 * width // 16), F32), vm((tok, width), BF16), vm((heads * 2 * wcol, head_dim), F32), vm((krow, head_dim), F32), vm((krow, head_dim), F32),
            vm((head_cols, 2 * wcol), F32),
            dma((5,)), dma((5,)), dma((7,)), dma((7, 10)), dma((1,)), dma((3,)), dma((2,)), dma((2,)),
            dma((1,)), dma((1,)), dma((1,)), dma((1,)), dma((1,)), dma((3,)), dma((1,)), dma((2, 3)), dma((1,)), dma((1,)),
        ]
        anyspec = pl.BlockSpec(memory_space=pl.ANY)
        vspec = pl.BlockSpec(memory_space=pltpu.VMEM)
        shapes = (jax.ShapeDtypeStruct((tok, width), BF16), jax.ShapeDtypeStruct((heads * 2 * wcol, head_dim), F32),
                  jax.ShapeDtypeStruct((krow, head_dim), F32), jax.ShapeDtypeStruct((krow, head_dim), F32),
                  jax.ShapeDtypeStruct((head_cols, 2 * wcol), F32))
        outs = pl.pallas_call(
            functools.partial(body, cfg),
            out_shape=tuple(pltpu.VMEM(a.shape, a.dtype) for a in shapes),
            in_specs=[anyspec] * 6,
            out_specs=(anyspec,) * 5,
            scratch_shapes=scratch,
            compiler_params=pltpu.CompilerParams(collective_id=0, has_side_effects=True, vmem_limit_bytes=VMEM_LIMIT),
            name='attn_bwd',
        )(x_loc[0], dy_loc[0], w_q.reshape(width * heads, head_dim), w_o.reshape(head_cols, width), w_k[0], w_v[0])
        dx, dwq, dwk, dwv, dwo = pl.pallas_call(
            copy_out,
            out_shape=shapes,
            in_specs=[vspec] * 5,
            out_specs=(anyspec,) * 5,
            scratch_shapes=[dma((5,))],
            compiler_params=pltpu.CompilerParams(vmem_limit_bytes=4 * 1024 * 1024),
            name='copy_out',
        )(*outs)
        return (dx[None], dwq.reshape(2 * wcol, heads, head_dim), dwk, dwv, dwo.reshape(heads, head_dim, 2 * wcol))

    kv_rows = P(('pod', 'model', 'data'), None)
    return jax.shard_map(device_step, mesh=mesh,
                         in_specs=(tok_spec, tok_spec, P(None, 'model', None), P(), P(), P('model', None, None)),
                         out_specs=(tok_spec, P(('pod', 'data'), 'model', None), kv_rows, kv_rows, P(('pod', 'model'), None, 'data')),
                         check_vma=False)
```

```python
import functools

import jax
import jax.numpy as jnp
from jax import lax
from jax.experimental import pallas as pl
from jax.experimental.pallas import tpu as pltpu
from jax.sharding import PartitionSpec as P

F32 = jnp.float32
BF16 = jnp.bfloat16
NN = (((1,), (0,)), ((), ()))
NT = (((1,), (1,)), ((), ()))
TN = (((0,), (0,)), ((), ()))


def dot(a, b, dims):
    return lax.dot_general(a, b, dims, preferred_element_type=F32)


def body(cfg, x_hbm, dy_hbm, wq_hbm, wo_hbm, wk_hbm, wv_hbm,
         dx_out, dwq_out, dwk_out, dwv_out, dwo_out,
         xf, yf, wqs, wo, wkv, wq2, wq2f, qf, kv, of, prob, dsf, dqf, dof, kvb, dqa,
         kvp, kvr, kr, dwa, yr, wkp, wkr, dxacc, dx_ref, dwq_ref, dwk_ref, dwv_ref, dwo_ref,
         load_sem, out_sem, ag_s, ag_r, wy_s, wy_r, wd_s, wd_r, dq_s, dq_r,
         kd_s, kd_r, kr_s, kr_r, yr_s, yr_r, wk_s, wk_r):
    tok, width, head_cols, head_dim, chips, rows = cfg
    half = tok // 2
    chunk = 2 * tok
    seq = chips * chunk
    heads = head_cols // head_dim
    wcol = width // (2 * rows)
    hcol = width // 2
    qrow = width // 8
    erow = rows * qrow
    brow = (width - erow) // 2
    scale = head_dim ** -0.5

    me = lax.axis_index('model')
    cx = me // 2
    cc = me % 2
    cp = 1 - cc
    xright = (cx + 1) % chips
    xleft = (cx + chips - 1) % chips
    xfar = (cx + 2) % chips
    my = lax.axis_index('data')
    yup = (my + 1) % rows
    ydn = (my + rows - 1) % rows
    yfar = (my + 2) % rows
    to_r = {'model': xright * 2 + cc}
    to_l = {'model': xleft * 2 + cc}
    to_p = {'model': cx * 2 + cp}
    to_u = {'data': yup}
    to_d = {'data': ydn}
    to_f = {'data': yfar}

    def rcopy(src, dst, ssem, rsem, dev):
        return pltpu.make_async_remote_copy(src_ref=src, dst_ref=dst, send_sem=ssem, recv_sem=rsem,
                                            device_id=dev, device_id_type=pl.DeviceIdType.MESH)

    def piece(arr, xc, core, h, base):
        r = pl.ds((xc * 2 + core) * tok + h * half, half)
        if arr == 0:
            return xf.at[r, :]
        if arr == 3:
            return kvb.at[r, :]
        slot = (xc + chips - base) % chips
        if arr == 4:
            return wqs.at[core, slot, pl.ds(my * qrow + h * (qrow // 2), qrow // 2), :]
        if arr >= 5:
            return wqs.at[core, slot, pl.ds(erow + (arr - 5) * brow + h * (brow // 2), brow // 2), :]
        return yf.at[r, pl.ds((arr - 1) * hcol, hcol)]

    def ag_slot(xc, base, h, cross):
        away = (xc + chips - base) % chips
        return 2 * chips - 2 + away if cross else 2 * away - 2 + h

    def ag_copy(arr, idx, xc, core, h, dev):
        base = {'r': xright, 'l': xleft, 'p': cx}[dev]
        return rcopy(piece(arr, xc, core, h, cx), piece(arr, xc, core, h, base), ag_s.at[arr],
                     ag_r.at[arr, ag_slot(xc, base, h, dev == 'p')], {'r': to_r, 'l': to_l, 'p': to_p}[dev])

    def ag_ring_first(arr):
        return [ag_copy(arr, 0, cx, cc, 0, 'r'), ag_copy(arr, 2, cx, cc, 1, 'l')]

    def ag_first(arr):
        return ag_ring_first(arr) + [ag_copy(arr, 4, cx, cc, 0, 'p'), ag_copy(arr, 5, cx, cc, 1, 'p')]

    def ag_second(arr):
        return [ag_copy(arr, 1, cx, cc, 1, 'r'), ag_copy(arr, 3, cx, cc, 0, 'l')]

    def ag_own(arr):
        return ag_first(arr) + ag_second(arr)

    def ag_relay(arr):
        return [ag_copy(arr, 6, xleft, cc, 0, 'r'), ag_copy(arr, 7, xright, cc, 1, 'l')]

    def ag_cross(arr, idx, xc, h):
        return ag_copy(arr, idx, xc, cc, h, 'p')

    def ag_wait(arr, xc, core, h):
        p = piece(arr, xc, core, h, cx)
        rcopy(p, p, ag_s.at[arr], ag_r.at[arr, ag_slot(xc, cx, h, False)], to_p).wait_recv()

    def ag_relays(arr):
        relays = ag_relay(arr)
        ag_wait(arr, xleft, cc, 0)
        relays[0].start()
        ag_wait(arr, xright, cc, 1)
        relays[1].start()

    def ag_stage1(arr):
        ag_relays(arr)
        ag_cross(arr, 8, xleft, 0).start()
        ag_cross(arr, 11, xright, 1).start()

    def ag_stage2(arr):
        ag_wait(arr, xright, cc, 0)
        ag_cross(arr, 10, xright, 0).start()
        ag_wait(arr, xleft, cc, 1)
        ag_cross(arr, 9, xleft, 1).start()

    def ag_stage3(arr):
        ag_wait(arr, xfar, cc, 0)
        ag_cross(arr, 12, xfar, 0).start()
        ag_wait(arr, xfar, cc, 1)
        ag_cross(arr, 13, xfar, 1).start()

    def ag_partner(arr, xc):
        r = pl.ds((xc * 2 + cp) * tok, tok)
        if arr == 0:
            p = xf.at[r, :]
        elif arr == 3:
            p = kvb.at[r, :]
        elif arr >= 5:
            p = wqs.at[cp, (xc + chips - cx) % chips, pl.ds(erow + (arr - 5) * brow, brow), :]
        else:
            p = yf.at[r, pl.ds((arr - 1) * hcol, hcol)]
        rcopy(p, p, ag_s.at[arr], ag_r.at[arr, ag_slot(xc, cx, 0, True)], to_p).wait_recv()

    def ag_sent(arr):
        r = pl.ds(0, 7 * tok)
        p = {0: xf.at[r, :], 1: yf.at[r, pl.ds(0, hcol)], 2: yf.at[r, pl.ds(0, hcol)], 3: kvb.at[r, :],
             4: wqs.at[0, 0, pl.ds(0, 3 * qrow), :], 5: wqs.at[:, 0, pl.ds(0, 7 * brow // 2), :],
             6: wqs.at[:, 0, pl.ds(0, 7 * brow // 2), :]}[arr]
        rcopy(p, p, ag_s.at[arr], ag_r.at[arr, 0], to_p).wait_send()

    def wy_copy(idx, q, h, dev):
        p = wqs.at[cc, pl.ds(1, chips - 1), pl.ds(q * qrow + h * (qrow // 2), qrow // 2), :]
        return rcopy(p, p, wy_s.at[0], wy_r.at[idx], dev)

    wy_own = [wy_copy(0, my, 0, to_u), wy_copy(1, my, 1, to_d), wy_copy(2, my, 1, to_u), wy_copy(2, my, 0, to_d)]
    wy_relay = [wy_copy(2, ydn, 0, to_u), wy_copy(2, yup, 1, to_d)]

    def wy_pass():
        wy_copy(0, ydn, 0, to_u).wait_recv()
        wy_relay[0].start()
        wy_copy(1, yup, 1, to_u).wait_recv()
        wy_relay[1].start()

    def wy_total(count):
        p = wqs.at[cc, pl.ds(1, chips - 1), pl.ds(0, count * (qrow // 2)), :]
        return rcopy(p, p, wy_s.at[0], wy_r.at[2], to_u)

    wd_own = rcopy(wqs.at[cc, 0, pl.ds(0, erow), :], wqs.at[cc, 0, pl.ds(0, erow), :], wd_s.at[0], wd_r.at[0], to_p)
    wd_rest = rcopy(wqs.at[cc, pl.ds(1, chips - 1), pl.ds(0, erow), :], wqs.at[cc, pl.ds(1, chips - 1), pl.ds(0, erow), :],
                    wd_s.at[1], wd_r.at[1], to_p)

    def wy_end():
        wy_total(4).wait_recv()
        wd_rest.start()

    def dq_copy(xc, core):
        return rcopy(dqf.at[pl.ds((xc * 2 + core) * tok, tok), :], dqa.at[(cx + chips - xc) % chips, cc],
                     dq_s.at[0], dq_r.at[0], {'model': xc * 2 + core})

    dq_total = rcopy(dqf.at[pl.ds(0, 7 * tok), :], dqf.at[pl.ds(0, 7 * tok), :], dq_s.at[0], dq_r.at[0], to_p)

    def kd_copy(xc):
        return rcopy(kvp.at[xc * 2 + cp], kvr.at[xc], kd_s.at[0], kd_r.at[0], to_p)

    kd_total = rcopy(kvr, kvr, kd_s.at[0], kd_r.at[0], to_p)

    def kpart(xc, h):
        return kvp.at[xc * 2 + cc, pl.ds(h * half, half), :]

    def ring_src(kind, side):
        if kind == 0:
            return (xright, 1) if side == 0 else (xleft, 0)
        if kind == 1:
            return (xfar, 0) if side == 0 else (xfar, 1)
        return (xright, 0) if side == 0 else (xleft, 1)

    def k_copy(side, kind):
        xc, h = ring_src(kind, side)
        return rcopy(kpart(xc, h), kr.at[side, kind], kr_s.at[0], kr_r.at[side if kind == 1 else 2],
                     to_r if side == 0 else to_l)

    def k_pass():
        for side in range(2):
            k_copy(side, 1).wait_recv()
            xc, h = ring_src(2, side)
            ref = kpart(xc, h)
            ref[...] = ref[...] + kr[side, 1]
            k_copy(side, 2).start()

    order = ((yfar, 0), (yfar, 1), (yup, 1), (ydn, 0), (yup, 0), (ydn, 1), (my, 0), (my, 1))

    def y_blk(w, kind, side):
        pos = {(1, 0): 0, (1, 1): 1, (0, 0): 2, (0, 1): 3, (2, 0): 4, (2, 1): 5, (3, 0): 6, (3, 1): 7}[kind, side]
        if w == 0:
            return pos
        return order[pos][0] * 2 + order[pos][1]

    def y_copy(w, side, kind):
        return rcopy(dwa.at[w, y_blk(w, kind, side)], yr.at[w, side, kind], yr_s.at[0], yr_r.at[w, side if kind == 1 else 2],
                     to_u if side == 0 else to_d)

    def dw_block(w, kind, side):
        blk = y_blk(w, kind, side)
        if w == 0:
            dwa[0, blk] = dot(of[...], yf[:, blk * wcol:(blk + 1) * wcol], TN)
        else:
            dwa[1, blk] = dot(dqf[...], xf[:, pl.ds(pl.multiple_of(blk * wcol, wcol), wcol)], TN)

    def y_first(w, kind):
        for side in range(2):
            dw_block(w, kind, side)
            y_copy(w, side, kind).start()

    def dw_blocks(w, kind):
        for side in range(2):
            dw_block(w, kind, side)

    def y_pass(w):
        for side in range(2):
            y_copy(w, side, 1).wait_recv()
            blk = y_blk(w, 2, side)
            dwa[w, blk] = dwa[w, blk] + yr[w, side, 1]
            y_copy(w, side, 2).start()

    def y_final(w):
        p = yr.at[w, :, pl.ds(0, 2)]
        rcopy(p, p, yr_s.at[0], yr_r.at[w, 2], to_u).wait_recv()
        first = dwa[w, y_blk(w, 3, 0)] + yr[w, 1, 0] + yr[w, 0, 2]
        second = dwa[w, y_blk(w, 3, 1)] + yr[w, 0, 0] + yr[w, 1, 2]
        return first, second

    own_rows = pl.ds(me * tok, tok)
    loads = [pltpu.make_async_copy(x_hbm, xf.at[own_rows, :], load_sem.at[0]),
             pltpu.make_async_copy(wq_hbm, wq2, load_sem.at[1]),
             pltpu.make_async_copy(wk_hbm, wkv.at[:, pl.ds(0, head_dim)], load_sem.at[2]),
             pltpu.make_async_copy(wv_hbm, wkv.at[:, pl.ds(head_dim, head_dim)], load_sem.at[2])]
    for pos, (dest, part) in enumerate(order):
        src = pl.ds(pl.multiple_of((dest * 2 + part) * wcol, wcol), wcol)
        dst = pl.ds(pos * wcol, wcol)
        loads.append(pltpu.make_async_copy(dy_hbm.at[:, src], yf.at[own_rows, dst], load_sem.at[3]))
        loads.append(pltpu.make_async_copy(wo_hbm.at[:, src], wo.at[:, dst], load_sem.at[4]))
    for cp_ in loads:
        cp_.start()
    barrier = pltpu.get_barrier_semaphore()
    peers = [{'model': (me + k) % (2 * chips)} for k in range(1, 2 * chips)]
    for dev in peers + [to_u, to_d, to_f]:
        pl.semaphore_signal(barrier, inc=1, device_id=dev, device_id_type=pl.DeviceIdType.MESH)
    with jax.named_scope('barrier'):
        pl.semaphore_wait(barrier, 2 * chips + 2)
    loads[0].wait()
    for cp_ in ag_first(0):
        cp_.start()
    with jax.named_scope('loadw'):
        loads[1].wait()
        for k, ref in ((2, wkv), (3, yf.at[own_rows, :]), (4, wo)):
            pltpu.make_async_copy(ref, ref, load_sem.at[k]).wait()
        step = 2 * width // 8

        @pl.loop(0, 8)
        def _(b):
            r2 = pl.ds(pl.multiple_of(b * step, step), step)
            wq2f[r2, :] = wq2[r2, :].astype(F32)
            r1 = pl.ds(pl.multiple_of(b * (step // 2), step // 2), step // 2)
            for h in range(heads):
                wqs[cc, 0, r1, h * head_dim:(h + 1) * head_dim] = wq2f[pl.ds(b * step + h, step // 2, stride=heads), :].astype(BF16)

    for cp_ in ag_ring_first(4) + ag_second(4) + ag_second(0):
        cp_.start()
    wd_own.start()

    def chunk_of(s):
        return (cx + s + s // 2 - 2 * (s // 3)) % chips

    @pl.loop(0, chips)
    def _(s):
        @pl.when(s == 0)
        def _():
            ag_partner(0, cx)

        @pl.when(s == 1)
        def _():
            with jax.named_scope('q1'):
                ag_relays(4)
                ag_stage1(0)
                for cp_ in ag_own(1):
                    cp_.start()
                ag_stage2(0)
            with jax.named_scope('q1w'):
                for xc, h in ((xleft, 1), (xright, 0), (xfar, 0), (xfar, 1)):
                    ag_wait(4, xc, cc, h)
                for cp_ in wy_own:
                    cp_.start()
            ag_partner(0, xright)

        @pl.when(s == 2)
        def _():
            ag_partner(0, xleft)

        @pl.when(s == 3)
        def _():
            ag_stage3(0)
            ag_partner(0, xfar)

        r = pl.ds(chunk_of(s) * chunk, chunk)
        xc = xf[r, :]
        qf[r, :] = dot(xc, wqs[cc, 0], NN).astype(BF16)
        kv[r, :] = dot(xc, wkv[...], NN).astype(BF16)

    @pl.loop(0, chips)
    def _(s):
        @pl.when(s == 1)
        def _():
            with jax.named_scope('f1'):
                ag_stage1(1)
                for cp_ in ag_own(2):
                    cp_.start()

        @pl.when(s == 2)
        def _():
            with jax.named_scope('f2'):
                wy_pass()
                ag_stage2(1)

        i = chunk_of(s)
        r = pl.ds(i * chunk, chunk)
        row_id = lax.broadcasted_iota(jnp.int32, (chunk, seq), 0) + i * chunk
        keep = row_id >= lax.broadcasted_iota(jnp.int32, (chunk, seq), 1)
        for h in range(heads):
            hc = pl.ds(h * head_dim, head_dim)
            sc = dot(qf[r, hc], kv[:, 0:head_dim], NT) * scale
            sc = jnp.where(keep, sc, -jnp.inf)
            ex = jnp.exp(sc - jnp.max(sc, axis=-1, keepdims=True))
            pr = ex * (1.0 / jnp.sum(ex, axis=-1, keepdims=True))
            prob[h, r, :] = pr
            of[r, hc] = dot(pr.astype(BF16), kv[:, head_dim:], NN).astype(BF16)

    def mid_relays():
        ag_stage1(2)
        for cp_ in ag_own(5):
            cp_.start()

    with jax.named_scope('b0'):
        ag_stage3(1)
        ag_partner(1, cx)
        ag_partner(2, cx)

    @pl.loop(0, chips)
    def _(s):
        @pl.when(s == 1)
        def _():
            with jax.named_scope('b1'):
                for xc in (xright, xleft, xfar):
                    ag_partner(1, xc)
            with jax.named_scope('b1y'):
                y_first(0, 1)
                mid_relays()
                y_first(0, 0)
            with jax.named_scope('b1w'):
                ag_stage2(2)
                wy_end()
                ag_partner(2, xright)

        @pl.when(s == 2)
        def _():
            with jax.named_scope('b2'):
                ag_stage3(2)
                ag_partner(2, xleft)

        @pl.when(s == 3)
        def _():
            with jax.named_scope('b3'):
                ag_partner(2, xfar)

        with jax.named_scope('b_comp'):
            i = chunk_of(s)
            r = pl.ds(i * chunk, chunk)
            oc = of[r, :]
            do = dot(yf[r, :], wo[...], NT).astype(BF16)
            dof[r, :] = do
            od = do.astype(F32) * oc.astype(F32)
            for h in range(heads):
                hs = slice(h * head_dim, (h + 1) * head_dim)
                dp = dot(do[:, hs], kv[:, head_dim:], NT)
                ds = (prob[h, r, :] * (dp - jnp.sum(od[:, hs], axis=-1, keepdims=True))).astype(BF16)
                dsf[h, r, :] = ds
                dqf[r, hs] = (dot(ds, kv[:, 0:head_dim], NN) * scale).astype(BF16)

        @pl.when(s == 0)
        def _():
            dqa[0, cc] = dqf[own_rows, :]
            dq_copy(cx, cp).start()

        @pl.when(s > 0)
        def _():
            for core in range(2):
                dq_copy(i, core).start()

    y_first(1, 1)
    with jax.named_scope('t00_dkv'):
        for kc in range(chips):
            ks = slice(kc * chunk, (kc + 1) * chunk)
            qs = slice(kc * chunk, seq)
            dk = jnp.zeros((chunk, head_dim), F32)
            dv = jnp.zeros((chunk, head_dim), F32)
            for h in range(heads):
                hs = slice(h * head_dim, (h + 1) * head_dim)
                dk = dk + dot(dsf[h, qs, ks], qf[qs, hs], TN)
                dv = dv + dot(prob[h, qs, ks].astype(BF16), dof[qs, hs], TN)
            kvp[2 * kc:2 * kc + 2, :, 0:head_dim] = (dk * scale).reshape(2, tok, head_dim)
            kvp[2 * kc:2 * kc + 2, :, head_dim:] = dv.reshape(2, tok, head_dim)
        for xc in range(chips):
            kd_copy(xc).start()

    def kd_ring():
        kd_total.wait_recv()
        for xc in range(chips):
            blk = xc * 2 + cc
            kvp[blk] = kvp[blk] + kvr[xc]
        for kind in (1, 0):
            for side in range(2):
                k_copy(side, kind).start()

    with jax.named_scope('t00_y1'):
        y_first(1, 0)
        kd_ring()

    own = cx * 2 + cc

    cuts = (0, erow // 2, erow, erow + brow, width)

    def dx_near(j):
        cols = slice(cuts[j], cuts[j + 1])
        acc = dot(kvb[own_rows, :], wkv[cols, :], NT)
        for slot in (0, 1, chips - 1):
            for core in range(2):
                acc = acc + dot(dqa[slot, core], wqs[core, slot, cols, :], NT)
        return acc

    def dx_far(j, acc):
        cols = slice(cuts[j], cuts[j + 1])
        for core in range(2):
            acc = acc + dot(dqa[2, core], wqs[core, 2, cols, :], NT)
        dx_ref[:, cols] = acc.astype(BF16)

    def dx_part(j):
        dx_far(j, dx_near(j))

    def out_copy(k, src, dst):
        return pltpu.make_async_copy(src, dst, out_sem.at[k])

    outs = [out_copy(0, dx_ref, dx_out), out_copy(1, dwq_ref, dwq_out), out_copy(2, dwk_ref, dwk_out),
            out_copy(3, dwv_ref, dwv_out), out_copy(4, dwo_ref, dwo_out)]

    with jax.named_scope('t04_ag5'):
        ag_stage1(5)
    with jax.named_scope('t05_y0'):
        dw_blocks(0, 2)
        y_pass(0)
        dw_blocks(0, 3)
        dw_blocks(1, 2)
    with jax.named_scope('t06_ag5'):
        ag_stage2(5)
    with jax.named_scope('t07_kpass'):
        k_pass()
        for cp_ in ag_first(6):
            cp_.start()
    with jax.named_scope('t08_y1'):
        dw_blocks(1, 3)
        y_pass(1)
    with jax.named_scope('t09_ag5'):
        ag_stage3(5)
    with jax.named_scope('t10_kfin'):
        p = kr.at[:, pl.ds(0, 2)]
        rcopy(p, p, kr_s.at[0], kr_r.at[2], to_r).wait_recv()
        kvb[pl.ds(me * tok, half), :] = (kvp[own, 0:half, :] + kr[1, 0] + kr[0, 2]).astype(BF16)
        kvb[pl.ds(me * tok + half, half), :] = (kvp[own, half:, :] + kr[0, 0] + kr[1, 2]).astype(BF16)
        for cp_ in ag_own(3) + ag_second(6):
            cp_.start()
    with jax.named_scope('t11_dqw'):
        dq_total.wait_recv()
        wd_own.wait_recv()
        wd_rest.wait_recv()
    with jax.named_scope('t12_dxa'):
        dx_part(0)
    with jax.named_scope('t13_ag3'):
        ag_stage1(3)
        ag_stage1(6)
    with jax.named_scope('t14_dxa'):
        dx_part(1)
    with jax.named_scope('t15_ag3'):
        ag_stage2(3)
        ag_stage2(6)
    with jax.named_scope('t16_ag3'):
        ag_stage3(3)
        for xc in (cx, xright, xleft, xfar):
            ag_partner(3, xc)
    mrow = width // (2 * chips)
    krow = mrow // rows
    with jax.named_scope('t18_wk'):
        part = dot(xf[:, pl.ds(pl.multiple_of(me * mrow, mrow), mrow)], kvb[...], TN)
        wkp[...] = part.reshape(rows, krow, 2 * head_dim)

    def wk_copy(idx, blk, dev):
        return rcopy(wkp.at[blk], wkr.at[idx], wk_s.at[0], wk_r.at[0], dev)

    wk_total = rcopy(wkr, wkr, wk_s.at[0], wk_r.at[0], to_u)

    wk_copies = [wk_copy(0, yup, to_u), wk_copy(1, ydn, to_d), wk_copy(2, yfar, to_f)]
    for cp_ in wk_copies:
        cp_.start()
    with jax.named_scope('t19_dx2'):
        for xc in (cx, xright, xleft, xfar):
            ag_partner(5, xc)
        dx_part(2)
    with jax.named_scope('t19_ag6'):
        for xc in (cx, xright, xleft):
            ag_partner(6, xc)
        dxacc[...] = dx_near(3)
    with jax.named_scope('t19_ag6f'):
        ag_stage3(6)
    with jax.named_scope('t19_y0f'):
        first, second = y_final(0)
        dwo_ref[:, 0:wcol] = first
        dwo_ref[:, wcol:] = second
        outs[4].start()
    with jax.named_scope('t19_dx3'):
        ag_partner(6, xfar)
        dx_far(3, dxacc[...])
        outs[0].start()
    with jax.named_scope('t20_y1f'):
        for idx, val in enumerate(y_final(1)):
            val = val.T
            for h in range(heads):
                dwq_ref[pl.ds(idx * wcol * heads + h, wcol, stride=heads), :] = val[:, h * head_dim:(h + 1) * head_dim]
        outs[1].start()
    with jax.named_scope('t21_wkf'):
        wk_total.wait_recv()
        wk_sum = wkp[my] + wkr[0] + wkr[1] + wkr[2]
        dwk_ref[...] = wk_sum[:, 0:head_dim]
        dwv_ref[...] = wk_sum[:, head_dim:]
        outs[2].start()
        outs[3].start()

    with jax.named_scope('t22_sends'):
        for arr in range(7):
            ag_sent(arr)
        wd_own.wait_send()
        wd_rest.wait_send()
        wy_total(6).wait_send()
        dq_total.wait_send()
        kd_total.wait_send()
        rcopy(kvp.at[pl.ds(0, 3)], kvp.at[pl.ds(0, 3)], kr_s.at[0], kr_r.at[0], to_r).wait_send()
        rcopy(dwa.at[:, pl.ds(0, 6)], dwa.at[:, pl.ds(0, 6)], yr_s.at[0], yr_r.at[0, 0], to_u).wait_send()
        wk_total.wait_send()
        for cp_ in outs:
            cp_.wait()


def copy_out(*refs):
    n = (len(refs) - 1) // 2
    sem = refs[-1]
    copies = [pltpu.make_async_copy(refs[k], refs[n + k], sem.at[k]) for k in range(n)]
    for cp_ in copies:
        cp_.start()
    for cp_ in copies:
        cp_.wait()


VMEM_LIMIT = 60 * 1000 * 1000


def solution(mesh):
    model_size = mesh.shape['model']
    data_size = mesh.shape['data']
    tok_spec = P(('pod', 'data'), 'model', None)
    chips = model_size // 2

    def device_step(x_loc, dy_loc, w_q, w_k, w_v, w_o):
        tok, width = x_loc.shape[1:]
        head_dim = w_k.shape[2]
        head_cols = w_q.shape[1] * head_dim
        assert chips == 4 and data_size == 4 and w_k.shape[0] == 1 and x_loc.shape[0] == 1
        seq = model_size * tok
        half = tok // 2
        heads = head_cols // head_dim
        wcol = width // (2 * data_size)
        krow = width // (model_size * data_size)
        cfg = (tok, width, head_cols, head_dim, chips, data_size)
        vm = pltpu.VMEM
        dma = pltpu.SemaphoreType.DMA
        scratch = [
            vm((seq, width), BF16), vm((seq, width), BF16), vm((2, chips, width, head_cols), BF16), vm((head_cols, width), BF16),
            vm((width, 2 * head_dim), BF16), vm((heads * width, head_dim), BF16), vm((heads * width, head_dim), F32),
            vm((seq, head_cols), BF16), vm((seq, 2 * head_dim), BF16), vm((seq, head_cols), BF16),
            vm((heads, seq, seq), F32), vm((heads, seq, seq), BF16), vm((seq, head_cols), BF16), vm((seq, head_cols), BF16),
            vm((seq, 2 * head_dim), BF16), vm((chips, 2, tok, head_cols), BF16),
            vm((model_size, tok, 2 * head_dim), F32), vm((chips, tok, 2 * head_dim), F32), vm((2, 3, half, 2 * head_dim), F32),
            vm((2, 2 * data_size, head_cols, wcol), F32), vm((2, 2, 3, head_cols, wcol), F32),
            vm((data_size, krow, 2 * head_dim), F32), vm((3, krow, 2 * head_dim), F32),
            vm((tok, width // 4), F32), vm((tok, width), BF16), vm((heads * 2 * wcol, head_dim), F32), vm((krow, head_dim), F32), vm((krow, head_dim), F32),
            vm((head_cols, 2 * wcol), F32),
            dma((5,)), dma((5,)), dma((7,)), dma((7, 10)), dma((1,)), dma((3,)), dma((2,)), dma((2,)),
            dma((1,)), dma((1,)), dma((1,)), dma((1,)), dma((1,)), dma((3,)), dma((1,)), dma((2, 3)), dma((1,)), dma((1,)),
        ]
        anyspec = pl.BlockSpec(memory_space=pl.ANY)
        vspec = pl.BlockSpec(memory_space=pltpu.VMEM)
        shapes = (jax.ShapeDtypeStruct((tok, width), BF16), jax.ShapeDtypeStruct((heads * 2 * wcol, head_dim), F32),
                  jax.ShapeDtypeStruct((krow, head_dim), F32), jax.ShapeDtypeStruct((krow, head_dim), F32),
                  jax.ShapeDtypeStruct((head_cols, 2 * wcol), F32))
        outs = pl.pallas_call(
            functools.partial(body, cfg),
            out_shape=tuple(pltpu.VMEM(a.shape, a.dtype) for a in shapes),
            in_specs=[anyspec] * 6,
            out_specs=(anyspec,) * 5,
            scratch_shapes=scratch,
            compiler_params=pltpu.CompilerParams(collective_id=0, has_side_effects=True, vmem_limit_bytes=VMEM_LIMIT),
            name='attn_bwd',
        )(x_loc[0], dy_loc[0], w_q.reshape(width * heads, head_dim), w_o.reshape(head_cols, width), w_k[0], w_v[0])
        dx, dwq, dwk, dwv, dwo = pl.pallas_call(
            copy_out,
            out_shape=shapes,
            in_specs=[vspec] * 5,
            out_specs=(anyspec,) * 5,
            scratch_shapes=[dma((5,))],
            compiler_params=pltpu.CompilerParams(vmem_limit_bytes=4 * 1024 * 1024),
            name='copy_out',
        )(*outs)
        return (dx[None], dwq.reshape(2 * wcol, heads, head_dim), dwk, dwv, dwo.reshape(heads, head_dim, 2 * wcol))

    kv_rows = P(('pod', 'model', 'data'), None)
    return jax.shard_map(device_step, mesh=mesh,
                         in_specs=(tok_spec, tok_spec, P(None, 'model', None), P(), P(), P('model', None, None)),
                         out_specs=(tok_spec, P(('pod', 'data'), 'model', None), kv_rows, kv_rows, P(('pod', 'model'), None, 'data')),
                         check_vma=False)
```
